256 devices in a mesh: img: 8 (over y, core), tile: 32 (over z, x).
Axes of the slice: x: 4, y: 4, z: 8, core: 2. Of those that a mesh axis runs over, the one named last changes fastest.
Arguments:
- means: float32 [3, 524288], P(None, ('img', 'tile')), may hold values from -3 to 3
- log_scales: float32 [3, 524288], P(None, ('img', 'tile')), may hold values from -6 to -3
- quat_w: float32 [1, 524288], P(None, ('img', 'tile')), may hold values from 1 to 2
- quat_v: float32 [3, 524288], P(None, ('img', 'tile')), may hold values from -1 to 1
- opacity: float32 [1, 524288], P(None, ('img', 'tile')), may hold values from -6 to 6
- sh_coeffs: float32 [48, 524288], P(None, ('img', 'tile')), may hold values from -3 to 3
- cameras: float32 [8, 10], replicated, may hold values from -300 to 300
- requests: int32 [8, 32, 8, 32, 16], P('img', 'tile'), may hold values from 0 to 2047, as said below
- lists: int32 [8, 256, 256], P('img', 'tile'), may hold values from 0 to 4095, as said below
- counts: int32 [8, 256], P('img', 'tile'), may hold values from 1 to 256
- image_cot: float32 [8, 3, 256, 256], P('img', None, 'tile'), may hold values from -6 to 6
Outputs:
- rendered: float32 [8, 3, 256, 256], P('img', None, 'tile')
- param_grad: float32 [59, 524288], P(None, ('img', 'tile'))
- camera_grad: float32 [8, 10], replicated
The draws below stay inside these ranges and needn't reach their ends.
Inputs may be any that keep to these rules, and one draw needn't show every extreme that they name: Entries may repeat within a device's requests. `lists`: each entry names a request slot of the device that renders the tile; slot (a * 32 + b) * 16 + c is requests[i, t, a, b, c]; only the first counts entries of a list are live.
All inputs are finite; a program needn't handle non-finite values.
Results may differ from the reference program's by a relative error of at most 0.0003.
Values sent between devices are 32-bit elements; how exact they have to be, the bound alone decides.
No kernel may reach another device: no remote copies, remote signals or barrier semaphores. Data moves between devices by JAX's collectives and lax.ppermute only.
A program may use at most 64 MiB of HBM per device.

```python
import math
import jax
import jax.numpy as jnp
from jax import lax

NG_DEV = 2048
TILES_DEV = 8
LIST = 256
CAP = 16
TILE_SIDE = 16
TW = 16
G = 524288
TILES = 256
SLOTS = 4096
PIX = 256
N_IMG = 8
N_TILE = 32


def scene_integers(key):
    base = jax.random.fold_in(key, 4409)
    requests = jax.random.randint(jax.random.fold_in(base, 1), (N_IMG, N_TILE, N_IMG, N_TILE, CAP), 0, NG_DEV, dtype=jnp.int32)
    lists = jax.random.randint(jax.random.fold_in(base, 2), (N_IMG, TILES, LIST), 0, SLOTS, dtype=jnp.int32)
    counts = jax.random.randint(jax.random.fold_in(base, 3), (N_IMG, TILES), 1, LIST + 1, dtype=jnp.int32)
    return (requests, lists, counts)


def scene_cameras(key):
    base = jax.random.fold_in(key, 5501)
    quats = jax.random.normal(jax.random.fold_in(base, 1), (N_IMG, 4), dtype=jnp.float32)
    quats = quats / jnp.sqrt(jnp.sum(quats * quats, axis=1, keepdims=True))
    unit_w, unit_x, unit_y, unit_z = (quats[:, 0], quats[:, 1], quats[:, 2], quats[:, 3])
    first_row = jnp.stack([1.0 - 2.0 * (unit_y * unit_y + unit_z * unit_z), 2.0 * (unit_x * unit_y - unit_w * unit_z), 2.0 * (unit_x * unit_z + unit_w * unit_y)], axis=1)
    second_row = jnp.stack([2.0 * (unit_x * unit_y + unit_w * unit_z), 1.0 - 2.0 * (unit_x * unit_x + unit_z * unit_z), 2.0 * (unit_y * unit_z - unit_w * unit_x)], axis=1)
    third_row = jnp.stack([2.0 * (unit_x * unit_z - unit_w * unit_y), 2.0 * (unit_y * unit_z + unit_w * unit_x), 1.0 - 2.0 * (unit_x * unit_x + unit_y * unit_y)], axis=1)
    gain = jnp.exp(jax.random.uniform(jax.random.fold_in(base, 2), (N_IMG,), jnp.float32, math.log(150.0), math.log(300.0)))
    offset = jax.random.uniform(jax.random.fold_in(base, 3), (N_IMG, 2), jnp.float32, -20.0, 20.0)
    polar = jax.random.uniform(jax.random.fold_in(base, 4), (N_IMG, 1), jnp.float32, 0.3, 2.8)
    azimuth = jax.random.uniform(jax.random.fold_in(base, 5), (N_IMG, 1), jnp.float32, -math.pi, math.pi)
    cameras = jnp.concatenate([gain[:, None] * first_row, gain[:, None] * second_row, offset, polar, azimuth], axis=1)
    return (cameras, third_row, gain)


def draw_requests(key, part):
    return scene_integers(key)[0]


def draw_lists(key, part):
    return scene_integers(key)[1]


def draw_counts(key, part):
    return scene_integers(key)[2]


def draw_cameras(key, part):
    return scene_cameras(key)[0].astype(jnp.float32)


def draw_means(key, part):
    requests, lists, counts = scene_integers(key)
    cameras, depth_axis, gain = scene_cameras(key)
    tile_owner = (jnp.arange(TILES, dtype=jnp.int32) // TILES_DEV)[None, :, None]
    image_index = jnp.arange(N_IMG, dtype=jnp.int32)[:, None, None]
    owner_flat = lists // CAP
    choose = lists % CAP
    local = requests[image_index, tile_owner, owner_flat // N_TILE, owner_flat % N_TILE, choose]
    gaussian_ids = (owner_flat * NG_DEV + local).reshape(-1)
    entry_ids = jnp.arange(N_IMG * TILES * LIST, dtype=jnp.int32).reshape(N_IMG, TILES, LIST)
    live = jnp.arange(LIST, dtype=jnp.int32)[None, None, :] < counts[:, :, None]
    score = jnp.where(live, entry_ids, -1).reshape(-1)
    winner = jnp.full((G,), -1, dtype=jnp.int32).at[gaussian_ids].max(score)
    placed = winner >= 0
    safe = jnp.maximum(winner, 0)
    win_image = safe // (TILES * LIST)
    win_tile = safe // LIST % TILES
    place_key = jax.random.fold_in(key, 6607)
    jitter = jax.random.uniform(jax.random.fold_in(place_key, 1), (2, G), jnp.float32, -12.0, 12.0)
    height = TILE_SIDE * TILES / TW
    centre_x = (TILE_SIDE * (win_tile % TW)).astype(jnp.float32) + 0.5 * TILE_SIDE - 0.5 * TILE_SIDE * TW
    centre_y = (TILE_SIDE * (win_tile // TW)).astype(jnp.float32) + 0.5 * TILE_SIDE - 0.5 * height
    chosen = cameras[win_image]
    target_x = centre_x + jitter[0] - chosen[:, 6]
    target_y = centre_y + jitter[1] - chosen[:, 7]
    squared_gain = (gain * gain)[win_image]
    along = (chosen[:, 0:3] * target_x[:, None] + chosen[:, 3:6] * target_y[:, None]) / squared_gain[:, None]
    depth = jax.random.uniform(jax.random.fold_in(place_key, 2), (G,), jnp.float32, -1.0, 1.0)
    aimed = along + depth[:, None] * depth_axis[win_image]
    loose = jax.random.uniform(jax.random.fold_in(place_key, 3), (G, 3), jnp.float32, -1.0, 1.0)
    result = jnp.where(placed[:, None], aimed, loose)
    return result.T.astype(jnp.float32)


def block_scale(own_key, shape, split, smallest, top_value):
    level, own = 1.0, jax.random.fold_in(own_key, 6)
    for axis_at, parts in split:
        steps = jnp.exp(jax.random.uniform(jax.random.fold_in(own, axis_at), (parts,), jnp.float32, smallest / len(split), top_value / len(split)))
        level = level * jnp.repeat(steps, shape[axis_at] // parts).reshape([-1 if axis == axis_at else 1 for axis in range(len(shape))])
    return level


def scatter_about(stream_key, shape, spread, limit, pieces=(), kind=jnp.bfloat16):
    values = jax.random.normal(stream_key, shape, jnp.float32) * spread
    if len(pieces) > 0:
        values = block_scale(stream_key, shape, pieces, -0.22, 0.18) * values
    return jnp.clip(values, min=-limit, max=limit).astype(kind)


def setup_inputs(seed: int = 0) -> dict:
    arg_keys = jax.random.split(jax.random.key(seed), 12)
    return {
        "means": draw_means(jax.random.fold_in(arg_keys[11], 71), 0),
        "log_scales": jnp.clip(-6.0 + 3.0 * jax.random.uniform(arg_keys[1], (3, G), jnp.float32) ** block_scale(arg_keys[1], (3, G), ((1, 256),), -0.2, 0.2), -6.0, -3.0),
        "quat_w": jnp.clip(1.0 + 1.0 * jax.random.uniform(arg_keys[2], (1, G), jnp.float32) ** block_scale(arg_keys[2], (1, G), ((1, 256),), -0.2, 0.2), 1.0, 2.0),
        "quat_v": jnp.clip(jax.random.uniform(arg_keys[3], (3, G), jnp.float32, -1.0, 1.0) * block_scale(arg_keys[3], (3, G), ((1, 256),), -0.4, 0.0), -1.0, 1.0),
        "opacity": jnp.clip(jax.random.uniform(arg_keys[4], (1, G), jnp.float32, -6.0, 6.0) * block_scale(arg_keys[4], (1, G), ((1, 256),), -0.4, 0.0), -6.0, 6.0),
        "sh_coeffs": scatter_about(arg_keys[5], (48, G), 0.5, 3.0, ((1, 256),), jnp.float32),
        "cameras": draw_cameras(jax.random.fold_in(arg_keys[11], 71), 0),
        "requests": draw_requests(jax.random.fold_in(arg_keys[11], 71), 0),
        "lists": draw_lists(jax.random.fold_in(arg_keys[11], 71), 0),
        "counts": draw_counts(jax.random.fold_in(arg_keys[11], 71), 0),
        "image_cot": scatter_about(arg_keys[10], (N_IMG, 3, TILES, PIX), 1.0, 6.0, ((0, 8), (2, 32)), jnp.float32),
    }


sh_first = 0.28209479177387814
sh_second = 0.4886025119029199
sh_third = (1.0925484305920792, -1.0925484305920792, 0.31539156525252005, -1.0925484305920792, 0.5462742152960396)
sh_fourth = (-0.5900435899266435, 2.890611442640554, -0.4570457994644658, 0.3731763325901154, -0.4570457994644658, 1.445305721320277, -0.5900435899266435)
dilation = 0.3

def harmonic_values(camera):
    polar_angle = camera[8]
    azimuth = camera[9]
    view_x = jnp.sin(polar_angle) * jnp.cos(azimuth)
    view_y = jnp.sin(polar_angle) * jnp.sin(azimuth)
    view_z = jnp.cos(polar_angle)
    square_x = view_x * view_x
    square_y = view_y * view_y
    square_z = view_z * view_z
    return jnp.stack([sh_first + 0.0 * view_x, -sh_second * view_y, sh_second * view_z, -sh_second * view_x, sh_third[0] * view_x * view_y, sh_third[1] * view_y * view_z, sh_third[2] * (2.0 * square_z - square_x - square_y), sh_third[3] * view_x * view_z, sh_third[4] * (square_x - square_y), sh_fourth[0] * view_y * (3.0 * square_x - square_y), sh_fourth[1] * view_x * view_y * view_z, sh_fourth[2] * view_y * (4.0 * square_z - square_x - square_y), sh_fourth[3] * view_z * (2.0 * square_z - 3.0 * square_x - 3.0 * square_y), sh_fourth[4] * view_x * (4.0 * square_z - square_x - square_y), sh_fourth[5] * view_z * (square_x - square_y), sh_fourth[6] * view_x * (square_x - 3.0 * square_y)])

def project(params, camera):
    trailing = params.shape[1:]
    mean_x, mean_y, mean_z = (params[0], params[1], params[2])
    screen_x = camera[0] * mean_x + camera[1] * mean_y + camera[2] * mean_z + camera[6]
    screen_y = camera[3] * mean_x + camera[4] * mean_y + camera[5] * mean_z + camera[7]
    quat_norm = jnp.sqrt(params[6] * params[6] + params[7] * params[7] + params[8] * params[8] + params[9] * params[9])
    unit_w = params[6] / quat_norm
    unit_x = params[7] / quat_norm
    unit_y = params[8] / quat_norm
    unit_z = params[9] / quat_norm
    rotation = ((1.0 - 2.0 * (unit_y * unit_y + unit_z * unit_z), 2.0 * (unit_x * unit_y - unit_w * unit_z), 2.0 * (unit_x * unit_z + unit_w * unit_y)), (2.0 * (unit_x * unit_y + unit_w * unit_z), 1.0 - 2.0 * (unit_x * unit_x + unit_z * unit_z), 2.0 * (unit_y * unit_z - unit_w * unit_x)), (2.0 * (unit_x * unit_z - unit_w * unit_y), 2.0 * (unit_y * unit_z + unit_w * unit_x), 1.0 - 2.0 * (unit_x * unit_x + unit_y * unit_y)))
    stretch = (jnp.exp(params[3]), jnp.exp(params[4]), jnp.exp(params[5]))

    def image_row(first_coef, second_coef, third_coef):
        return [(first_coef * rotation[0][col_idx] + second_coef * rotation[1][col_idx] + third_coef * rotation[2][col_idx]) * stretch[col_idx] for col_idx in range(3)]
    upper_row = image_row(camera[0], camera[1], camera[2])
    lower_row = image_row(camera[3], camera[4], camera[5])
    cov_xx = upper_row[0] * upper_row[0] + upper_row[1] * upper_row[1] + upper_row[2] * upper_row[2] + dilation
    cov_xy = upper_row[0] * lower_row[0] + upper_row[1] * lower_row[1] + upper_row[2] * lower_row[2]
    cov_yy = lower_row[0] * lower_row[0] + lower_row[1] * lower_row[1] + lower_row[2] * lower_row[2] + dilation
    determinant = cov_xx * cov_yy - cov_xy * cov_xy
    base_opacity = jax.nn.sigmoid(params[10])
    harmonics = harmonic_values(camera).reshape((1, 16) + (1,) * len(trailing))
    coeffs = params[11:59].reshape((3, 16) + trailing)
    colours = 0.5 + lax.optimization_barrier(jnp.sum(coeffs * harmonics, axis=1))
    return jnp.stack([screen_x, screen_y, cov_yy / determinant, -cov_xy / determinant, cov_xx / determinant, base_opacity, colours[0], colours[1], colours[2]], axis=0)

def render_tile(features, live_count, tile_number, height):
    entries = features.shape[1]
    pixel = jnp.arange(TILE_SIDE * TILE_SIDE, dtype=jnp.int32)
    tile_col = tile_number % TW
    tile_row = tile_number // TW
    pixel_x = (TILE_SIDE * tile_col + pixel % TILE_SIDE).astype(jnp.float32) + 0.5 - 0.5 * TILE_SIDE * TW
    pixel_y = (TILE_SIDE * tile_row + pixel // TILE_SIDE).astype(jnp.float32) + 0.5 - 0.5 * height
    delta_x = pixel_x[:, None] - features[0][None, :]
    delta_y = pixel_y[:, None] - features[1][None, :]
    power = -0.5 * (features[2][None, :] * delta_x * delta_x + features[4][None, :] * delta_y * delta_y) - features[3][None, :] * delta_x * delta_y
    live = jnp.arange(entries, dtype=jnp.int32) < live_count
    alpha = jnp.where(live[None, :], features[5][None, :] * jnp.exp(power), jnp.float32(0.0))
    log_keep = jnp.log1p(-alpha)
    log_before = jnp.cumsum(log_keep, axis=1) - log_keep
    weights = alpha * jnp.exp(log_before)
    return jnp.einsum('ce,pe->cp', features[6:9], weights, precision=lax.Precision.HIGHEST)

def reference(means, log_scales, quat_w, quat_v, opacity, sh_coeffs, cameras, requests, lists, counts, image_cot):
    params = jnp.concatenate([means, log_scales, quat_w, quat_v, opacity, sh_coeffs], axis=0)
    owners = jnp.arange(N_IMG * N_TILE, dtype=jnp.int32).reshape(N_IMG, N_TILE)
    global_ids = (owners[None, None, :, :, None] * NG_DEV + requests).reshape(N_IMG, N_TILE, SLOTS)
    tile_owner = jnp.arange(TILES, dtype=jnp.int32) // TILES_DEV
    image_index = jnp.arange(N_IMG, dtype=jnp.int32)
    tile_ids = global_ids[image_index[:, None, None], tile_owner[None, :, None], lists]
    height = TILE_SIDE * TILES / TW
    numbers = jnp.tile(jnp.arange(TILES, dtype=jnp.int32), N_IMG)
    flat_counts = counts.reshape(-1)

    def render_packed(packed):
        return render_tile(packed[0], packed[1], packed[2], height)

    def forward(all_params, all_cameras):
        gathered = all_params[:, tile_ids]
        features = jax.vmap(project, in_axes=(1, 0), out_axes=1)(gathered, all_cameras)
        flat = features.transpose(1, 2, 0, 3).reshape(N_IMG * TILES, 9, LIST)
        images = lax.map(jax.checkpoint(render_packed), (flat, flat_counts, numbers))
        return images.reshape(N_IMG, TILES, 3, PIX).transpose(0, 2, 1, 3)
    rendered, pullback = jax.vjp(forward, params, cameras)
    param_grad, camera_grad = pullback(image_cot)
    return (rendered, param_grad, camera_grad)
```

```python
import jax
import jax.numpy as jnp
from jax import lax
from jax.experimental import pallas as pl
from jax.experimental.pallas import tpu as pltpu
from jax.sharding import PartitionSpec as P

TILE_SIDE = 16
TW = 16
ALL = ("img", "tile")
N_IMG = 8
N_TILE = 32
CAP = 16
OWNED = 2048
LIST = 256
TILES_HERE = 8
PIX = 256
LANES = 128
N_FEAT = 24
N_USED = 9
N_GRAD = 9
FEAT_ROWS = 3
GRAD_ROWS = 2

sh_first = 0.28209479177387814
sh_second = 0.4886025119029199
sh_third = (
    1.0925484305920792,
    -1.0925484305920792,
    0.31539156525252005,
    -1.0925484305920792,
    0.5462742152960396,
)
sh_fourth = (
    -0.5900435899266435,
    2.890611442640554,
    -0.4570457994644658,
    0.3731763325901154,
    -0.4570457994644658,
    1.445305721320277,
    -0.5900435899266435,
)
dilation = 0.3
LOG2E = 1.4426950408889634
f32 = jnp.float32
bf16 = jnp.bfloat16


def harmonics_of(polar, azimuth):
    sin_p, cos_p = jnp.sin(polar), jnp.cos(polar)
    x = sin_p * jnp.cos(azimuth)
    y = sin_p * jnp.sin(azimuth)
    z = cos_p
    xx, yy, zz = x * x, y * y, z * z
    return jnp.stack(
        [
            sh_first + 0.0 * x,
            -sh_second * y,
            sh_second * z,
            -sh_second * x,
            sh_third[0] * x * y,
            sh_third[1] * y * z,
            sh_third[2] * (2.0 * zz - xx - yy),
            sh_third[3] * x * z,
            sh_third[4] * (xx - yy),
            sh_fourth[0] * y * (3.0 * xx - yy),
            sh_fourth[1] * x * y * z,
            sh_fourth[2] * y * (4.0 * zz - xx - yy),
            sh_fourth[3] * z * (2.0 * zz - 3.0 * xx - 3.0 * yy),
            sh_fourth[4] * x * (4.0 * zz - xx - yy),
            sh_fourth[5] * z * (xx - yy),
            sh_fourth[6] * x * (xx - 3.0 * yy),
        ],
        axis=-1,
    )


def camera_table(cameras):
    polar, azimuth = cameras[:, 8], cameras[:, 9]
    one = jnp.ones_like(polar)
    zero = jnp.zeros_like(polar)
    values, d_polar = jax.jvp(harmonics_of, (polar, azimuth), (one, zero))
    d_azimuth = jax.jvp(harmonics_of, (polar, azimuth), (zero, one))[1]
    return jnp.concatenate([cameras, values, d_polar, d_azimuth], axis=1)


def shape_matrix(log_scales, quat):
    w, x, y, z = quat
    norm = jnp.sqrt(w * w + x * x + y * y + z * z)
    w, x, y, z = w / norm, x / norm, y / norm, z / norm
    rotation = (
        (1.0 - 2.0 * (y * y + z * z), 2.0 * (x * y - w * z), 2.0 * (x * z + w * y)),
        (2.0 * (x * y + w * z), 1.0 - 2.0 * (x * x + z * z), 2.0 * (y * z - w * x)),
        (2.0 * (x * z - w * y), 2.0 * (y * z + w * x), 1.0 - 2.0 * (x * x + y * y)),
    )
    stretch = [jnp.exp(v) for v in log_scales]
    return [[rotation[r][c] * stretch[c] for c in range(3)] for r in range(3)]


def swap_groups(vregs):
    vregs = list(vregs)
    group = lax.broadcasted_iota(jnp.int32, (8, LANES), 1) // CAP
    for bit in (1, 2, 4):
        low = (group & bit) == 0
        for i in range(8):
            if i & bit:
                continue
            a, b = vregs[i], vregs[i + bit]
            vregs[i] = jnp.where(low, a, pltpu.roll(b, CAP * bit, 1))
            vregs[i + bit] = jnp.where(low, pltpu.roll(a, LANES - CAP * bit, 1), b)
    return vregs


def lane_take(table, lanes):
    return jnp.take_along_axis(table, lanes, axis=1, mode="promise_in_bounds")


def halves(value):
    high = value.astype(bf16)
    return high, (value - high.astype(f32)).astype(bf16)


def dot(a, b):
    return lax.dot_general(a, b, (((1,), (0,)), ((), ())), preferred_element_type=f32)


def dot_t(a, b):
    return lax.dot_general(a, b, (((1,), (1,)), ((), ())), preferred_element_type=f32)


PROJECT_CHUNK = 256


def project_kernel(means, log_scales, quat_w, quat_v, opacity, sh, cam, out):
    column = [jnp.broadcast_to(cam[:, m : m + 1], (N_IMG, PROJECT_CHUNK)) for m in range(8)]

    def chunk(h, carry):
        at = pl.ds(pl.multiple_of(h * PROJECT_CHUNK, PROJECT_CHUNK), PROJECT_CHUNK)
        mean = [means[c : c + 1, at] for c in range(3)]
        quat = [quat_w[0:1, at]] + [quat_v[c : c + 1, at] for c in range(3)]
        m = shape_matrix([log_scales[c : c + 1, at] for c in range(3)], quat)
        for row in range(2):
            a = column[3 * row : 3 * row + 3]
            out[row, :, at] = a[0] * mean[0] + a[1] * mean[1] + a[2] * mean[2] + column[6 + row]
        p = [
            [
                sum(column[3 * row + r] * m[r][c] for r in range(3))
                for c in range(3)
            ]
            for row in range(2)
        ]
        s00 = p[0][0] * p[0][0] + p[0][1] * p[0][1] + p[0][2] * p[0][2] + dilation
        s01 = p[0][0] * p[1][0] + p[0][1] * p[1][1] + p[0][2] * p[1][2]
        s11 = p[1][0] * p[1][0] + p[1][1] * p[1][1] + p[1][2] * p[1][2] + dilation
        det = s00 * s11 - s01 * s01
        out[2, :, at] = s11 / det
        out[3, :, at] = -s01 / det
        out[4, :, at] = s00 / det
        base = 1.0 / (1.0 + jnp.exp(-opacity[0:1, at]))
        out[5, :, at] = jnp.broadcast_to(base, (N_IMG, PROJECT_CHUNK))
        for c in range(3):
            out[9 + c, :, at] = jnp.broadcast_to(mean[c], (N_IMG, PROJECT_CHUNK))
            for row in range(2):
                out[12 + 3 * row + c, :, at] = (
                    m[c][0] * p[row][0] + m[c][1] * p[row][1] + m[c][2] * p[row][2]
                )
        for base_row, first, start in ((6, 10, 0.5), (18, 26, 0.0), (21, 42, 0.0)):
            total = [jnp.full((N_IMG, PROJECT_CHUNK), start, f32) for _ in range(3)]
            for b in range(16):
                y = jnp.broadcast_to(cam[:, first + b : first + b + 1], (N_IMG, PROJECT_CHUNK))
                for k in range(3):
                    total[k] = total[k] + y * sh[16 * k + b : 16 * k + b + 1, at]
            for k in range(3):
                out[base_row + k, :, at] = total[k]
        return carry

    lax.fori_loop(0, OWNED // PROJECT_CHUNK, chunk, 0)


def asked_lanes(asked):
    group = lax.broadcasted_iota(jnp.int32, (8, LANES), 1) // CAP
    result = []
    for q in range(4):
        total = asked[pl.ds(8 * q, 8, stride=N_TILE), :]
        for k in range(1, 8):
            piece = asked[pl.ds(8 * q + k, 8, stride=N_TILE), :]
            total = jnp.where(group == k, pltpu.roll(piece, CAP * k, 1), total)
        result.append(total)
    return result


def pick_kernel(feats, asked, out):
    index = asked_lanes(asked)
    low = [v & (LANES - 1) for v in index]
    high = [v >> 7 for v in index]
    for g in range(FEAT_ROWS):
        picked = [[None] * 8 for _ in range(4)]
        for f in range(8):
            for q in range(4):
                value = jnp.zeros((8, LANES), f32)
                for h in range(OWNED // LANES):
                    table = feats[8 * g + f, :, h * LANES : (h + 1) * LANES]
                    value = jnp.where(high[q] == h, lane_take(table, low[q]), value)
                picked[q][f] = value
        for q in range(4):
            rows = swap_groups(picked[q])
            for k in range(8):
                out[pl.ds(FEAT_ROWS * (8 * q + k) + g, 8, stride=FEAT_ROWS * N_TILE), :] = rows[k]


def render_kernel(
    meta,
    rows,
    lists,
    cot,
    image,
    out,
    tab,
    feat,
    grads,
    slot,
    upper,
    lower,
    al_s,
    lk_s,
    lb_s,
    s_s,
    w_s,
    sw_s,
    g_s,
):
    tile_base = meta[TILES_HERE] * TILES_HERE
    for g in range(FEAT_ROWS):
        for q in range(4):
            pieces = [
                rows[pl.ds(FEAT_ROWS * (8 * q + k) + g, 8, stride=FEAT_ROWS * N_TILE), :]
                for k in range(8)
            ]
            pieces = swap_groups(pieces)
            for f in range(8):
                tab[8 * g + f, 8 * q : 8 * q + 8, :] = pieces[f]
    entry_lane = [lists[:, h * LANES : (h + 1) * LANES] & (LANES - 1) for h in range(2)]
    entry_chunk = []
    for h in range(2):
        s = lists[:, h * LANES : (h + 1) * LANES]
        entry_chunk.append(((s >> 7) & 3) * 8 + (s >> 9))

    def gather(ch, carry):
        new = []
        for f in range(N_USED):
            table = jnp.broadcast_to(tab[f, pl.ds(ch, 1), :], (8, LANES))
            for h in range(2):
                new.append(
                    jnp.where(entry_chunk[h] == ch, lane_take(table, entry_lane[h]), carry[2 * f + h])
                )
        return tuple(new)

    zero = jnp.zeros((8, LANES), f32)
    found = lax.fori_loop(0, 32, gather, tuple([zero] * (2 * N_USED)))
    for f in range(N_USED):
        for h in range(2):
            feat[f, :, h * LANES : (h + 1) * LANES] = found[2 * f + h]
    ri = lax.broadcasted_iota(jnp.int32, (LIST, LIST), 0)
    ci = lax.broadcasted_iota(jnp.int32, (LIST, LIST), 1)
    up = (ri < ci).astype(f32).astype(bf16)
    lo = (ri > ci).astype(f32).astype(bf16)
    for part in range(2):
        upper[part * LIST : (part + 1) * LIST, :] = up
        lower[part * LIST : (part + 1) * LIST, :] = lo
    slot[...] = jnp.zeros_like(slot)
    lane = lax.broadcasted_iota(jnp.int32, (1, LIST), 1)
    px = lax.broadcasted_iota(jnp.int32, (TILE_SIDE, LIST), 0).astype(f32) - 7.5
    pix = lax.broadcasted_iota(jnp.int32, (8, PIX), 1)
    which = lax.broadcasted_iota(jnp.int32, (8, PIX), 0)
    pxr = (pix % TILE_SIDE).astype(f32) - 7.5
    pyr = (pix // TILE_SIDE).astype(f32) - 7.5
    basis = jnp.where(
        which == 0,
        1.0,
        jnp.where(
            which == 1,
            pxr,
            jnp.where(
                which == 2,
                pyr,
                jnp.where(which == 3, pxr * pxr, jnp.where(which == 4, pxr * pyr, pyr * pyr)),
            ),
        ),
    ).astype(bf16)
    basis = jnp.concatenate([basis, basis], axis=1)
    ch_iota = lax.broadcasted_iota(jnp.int32, (32, LIST), 0)
    lane_iota = lax.broadcasted_iota(jnp.int32, (LANES, LIST), 0)

    def tile(j, carry):
        number = tile_base + j
        centre_x = (TILE_SIDE * (number % TW)).astype(f32) + (0.5 * TILE_SIDE - 0.5 * TILE_SIDE * TW)
        centre_y = (TILE_SIDE * (number // TW)).astype(f32) + (0.5 * TILE_SIDE - 0.5 * TILE_SIDE * TW)
        at = pl.ds(j, 1)
        ux = feat[0, at, :] - centre_x
        uy = feat[1, at, :] - centre_y
        ca, cb, cc = feat[2, at, :], feat[3, at, :], feat[4, at, :]
        op = jnp.where(lane < meta[j], feat[5, at, :], 0.0)
        op8 = jnp.broadcast_to(op, (TILE_SIDE, LIST))
        uy8 = jnp.broadcast_to(uy, (TILE_SIDE, LIST))
        cc8 = jnp.broadcast_to(cc * (-0.5 * LOG2E), (TILE_SIDE, LIST))
        dx = px - ux
        na = (ca * (-0.5 * LOG2E)) * dx * dx
        nb = (cb * (-LOG2E)) * dx
        colours = jnp.concatenate([feat[6 + k, at, :] for k in range(3)], axis=0)
        cots = jnp.concatenate([cot[k, at, :] for k in range(3)], axis=0)
        col_h, col_l = halves(colours)
        cot_h, cot_l = halves(cots)
        col_h, col_l, cot_h, cot_l = [v.astype(f32) for v in (col_h, col_l, cot_h, cot_l)]
        pad = jnp.zeros((4, LIST), f32)
        cot_k = jnp.concatenate([cot_h, cot_h, cot_l, cot_l, pad], axis=0)
        col_k = jnp.concatenate([col_h, col_l, col_h, col_l, pad], axis=0).astype(bf16)
        s_s[...] = dot(jnp.transpose(cot_k).astype(bf16), col_k)
        for py in range(TILE_SIDE):
            r = slice(TILE_SIDE * py, TILE_SIDE * (py + 1))
            dy = (py - 7.5) - uy8
            alpha = op8 * jnp.exp2(na + cc8 * dy * dy + nb * dy)
            al_s[r, :] = alpha
            hi, low = halves(jnp.log2(1.0 - alpha))
            lk_s[r, 0:LIST] = hi
            lk_s[r, LIST : 2 * LIST] = low
        lb_s[...] = dot(lk_s[...], upper[...])
        for py in range(TILE_SIDE):
            r = slice(TILE_SIDE * py, TILE_SIDE * (py + 1))
            w = al_s[r, :] * jnp.exp2(lb_s[r, :])
            hi, low = halves(w)
            w_s[r, :] = hi
            w_s[PIX + TILE_SIDE * py : PIX + TILE_SIDE * (py + 1), :] = low
            sw = s_s[r, :] * w
            s_s[r, :] = sw
            hi, low = halves(sw)
            sw_s[r, 0:LIST] = hi
            sw_s[r, LIST : 2 * LIST] = low
        lb_s[...] = dot(sw_s[...], lower[...])
        for py in range(TILE_SIDE):
            r = slice(TILE_SIDE * py, TILE_SIDE * (py + 1))
            alpha = al_s[r, :]
            g = s_s[r, :] - lb_s[r, :] * (alpha / (1.0 - alpha))
            hi, low = halves(g)
            g_s[r, :] = hi
            g_s[PIX + TILE_SIDE * py : PIX + TILE_SIDE * (py + 1), :] = low
        pad2 = jnp.zeros((2, LIST), f32)
        col_rows = jnp.concatenate([col_h, col_l, pad2], axis=0).astype(bf16)
        shown = dot_t(col_rows, w_s[0:PIX, :]) + dot_t(col_rows, w_s[PIX : 2 * PIX, :])
        for k in range(3):
            image[k, at, :] = shown[k : k + 1, :] + shown[3 + k : 4 + k, :]
        cot_rows = jnp.concatenate([cot_h, cot_l, pad2], axis=0).astype(bf16)
        gcol = dot(jnp.concatenate([cot_rows, cot_rows], axis=1), w_s[...])
        mom = dot(basis, g_s[...])
        m0, mx, my = mom[0:1, :], mom[1:2, :], mom[2:3, :]
        mxx, mxy, myy = mom[3:4, :], mom[4:5, :], mom[5:6, :]
        grad = [
            m0,
            mx - ux * m0,
            my - uy * m0,
            mxx - 2.0 * ux * mx + ux * ux * m0,
            mxy - ux * my - uy * mx + ux * uy * m0,
            myy - 2.0 * uy * my + uy * uy * m0,
        ] + [gcol[k : k + 1, :] + gcol[3 + k : 4 + k, :] for k in range(3)]
        s = lists[at, :]
        chunk = ((s >> 7) & 3) * 8 + (s >> 9)
        chunk_hit = ch_iota == chunk
        lane_hit = (lane_iota == (s & (LANES - 1))).astype(f32).astype(bf16)
        for f in range(N_GRAD):
            hi, low = halves(jnp.where(chunk_hit, grad[f], 0.0))
            grads[32 * f : 32 * (f + 1), 0:LIST] = hi
            grads[32 * f : 32 * (f + 1), LIST : 2 * LIST] = low
        slot[...] += dot_t(grads[...], jnp.concatenate([lane_hit, lane_hit], axis=1))
        return carry

    lax.fori_loop(0, TILES_HERE, tile, 0)

    terms = [jnp.zeros((8, LANES), f32) for _ in range(10)]
    for q in range(4):
        r = slice(8 * q, 8 * q + 8)
        ca, cb, cc = tab[2, r, :], tab[3, r, :], tab[4, r, :]
        gr = [slot[32 * f + 8 * q : 32 * f + 8 * q + 8, :] for f in range(N_GRAD)]
        du = (ca * gr[1] + cb * gr[2], cb * gr[1] + cc * gr[2])
        h00, h01, h11 = conic_pull(ca, cb, cc, gr[3], gr[4], gr[5])
        for c in range(3):
            mean, n0, n1 = tab[9 + c, r, :], tab[12 + c, r, :], tab[15 + c, r, :]
            terms[c] += du[0] * mean + 2.0 * (h00 * n0 + h01 * n1)
            terms[3 + c] += du[1] * mean + 2.0 * (h01 * n0 + h11 * n1)
            terms[8] += gr[6 + c] * tab[18 + c, r, :]
            terms[9] += gr[6 + c] * tab[21 + c, r, :]
        terms[6] += du[0]
        terms[7] += du[1]
    lanes = lax.broadcasted_iota(jnp.int32, (8, LANES), 1)
    share = jnp.zeros((8, LANES), f32)
    for m in range(10):
        total = jnp.sum(jnp.sum(terms[m], axis=0, keepdims=True), axis=1, keepdims=True)
        share = jnp.where(lanes == CAP + m, jnp.broadcast_to(total, (8, LANES)), share)
    for q in range(4):
        pieces = swap_groups([slot[32 * f + 8 * q : 32 * f + 8 * q + 8, :] for f in range(8)])
        last = slot[32 * 8 + 8 * q : 32 * 8 + 8 * q + 8, :]
        for k in range(8):
            first_row = GRAD_ROWS * (8 * q + k)
            stride = GRAD_ROWS * N_TILE
            out[pl.ds(first_row, 8, stride=stride), :] = pieces[k]
            moved = last if k == 0 else pltpu.roll(last, LANES - CAP * k, 1)
            out[pl.ds(first_row + 1, 8, stride=stride), :] = jnp.where(lanes < CAP, moved, share)


def conic_pull(ca, cb, cc, qxx, qxy, qyy):
    t00, t01 = ca * qxx + cb * qxy, ca * qxy + cb * qyy
    t10, t11 = cb * qxx + cc * qxy, cb * qxy + cc * qyy
    return 0.5 * (t00 * ca + t01 * cb), 0.5 * (t00 * cb + t01 * cc), 0.5 * (t10 * cb + t11 * cc)


PULL_CHUNK = 128


def pull_kernel(
    returned, asked, feats, log_scales, quat_w, quat_v, cam, out, cam_out, row_s, idx_s, lhs_s, sum_s, y_s, gc_s
):
    index = asked_lanes(asked)
    for q in range(4):
        idx_s[:, q * LANES : (q + 1) * LANES] = index[q]
    stride = GRAD_ROWS * N_TILE
    group = lax.broadcasted_iota(jnp.int32, (8, LANES), 1) // CAP
    camera = jnp.zeros((8, LANES), f32)
    for q in range(4):
        pieces = [returned[pl.ds(GRAD_ROWS * (8 * q + k), 8, stride=stride), :] for k in range(8)]
        pieces = swap_groups(pieces)
        for f in range(8):
            row_s[f, :, q * LANES : (q + 1) * LANES] = pieces[f]
        last = None
        for k in range(8):
            piece = returned[pl.ds(GRAD_ROWS * (8 * q + k) + 1, 8, stride=stride), :]
            camera = camera + piece
            last = piece if k == 0 else jnp.where(group == k, pltpu.roll(piece, CAP * k, 1), last)
        row_s[8, :, q * LANES : (q + 1) * LANES] = last
    cam_out[...] = pltpu.roll(camera, LANES - CAP, 1)[:, 0:10]

    slots = N_TILE * CAP
    high_iota = lax.broadcasted_iota(jnp.int32, (16, slots), 0)
    lane_iota = lax.broadcasted_iota(jnp.int32, (LANES, slots), 0)

    def image(i, carry):
        at = pl.ds(i, 1)
        s = idx_s[at, :]
        high_hit = high_iota == (s >> 7)
        lane_hit = (lane_iota == (s & (LANES - 1))).astype(f32).astype(bf16)
        for f in range(N_GRAD):
            hi, low = halves(jnp.where(high_hit, row_s[f, at, :], 0.0))
            lhs_s[16 * f : 16 * (f + 1), 0:slots] = hi
            lhs_s[16 * f : 16 * (f + 1), slots : 2 * slots] = low
        sum_s[pl.ds(pl.multiple_of(i * (16 * N_GRAD), 16), 16 * N_GRAD), :] = dot_t(
            lhs_s[...], jnp.concatenate([lane_hit, lane_hit], axis=1)
        )
        return carry

    lax.fori_loop(0, N_IMG, image, 0)

    column = [jnp.broadcast_to(cam[:, m : m + 1], (N_IMG, PULL_CHUNK)) for m in range(6)]

    def chunk(h, carry):
        at = pl.ds(pl.multiple_of(h * PULL_CHUNK, PULL_CHUNK), PULL_CHUNK)
        gr = [sum_s[pl.ds(16 * f + h, 8, stride=16 * N_GRAD), :] for f in range(N_GRAD)]
        ca, cb, cc = feats[2, :, at], feats[3, :, at], feats[4, :, at]
        du = (ca * gr[1] + cb * gr[2], cb * gr[1] + cc * gr[2])
        h00, h01, h11 = conic_pull(ca, cb, cc, gr[3], gr[4], gr[5])
        a0, a1 = column[0:3], column[3:6]

        def over_images(v):
            return jnp.sum(v, axis=0, keepdims=True)

        for c in range(3):
            out[c : c + 1, at] = over_images(a0[c] * du[0] + a1[c] * du[1])
        t0 = [h00 * a0[c] + h01 * a1[c] for c in range(3)]
        t1 = [h01 * a0[c] + h11 * a1[c] for c in range(3)]
        v = [[None] * 3 for _ in range(3)]
        for c in range(3):
            for d in range(c, 3):
                v[c][d] = v[d][c] = over_images(t0[c] * a0[d] + t1[c] * a1[d])
        ls = [log_scales[c : c + 1, at] for c in range(3)]
        quat = [quat_w[0:1, at]] + [quat_v[c : c + 1, at] for c in range(3)]
        m, pull = jax.vjp(shape_matrix, ls, quat)
        dm = [[2.0 * sum(v[r][d] * m[d][c] for d in range(3)) for c in range(3)] for r in range(3)]
        dls, dquat = pull(dm)
        for c in range(3):
            out[3 + c : 4 + c, at] = dls[c]
        for c in range(4):
            out[6 + c : 7 + c, at] = dquat[c]
        base = feats[5, 0:1, at]
        out[10:11, at] = over_images(gr[0]) * (1.0 - base)
        for k in range(3):
            gc_s[8 * k : 8 * k + 8, at] = gr[6 + k]
        return carry

    lax.fori_loop(0, OWNED // PULL_CHUNK, chunk, 0)

    y_h, y_l = halves(jnp.transpose(cam[:, 10:26]))
    y_all = jnp.concatenate([y_h.astype(f32), y_h.astype(f32), y_l.astype(f32), y_l.astype(f32)], axis=1).astype(bf16)
    for k in range(3):
        g_h, g_l = halves(gc_s[8 * k : 8 * k + 8, :])
        g_all = jnp.concatenate([g_h.astype(f32), g_l.astype(f32), g_h.astype(f32), g_l.astype(f32)], axis=0).astype(bf16)
        out[11 + 16 * k : 27 + 16 * k, :] = dot(y_all, g_all)


def whole(memory=pltpu.VMEM):
    return pl.BlockSpec(memory_space=memory)


def call(kernel, name, out_shape, scratch, n_in, smem=0):
    return pl.pallas_call(
        kernel,
        name=name,
        out_shape=out_shape,
        in_specs=[whole(pltpu.SMEM)] * smem + [whole()] * (n_in - smem),
        out_specs=jax.tree.map(lambda _: whole(), out_shape),
        scratch_shapes=scratch,
        compiler_params=pltpu.CompilerParams(vmem_limit_bytes=32 << 20),
    )


def exchange(array):
    return lax.all_to_all(array, ALL, split_axis=0, concat_axis=0, tiled=True)


def exchange_rows(array, rows):
    shape = array.shape
    return exchange(array.reshape(-1, 1, rows * LANES)).reshape(shape)


def local(
    means, log_scales, quat_w, quat_v, opacity, sh_coeffs, cameras, requests, lists, counts, image_cot
):
    devices = N_IMG * N_TILE
    wanted = jnp.pad(requests.reshape(devices, CAP), ((0, 0), (0, LANES - CAP)))
    asked = exchange_rows(wanted, 1)
    cam = camera_table(cameras)
    feats = call(
        project_kernel, "project", jax.ShapeDtypeStruct((N_FEAT, N_IMG, OWNED), f32), [], 7
    )(means, log_scales, quat_w, quat_v, opacity, sh_coeffs, cam)
    packed = call(
        pick_kernel, "pick", jax.ShapeDtypeStruct((FEAT_ROWS * devices, LANES), f32), [], 2
    )(feats, asked)
    rows = exchange_rows(packed, FEAT_ROWS)
    meta = jnp.concatenate([counts[0], lax.axis_index("tile").astype(jnp.int32)[None]])
    rendered, slot_grads = call(
        render_kernel,
        "render",
        (
            jax.ShapeDtypeStruct((3, TILES_HERE, PIX), f32),
            jax.ShapeDtypeStruct((GRAD_ROWS * devices, LANES), f32),
        ),
        [
            pltpu.VMEM((N_FEAT, 32, LANES), f32),
            pltpu.VMEM((N_USED, 8, LIST), f32),
            pltpu.VMEM((32 * N_GRAD, 2 * LIST), bf16),
            pltpu.VMEM((32 * N_GRAD, LANES), f32),
            pltpu.VMEM((2 * LIST, LIST), bf16),
            pltpu.VMEM((2 * LIST, LIST), bf16),
            pltpu.VMEM((PIX, LIST), f32),
            pltpu.VMEM((PIX, 2 * LIST), bf16),
            pltpu.VMEM((PIX, LIST), f32),
            pltpu.VMEM((PIX, LIST), f32),
            pltpu.VMEM((2 * PIX, LIST), bf16),
            pltpu.VMEM((PIX, 2 * LIST), bf16),
            pltpu.VMEM((2 * PIX, LIST), bf16),
        ],
        4,
        smem=1,
    )(meta, rows, lists[0], image_cot[0])
    returned = exchange_rows(slot_grads, GRAD_ROWS)
    param_grad, camera_grad = call(
        pull_kernel,
        "pull",
        (
            jax.ShapeDtypeStruct((59, OWNED), f32),
            jax.ShapeDtypeStruct((N_IMG, 10), f32),
        ),
        [
            pltpu.VMEM((N_GRAD, N_IMG, N_TILE * CAP), f32),
            pltpu.VMEM((N_IMG, N_TILE * CAP), jnp.int32),
            pltpu.VMEM((16 * N_GRAD, 2 * N_TILE * CAP), bf16),
            pltpu.VMEM((N_IMG * 16 * N_GRAD, LANES), f32),
            pltpu.VMEM((16, LANES), f32),
            pltpu.VMEM((24, OWNED), f32),
        ],
        7,
    )(returned, asked, feats, log_scales, quat_w, quat_v, cam)
    return (rendered[None], param_grad, camera_grad)


def solution(mesh):
    own = P(None, ALL)
    return jax.shard_map(
        local,
        mesh=mesh,
        in_specs=(
            own,
            own,
            own,
            own,
            own,
            own,
            P(),
            P("img", "tile", None, None, None),
            P("img", "tile", None),
            P("img", "tile"),
            P("img", None, "tile", None),
        ),
        out_specs=(P("img", None, "tile", None), own, P()),
        check_vma=False,
    )
```

```python
import jax
import jax.numpy as jnp
from jax import lax
from jax.experimental import pallas as pl
from jax.experimental.pallas import tpu as pltpu
from jax.sharding import PartitionSpec as P

TILE_SIDE = 16
TW = 16
ALL = ("img", "tile")
ORDER = ("tile", "img")
N_IMG = 8
N_TILE = 32
CAP = 16
OWNED = 2048
LIST = 256
TILES_HERE = 8
PIX = 256
LANES = 128
N_FEAT = 24
N_USED = 9
N_GRAD = 9
FEAT_ROWS = 3
GRAD_ROWS = 2

sh_first = 0.28209479177387814
sh_second = 0.4886025119029199
sh_third = (
    1.0925484305920792,
    -1.0925484305920792,
    0.31539156525252005,
    -1.0925484305920792,
    0.5462742152960396,
)
sh_fourth = (
    -0.5900435899266435,
    2.890611442640554,
    -0.4570457994644658,
    0.3731763325901154,
    -0.4570457994644658,
    1.445305721320277,
    -0.5900435899266435,
)
dilation = 0.3
LOG2E = 1.4426950408889634
f32 = jnp.float32
bf16 = jnp.bfloat16


def harmonics_of(polar, azimuth):
    sin_p, cos_p = jnp.sin(polar), jnp.cos(polar)
    x = sin_p * jnp.cos(azimuth)
    y = sin_p * jnp.sin(azimuth)
    z = cos_p
    xx, yy, zz = x * x, y * y, z * z
    return [
        sh_first + 0.0 * x,
        -sh_second * y,
        sh_second * z,
        -sh_second * x,
        sh_third[0] * x * y,
        sh_third[1] * y * z,
        sh_third[2] * (2.0 * zz - xx - yy),
        sh_third[3] * x * z,
        sh_third[4] * (xx - yy),
        sh_fourth[0] * y * (3.0 * xx - yy),
        sh_fourth[1] * x * y * z,
        sh_fourth[2] * y * (4.0 * zz - xx - yy),
        sh_fourth[3] * z * (2.0 * zz - 3.0 * xx - 3.0 * yy),
        sh_fourth[4] * x * (4.0 * zz - xx - yy),
        sh_fourth[5] * z * (xx - yy),
        sh_fourth[6] * x * (xx - 3.0 * yy),
    ]


def shape_matrix(log_scales, quat):
    w, x, y, z = quat
    norm = jnp.sqrt(w * w + x * x + y * y + z * z)
    w, x, y, z = w / norm, x / norm, y / norm, z / norm
    rotation = (
        (1.0 - 2.0 * (y * y + z * z), 2.0 * (x * y - w * z), 2.0 * (x * z + w * y)),
        (2.0 * (x * y + w * z), 1.0 - 2.0 * (x * x + z * z), 2.0 * (y * z - w * x)),
        (2.0 * (x * z - w * y), 2.0 * (y * z + w * x), 1.0 - 2.0 * (x * x + y * y)),
    )
    stretch = [jnp.exp(v) for v in log_scales]
    return [[rotation[r][c] * stretch[c] for c in range(3)] for r in range(3)]


def swap_groups(vregs):
    vregs = list(vregs)
    group = lax.broadcasted_iota(jnp.int32, (8, LANES), 1) // CAP
    for bit in (1, 2, 4):
        low = (group & bit) == 0
        for i in range(8):
            if i & bit:
                continue
            a, b = vregs[i], vregs[i + bit]
            vregs[i] = jnp.where(low, a, pltpu.roll(b, CAP * bit, 1))
            vregs[i + bit] = jnp.where(low, pltpu.roll(a, LANES - CAP * bit, 1), b)
    return vregs


def lane_take(table, lanes):
    return jnp.take_along_axis(table, lanes, axis=1, mode="promise_in_bounds")


def halves(value):
    high = value.astype(bf16)
    return high, (value - high.astype(f32)).astype(bf16)


def dot(a, b):
    return lax.dot_general(a, b, (((1,), (0,)), ((), ())), preferred_element_type=f32)


def dot_t(a, b):
    return lax.dot_general(a, b, (((1,), (1,)), ((), ())), preferred_element_type=f32)


PROJECT_CHUNK = 256


def ask_kernel(wanted, out):
    padded = jnp.concatenate([wanted[...], jnp.zeros((LANES, LANES - N_TILE), jnp.int32)], axis=1)
    turned = jnp.transpose(padded)
    for b in range(N_TILE):
        out[8 * b : 8 * b + 8, :] = jnp.broadcast_to(turned[b : b + 1, :], (8, LANES))


def asked_lanes(asked, my_img):
    group = lax.broadcasted_iota(jnp.int32, (8, LANES), 1) // CAP
    base = LANES - CAP * my_img
    result = []
    for q in range(4):
        total = None
        for k in range(8):
            piece = pltpu.roll(asked[8 * (8 * q + k) : 8 * (8 * q + k) + 8, :], (base + CAP * k) & (LANES - 1), 1)
            total = piece if k == 0 else jnp.where(group == k, piece, total)
        result.append(total)
    return result


def project(means, log_scales, quat_w, quat_v, opacity, sh, cam, out, harm):
    column = [jnp.broadcast_to(cam[:, m : m + 1], (N_IMG, PROJECT_CHUNK)) for m in range(8)]

    def chunk(h, carry):
        at = pl.ds(pl.multiple_of(h * PROJECT_CHUNK, PROJECT_CHUNK), PROJECT_CHUNK)
        mean = [means[c : c + 1, at] for c in range(3)]
        quat = [quat_w[0:1, at]] + [quat_v[c : c + 1, at] for c in range(3)]
        m = shape_matrix([log_scales[c : c + 1, at] for c in range(3)], quat)
        for row in range(2):
            a = column[3 * row : 3 * row + 3]
            out[row, :, at] = a[0] * mean[0] + a[1] * mean[1] + a[2] * mean[2] + column[6 + row]
        p = [
            [
                sum(column[3 * row + r] * m[r][c] for r in range(3))
                for c in range(3)
            ]
            for row in range(2)
        ]
        s00 = p[0][0] * p[0][0] + p[0][1] * p[0][1] + p[0][2] * p[0][2] + dilation
        s01 = p[0][0] * p[1][0] + p[0][1] * p[1][1] + p[0][2] * p[1][2]
        s11 = p[1][0] * p[1][0] + p[1][1] * p[1][1] + p[1][2] * p[1][2] + dilation
        det = s00 * s11 - s01 * s01
        out[2, :, at] = s11 / det
        out[3, :, at] = -s01 / det
        out[4, :, at] = s00 / det
        base = 1.0 / (1.0 + jnp.exp(-opacity[0:1, at]))
        out[5, :, at] = jnp.broadcast_to(base, (N_IMG, PROJECT_CHUNK))
        for c in range(3):
            out[9 + c, :, at] = jnp.broadcast_to(mean[c], (N_IMG, PROJECT_CHUNK))
            for row in range(2):
                out[12 + 3 * row + c, :, at] = (
                    m[c][0] * p[row][0] + m[c][1] * p[row][1] + m[c][2] * p[row][2]
                )
        for base_row, first, start in ((6, 0, 0.5), (18, 16, 0.0), (21, 32, 0.0)):
            total = [jnp.full((N_IMG, PROJECT_CHUNK), start, f32) for _ in range(3)]
            for b in range(16):
                y = jnp.concatenate([harm[first + b]] * (PROJECT_CHUNK // LANES), axis=1)
                for k in range(3):
                    total[k] = total[k] + y * sh[16 * k + b : 16 * k + b + 1, at]
            for k in range(3):
                out[base_row + k, :, at] = total[k]
        return carry

    lax.fori_loop(0, OWNED // PROJECT_CHUNK, chunk, 0)


def pick_kernel(
    meta, asked, means, log_scales, quat_w, quat_v, opacity, sh, cam, out, conic, table, feats, harm
):
    polar = jnp.broadcast_to(cam[:, 8:9], (N_IMG, LANES))
    azimuth = jnp.broadcast_to(cam[:, 9:10], (N_IMG, LANES))
    one, zero = jnp.ones_like(polar), jnp.zeros_like(polar)
    values, d_polar = jax.jvp(harmonics_of, (polar, azimuth), (one, zero))
    d_azimuth = jax.jvp(harmonics_of, (polar, azimuth), (zero, one))[1]
    lanes = lax.broadcasted_iota(jnp.int32, (N_IMG, LANES), 1)
    packed = jnp.zeros((N_IMG, LANES), f32)
    for b in range(16):
        harm[b] = values[b]
        harm[16 + b] = d_polar[b]
        harm[32 + b] = d_azimuth[b]
        packed = jnp.where(lanes == b, values[b], packed)
    table[...] = packed
    project(means, log_scales, quat_w, quat_v, opacity, sh, cam, feats, harm)
    for f in range(4):
        conic[f] = feats[2 + f]
    index = asked_lanes(asked, meta[TILES_HERE + 1])
    low = [v & (LANES - 1) for v in index]
    high = [v >> 7 for v in index]
    for g in range(FEAT_ROWS):
        for q in range(4):
            picked = []
            for f in range(8):
                value = None
                for h in range(OWNED // LANES):
                    found = lane_take(feats[8 * g + f, :, h * LANES : (h + 1) * LANES], low[q])
                    value = found if h == 0 else jnp.where(high[q] == h, found, value)
                picked.append(value)
            rows = swap_groups(picked)
            for k in range(8):
                out[pl.ds(FEAT_ROWS * 8 * (8 * q + k) + g, 8, stride=FEAT_ROWS), :] = rows[k]


def render_kernel(
    meta,
    rows,
    lists,
    cot,
    image,
    out,
    tab,
    feat,
    grads,
    slot,
    upper,
    lower,
    al_s,
    lk_s,
    lb_s,
    s_s,
    w_s,
    sw_s,
):
    tile_base = meta[TILES_HERE] * TILES_HERE
    for g in range(FEAT_ROWS):
        for q in range(4):
            pieces = [
                rows[pl.ds(FEAT_ROWS * 8 * (8 * q + k) + g, 8, stride=FEAT_ROWS), :] for k in range(8)
            ]
            pieces = swap_groups(pieces)
            for f in range(8):
                tab[8 * g + f, 8 * q : 8 * q + 8, :] = pieces[f]
    entry_lane = [lists[:, h * LANES : (h + 1) * LANES] & (LANES - 1) for h in range(2)]
    entry_chunk = []
    for h in range(2):
        s = lists[:, h * LANES : (h + 1) * LANES]
        entry_chunk.append(((s >> 7) & 3) * 8 + (s >> 9))

    def gather(ch, carry):
        new = list(carry)
        for h in range(2):
            hit = entry_chunk[h] == ch
            for f in range(N_USED):
                row = jnp.broadcast_to(tab[f, pl.ds(ch, 1), :], (8, LANES))
                new[2 * f + h] = jnp.where(hit, lane_take(row, entry_lane[h]), carry[2 * f + h])
        return tuple(new)

    zero = jnp.zeros((8, LANES), f32)
    found = lax.fori_loop(0, 32, gather, tuple([zero] * (2 * N_USED)), unroll=8)
    for f in range(N_USED):
        for h in range(2):
            feat[f, :, h * LANES : (h + 1) * LANES] = found[2 * f + h]
    ri = lax.broadcasted_iota(jnp.int32, (LIST, LIST), 0)
    ci = lax.broadcasted_iota(jnp.int32, (LIST, LIST), 1)
    up = (ri < ci).astype(f32).astype(bf16)
    lo = (ri > ci).astype(f32).astype(bf16)
    for part in range(2):
        upper[part * LIST : (part + 1) * LIST, :] = up
        lower[part * LIST : (part + 1) * LIST, :] = lo
    slot[...] = jnp.zeros_like(slot)
    lane = lax.broadcasted_iota(jnp.int32, (1, LIST), 1)
    px = lax.broadcasted_iota(jnp.int32, (8, LIST), 0).astype(f32) - 7.5
    ch_iota = lax.broadcasted_iota(jnp.int32, (32, LIST), 0)
    lane_iota = lax.broadcasted_iota(jnp.int32, (LANES, LIST), 0)

    def row8(v):
        return jnp.broadcast_to(v, (8, LIST))

    def pair(pair_index, carry):
        tiles = [2 * pair_index, 2 * pair_index + 1]
        state = []
        for p in range(2):
            j = tiles[p]
            number = tile_base + j
            centre_x = (TILE_SIDE * (number % TW)).astype(f32) + (0.5 * TILE_SIDE - 0.5 * TILE_SIDE * TW)
            centre_y = (TILE_SIDE * (number // TW)).astype(f32) + (0.5 * TILE_SIDE - 0.5 * TILE_SIDE * TW)
            at = pl.ds(j, 1)
            ux = feat[0, at, :] - centre_x
            uy = row8(feat[1, at, :] - centre_y)
            ca, cb, cc = feat[2, at, :], feat[3, at, :], feat[4, at, :]
            op = row8(jnp.where(lane < meta[j], feat[5, at, :], 0.0))
            cc = row8(cc * (-0.5 * LOG2E))
            ux, na, nb = row8(ux), row8(ca * (-0.5 * LOG2E)), row8(cb * (-LOG2E))
            dx = [px - ux, px + (8.0 - ux)]
            na = [na * d * d for d in dx]
            nb = [nb * d for d in dx]
            colours = jnp.concatenate([feat[6 + k, at, :] for k in range(3)], axis=0)
            cots = jnp.concatenate([cot[k, at, :] for k in range(3)], axis=0)
            col_h, col_l, cot_h, cot_l = [v.astype(f32) for v in halves(colours) + halves(cots)]
            pad = jnp.zeros((4, LIST), f32)
            cot_k = jnp.concatenate([cot_h, cot_h, cot_l, cot_l, pad], axis=0)
            col_k = jnp.concatenate([col_h, col_l, col_h, col_l, pad], axis=0).astype(bf16)
            s_s[p] = dot(jnp.transpose(cot_k).astype(bf16), col_k)
            for py in range(TILE_SIDE):
                r = slice(TILE_SIDE * py, TILE_SIDE * (py + 1))
                dy = (py - 7.5) - uy
                cy = cc * dy * dy
                alpha = jnp.concatenate(
                    [op * jnp.exp2((na[h] + cy) + nb[h] * dy) for h in range(2)], axis=0
                )
                al_s[p, r, :] = alpha
                hi, low = halves(jnp.log2(1.0 - alpha))
                lk_s[p, r, 0:LIST] = hi
                lk_s[p, r, LIST : 2 * LIST] = low
            lb_s[p] = dot(lk_s[p], upper[...])
            state.append((at, uy, dx, col_h, col_l, cot_h, cot_l))
        for p in range(2):
            for py in range(TILE_SIDE):
                r = slice(TILE_SIDE * py, TILE_SIDE * (py + 1))
                w = al_s[p, r, :] * jnp.exp2(lb_s[p, r, :])
                hi, low = halves(w)
                w_s[p, r, :] = hi
                w_s[p, PIX + TILE_SIDE * py : PIX + TILE_SIDE * (py + 1), :] = low
                sw = s_s[p, r, :] * w
                s_s[p, r, :] = sw
                hi, low = halves(sw)
                sw_s[p, r, 0:LIST] = hi
                sw_s[p, r, LIST : 2 * LIST] = low
            lb_s[p] = dot(sw_s[p], lower[...])
        for p in range(2):
            at, uy, dx, col_h, col_l, cot_h, cot_l = state[p]
            pad2 = jnp.zeros((2, LIST), f32)
            col_rows = jnp.concatenate([col_h, col_l, pad2], axis=0).astype(bf16)
            shown = dot_t(col_rows, w_s[p, 0:PIX, :]) + dot_t(col_rows, w_s[p, PIX : 2 * PIX, :])
            for k in range(3):
                image[k, at, :] = shown[k : k + 1, :] + shown[3 + k : 4 + k, :]
            cot_rows = jnp.concatenate([cot_h, cot_l, pad2], axis=0).astype(bf16)
            gcol = dot(jnp.concatenate([cot_rows, cot_rows], axis=1), w_s[p])
            acc = [[None, None] for _ in range(3)]
            for py in range(TILE_SIDE):
                dy = (py - 7.5) - uy
                for h in range(2):
                    r = slice(TILE_SIDE * py + 8 * h, TILE_SIDE * py + 8 * h + 8)
                    alpha = al_s[p, r, :]
                    g = s_s[p, r, :] - lb_s[p, r, :] * (alpha / (1.0 - alpha))
                    gy = g * dy
                    for n, v in enumerate((g, gy, gy * dy)):
                        acc[n][h] = v if py == 0 else acc[n][h] + v

            def down(a, b):
                return jnp.sum(a + b, axis=0, keepdims=True)

            xg = [dx[h] * acc[0][h] for h in range(2)]
            grad = [
                down(acc[0][0], acc[0][1]),
                down(xg[0], xg[1]),
                down(acc[1][0], acc[1][1]),
                down(dx[0] * xg[0], dx[1] * xg[1]),
                down(dx[0] * acc[1][0], dx[1] * acc[1][1]),
                down(acc[2][0], acc[2][1]),
            ] + [gcol[k : k + 1, :] + gcol[3 + k : 4 + k, :] for k in range(3)]
            s = lists[at, :]
            chunk_hit = ch_iota == (((s >> 7) & 3) * 8 + (s >> 9))
            for f in range(N_GRAD):
                hi, low = halves(jnp.where(chunk_hit, grad[f], 0.0))
                grads[p, 32 * f : 32 * (f + 1), 0:LIST] = hi
                grads[p, 32 * f : 32 * (f + 1), LIST : 2 * LIST] = low
            lane_hit = (lane_iota == (s & (LANES - 1))).astype(f32).astype(bf16)
            slot[...] += dot_t(grads[p], jnp.concatenate([lane_hit, lane_hit], axis=1))
        return carry

    lax.fori_loop(0, TILES_HERE // 2, pair, 0)

    terms = [jnp.zeros((8, LANES), f32) for _ in range(10)]
    for q in range(4):
        r = slice(8 * q, 8 * q + 8)
        ca, cb, cc = tab[2, r, :], tab[3, r, :], tab[4, r, :]
        gr = [slot[32 * f + 8 * q : 32 * f + 8 * q + 8, :] for f in range(N_GRAD)]
        du = (ca * gr[1] + cb * gr[2], cb * gr[1] + cc * gr[2])
        h00, h01, h11 = conic_pull(ca, cb, cc, gr[3], gr[4], gr[5])
        for c in range(3):
            mean, n0, n1 = tab[9 + c, r, :], tab[12 + c, r, :], tab[15 + c, r, :]
            terms[c] += du[0] * mean + 2.0 * (h00 * n0 + h01 * n1)
            terms[3 + c] += du[1] * mean + 2.0 * (h01 * n0 + h11 * n1)
            terms[8] += gr[6 + c] * tab[18 + c, r, :]
            terms[9] += gr[6 + c] * tab[21 + c, r, :]
        terms[6] += du[0]
        terms[7] += du[1]
    lanes = lax.broadcasted_iota(jnp.int32, (8, LANES), 1)
    share = jnp.zeros((8, LANES), f32)
    for m in range(10):
        total = jnp.sum(jnp.sum(terms[m], axis=0, keepdims=True), axis=1, keepdims=True)
        share = jnp.where(lanes == CAP + m, jnp.broadcast_to(total, (8, LANES)), share)
    for q in range(4):
        pieces = swap_groups([slot[32 * f + 8 * q : 32 * f + 8 * q + 8, :] for f in range(8)])
        last = slot[32 * 8 + 8 * q : 32 * 8 + 8 * q + 8, :]
        for k in range(8):
            first_row = GRAD_ROWS * 8 * (8 * q + k)
            out[pl.ds(first_row, 8, stride=GRAD_ROWS), :] = pieces[k]
            moved = last if k == 0 else pltpu.roll(last, LANES - CAP * k, 1)
            out[pl.ds(first_row + 1, 8, stride=GRAD_ROWS), :] = jnp.where(lanes < CAP, moved, share)


def conic_pull(ca, cb, cc, qxx, qxy, qyy):
    t00, t01 = ca * qxx + cb * qxy, ca * qxy + cb * qyy
    t10, t11 = cb * qxx + cc * qxy, cb * qxy + cc * qyy
    return 0.5 * (t00 * ca + t01 * cb), 0.5 * (t00 * cb + t01 * cc), 0.5 * (t10 * cb + t11 * cc)


PULL_CHUNK = 128


def pull_kernel(
    meta, returned, asked, conic, table, log_scales, quat_w, quat_v, cam, out, cam_out, row_s, idx_s, lhs_s, sum_s, gc_s
):
    index = asked_lanes(asked, meta[TILES_HERE + 1])
    for q in range(4):
        idx_s[:, q * LANES : (q + 1) * LANES] = index[q]
    group = lax.broadcasted_iota(jnp.int32, (8, LANES), 1) // CAP
    camera = jnp.zeros((8, LANES), f32)
    for q in range(4):
        pieces = [returned[pl.ds(GRAD_ROWS * 8 * (8 * q + k), 8, stride=GRAD_ROWS), :] for k in range(8)]
        pieces = swap_groups(pieces)
        for f in range(8):
            row_s[f, :, q * LANES : (q + 1) * LANES] = pieces[f]
        last = None
        for k in range(8):
            piece = returned[pl.ds(GRAD_ROWS * 8 * (8 * q + k) + 1, 8, stride=GRAD_ROWS), :]
            camera = camera + piece
            last = piece if k == 0 else jnp.where(group == k, pltpu.roll(piece, CAP * k, 1), last)
        row_s[8, :, q * LANES : (q + 1) * LANES] = last
    cam_out[...] = pltpu.roll(camera, LANES - CAP, 1)[:, 0:10]

    slots = N_TILE * CAP
    high_iota = lax.broadcasted_iota(jnp.int32, (16, slots), 0)
    lane_iota = lax.broadcasted_iota(jnp.int32, (LANES, slots), 0)

    def image(i, carry):
        at = pl.ds(i, 1)
        s = idx_s[at, :]
        high_hit = high_iota == (s >> 7)
        lane_hit = (lane_iota == (s & (LANES - 1))).astype(f32).astype(bf16)
        for f in range(N_GRAD):
            hi, low = halves(jnp.where(high_hit, row_s[f, at, :], 0.0))
            lhs_s[16 * f : 16 * (f + 1), 0:slots] = hi
            lhs_s[16 * f : 16 * (f + 1), slots : 2 * slots] = low
        sum_s[pl.ds(pl.multiple_of(i * (16 * N_GRAD), 16), 16 * N_GRAD), :] = dot_t(
            lhs_s[...], jnp.concatenate([lane_hit, lane_hit], axis=1)
        )
        return carry

    lax.fori_loop(0, N_IMG, image, 0)

    column = [jnp.broadcast_to(cam[:, m : m + 1], (N_IMG, PULL_CHUNK)) for m in range(6)]

    def chunk(h, carry):
        at = pl.ds(pl.multiple_of(h * PULL_CHUNK, PULL_CHUNK), PULL_CHUNK)
        gr = [sum_s[pl.ds(16 * f + h, 8, stride=16 * N_GRAD), :] for f in range(N_GRAD)]
        ca, cb, cc = conic[0, :, at], conic[1, :, at], conic[2, :, at]
        du = (ca * gr[1] + cb * gr[2], cb * gr[1] + cc * gr[2])
        h00, h01, h11 = conic_pull(ca, cb, cc, gr[3], gr[4], gr[5])
        a0, a1 = column[0:3], column[3:6]

        def over_images(v):
            return jnp.sum(v, axis=0, keepdims=True)

        for c in range(3):
            out[c : c + 1, at] = over_images(a0[c] * du[0] + a1[c] * du[1])
        t0 = [h00 * a0[c] + h01 * a1[c] for c in range(3)]
        t1 = [h01 * a0[c] + h11 * a1[c] for c in range(3)]
        v = [[None] * 3 for _ in range(3)]
        for c in range(3):
            for d in range(c, 3):
                v[c][d] = v[d][c] = over_images(t0[c] * a0[d] + t1[c] * a1[d])
        ls = [log_scales[c : c + 1, at] for c in range(3)]
        quat = [quat_w[0:1, at]] + [quat_v[c : c + 1, at] for c in range(3)]
        m, pull = jax.vjp(shape_matrix, ls, quat)
        dm = [[2.0 * sum(v[r][d] * m[d][c] for d in range(3)) for c in range(3)] for r in range(3)]
        dls, dquat = pull(dm)
        for c in range(3):
            out[3 + c : 4 + c, at] = dls[c]
        for c in range(4):
            out[6 + c : 7 + c, at] = dquat[c]
        base = conic[3, 0:1, at]
        out[10:11, at] = over_images(gr[0]) * (1.0 - base)
        for k in range(3):
            gc_s[8 * k : 8 * k + 8, at] = gr[6 + k]
        return carry

    lax.fori_loop(0, OWNED // PULL_CHUNK, chunk, 0)

    y_h, y_l = halves(jnp.transpose(table[...])[0:16, :])
    y_all = jnp.concatenate([y_h.astype(f32), y_h.astype(f32), y_l.astype(f32), y_l.astype(f32)], axis=1).astype(bf16)
    for k in range(3):
        g_h, g_l = halves(gc_s[8 * k : 8 * k + 8, :])
        g_all = jnp.concatenate([g_h.astype(f32), g_l.astype(f32), g_h.astype(f32), g_l.astype(f32)], axis=0).astype(bf16)
        out[11 + 16 * k : 27 + 16 * k, :] = dot(y_all, g_all)


def whole(memory=pltpu.VMEM):
    return pl.BlockSpec(memory_space=memory)


def call(kernel, name, out_shape, scratch, n_in, smem=0):
    return pl.pallas_call(
        kernel,
        name=name,
        out_shape=out_shape,
        in_specs=[whole(pltpu.SMEM)] * smem + [whole()] * (n_in - smem),
        out_specs=jax.tree.map(lambda _: whole(), out_shape),
        scratch_shapes=scratch,
        compiler_params=pltpu.CompilerParams(vmem_limit_bytes=32 << 20),
    )


def exchange(array):
    return lax.all_to_all(array, ORDER, split_axis=0, concat_axis=0, tiled=True)


def exchange_rows(array, rows):
    shape = array.shape
    return exchange(array.reshape(-1, 1, rows * LANES)).reshape(shape)


def local(
    means, log_scales, quat_w, quat_v, opacity, sh_coeffs, cameras, requests, lists, counts, image_cot
):
    devices = N_IMG * N_TILE
    meta = jnp.concatenate(
        [counts[0], jnp.stack([lax.axis_index("tile"), lax.axis_index("img")]).astype(jnp.int32)]
    )
    by_owner = jnp.transpose(requests.reshape(N_IMG, N_TILE, CAP), (0, 2, 1)).reshape(N_IMG * CAP, N_TILE)
    wanted = call(ask_kernel, "ask", jax.ShapeDtypeStruct((devices, LANES), jnp.int32), [], 1)(by_owner)
    wanted, meta = lax.optimization_barrier((wanted, meta))
    asked = exchange_rows(wanted, 1)
    packed, conic, table = call(
        pick_kernel,
        "pick",
        (
            jax.ShapeDtypeStruct((FEAT_ROWS * devices, LANES), f32),
            jax.ShapeDtypeStruct((4, N_IMG, OWNED), f32),
            jax.ShapeDtypeStruct((N_IMG, LANES), f32),
        ),
        [pltpu.VMEM((N_FEAT, N_IMG, OWNED), f32), pltpu.VMEM((48, N_IMG, LANES), f32)],
        9,
        smem=1,
    )(meta, asked, means, log_scales, quat_w, quat_v, opacity, sh_coeffs, cameras)
    rows = exchange_rows(packed, FEAT_ROWS)
    rendered, slot_grads = call(
        render_kernel,
        "render",
        (
            jax.ShapeDtypeStruct((3, TILES_HERE, PIX), f32),
            jax.ShapeDtypeStruct((GRAD_ROWS * devices, LANES), f32),
        ),
        [
            pltpu.VMEM((N_FEAT, 32, LANES), f32),
            pltpu.VMEM((N_USED, 8, LIST), f32),
            pltpu.VMEM((2, 32 * N_GRAD, 2 * LIST), bf16),
            pltpu.VMEM((32 * N_GRAD, LANES), f32),
            pltpu.VMEM((2 * LIST, LIST), bf16),
            pltpu.VMEM((2 * LIST, LIST), bf16),
            pltpu.VMEM((2, PIX, LIST), f32),
            pltpu.VMEM((2, PIX, 2 * LIST), bf16),
            pltpu.VMEM((2, PIX, LIST), f32),
            pltpu.VMEM((2, PIX, LIST), f32),
            pltpu.VMEM((2, 2 * PIX, LIST), bf16),
            pltpu.VMEM((2, PIX, 2 * LIST), bf16),
        ],
        4,
        smem=1,
    )(meta, rows, lists[0], image_cot[0])
    returned = exchange_rows(slot_grads, GRAD_ROWS)
    param_grad, camera_grad = call(
        pull_kernel,
        "pull",
        (
            jax.ShapeDtypeStruct((59, OWNED), f32),
            jax.ShapeDtypeStruct((N_IMG, 10), f32),
        ),
        [
            pltpu.VMEM((N_GRAD, N_IMG, N_TILE * CAP), f32),
            pltpu.VMEM((N_IMG, N_TILE * CAP), jnp.int32),
            pltpu.VMEM((16 * N_GRAD, 2 * N_TILE * CAP), bf16),
            pltpu.VMEM((N_IMG * 16 * N_GRAD, LANES), f32),
            pltpu.VMEM((24, OWNED), f32),
        ],
        9,
        smem=1,
    )(meta, returned, asked, conic, table, log_scales, quat_w, quat_v, cameras)
    return (rendered[None], param_grad, camera_grad)


def solution(mesh):
    own = P(None, ALL)
    return jax.shard_map(
        local,
        mesh=mesh,
        in_specs=(
            own,
            own,
            own,
            own,
            own,
            own,
            P(),
            P("img", "tile", None, None, None),
            P("img", "tile", None),
            P("img", "tile"),
            P("img", None, "tile", None),
        ),
        out_specs=(P("img", None, "tile", None), own, P()),
        check_vma=False,
    )
```

```python
import jax
import jax.numpy as jnp
from jax import lax
from jax.experimental import pallas as pl
from jax.experimental.pallas import tpu as pltpu
from jax.sharding import PartitionSpec as P

TILE_SIDE = 16
TW = 16
ALL = ("img", "tile")
ORDER = ("tile", "img")
N_IMG = 8
N_TILE = 32
CAP = 16
OWNED = 2048
LIST = 256
TILES_HERE = 8
PIX = 256
LANES = 128
N_FEAT = 24
N_USED = 9
N_GRAD = 9
FEAT_ROWS = 3
GRAD_ROWS = 2

sh_first = 0.28209479177387814
sh_second = 0.4886025119029199
sh_third = (
    1.0925484305920792,
    -1.0925484305920792,
    0.31539156525252005,
    -1.0925484305920792,
    0.5462742152960396,
)
sh_fourth = (
    -0.5900435899266435,
    2.890611442640554,
    -0.4570457994644658,
    0.3731763325901154,
    -0.4570457994644658,
    1.445305721320277,
    -0.5900435899266435,
)
dilation = 0.3
LOG2E = 1.4426950408889634
f32 = jnp.float32
bf16 = jnp.bfloat16


def harmonics_of(polar, azimuth):
    sin_p, cos_p = jnp.sin(polar), jnp.cos(polar)
    x = sin_p * jnp.cos(azimuth)
    y = sin_p * jnp.sin(azimuth)
    z = cos_p
    xx, yy, zz = x * x, y * y, z * z
    return [
        sh_first + 0.0 * x,
        -sh_second * y,
        sh_second * z,
        -sh_second * x,
        sh_third[0] * x * y,
        sh_third[1] * y * z,
        sh_third[2] * (2.0 * zz - xx - yy),
        sh_third[3] * x * z,
        sh_third[4] * (xx - yy),
        sh_fourth[0] * y * (3.0 * xx - yy),
        sh_fourth[1] * x * y * z,
        sh_fourth[2] * y * (4.0 * zz - xx - yy),
        sh_fourth[3] * z * (2.0 * zz - 3.0 * xx - 3.0 * yy),
        sh_fourth[4] * x * (4.0 * zz - xx - yy),
        sh_fourth[5] * z * (xx - yy),
        sh_fourth[6] * x * (xx - 3.0 * yy),
    ]


def shape_matrix(log_scales, quat):
    w, x, y, z = quat
    norm = jnp.sqrt(w * w + x * x + y * y + z * z)
    w, x, y, z = w / norm, x / norm, y / norm, z / norm
    rotation = (
        (1.0 - 2.0 * (y * y + z * z), 2.0 * (x * y - w * z), 2.0 * (x * z + w * y)),
        (2.0 * (x * y + w * z), 1.0 - 2.0 * (x * x + z * z), 2.0 * (y * z - w * x)),
        (2.0 * (x * z - w * y), 2.0 * (y * z + w * x), 1.0 - 2.0 * (x * x + y * y)),
    )
    stretch = [jnp.exp(v) for v in log_scales]
    return [[rotation[r][c] * stretch[c] for c in range(3)] for r in range(3)]


def turn_groups(vregs):
    group = lax.broadcasted_iota(jnp.int32, (8, LANES), 1) // CAP
    work = [vregs[-k % 8] for k in range(8)]
    for bit in (1, 2, 4):
        move = (group & bit) != 0
        work = [jnp.where(move, work[(k - bit) % 8], work[k]) for k in range(8)]
    return work


def rotate(value, groups):
    if isinstance(groups, int):
        shift = CAP * groups % LANES
        return value if shift == 0 else pltpu.roll(value, shift, 1)
    return pltpu.roll(value, (CAP * groups) & (LANES - 1), 1)


def swap_groups(vregs, turned=0, leave=False):
    vregs = turn_groups([rotate(v, i + LANES // CAP - turned) for i, v in enumerate(vregs)])
    return vregs if leave else [rotate(v, -g) for g, v in enumerate(vregs)]


def lane_take(table, lanes):
    return jnp.take_along_axis(table, lanes, axis=1, mode="promise_in_bounds")


def halves(value):
    high = value.astype(bf16)
    return high, (value - high.astype(f32)).astype(bf16)


def dot(a, b):
    return lax.dot_general(a, b, (((1,), (0,)), ((), ())), preferred_element_type=f32)


def dot_t(a, b):
    return lax.dot_general(a, b, (((1,), (1,)), ((), ())), preferred_element_type=f32)


PROJECT_CHUNK = 256


def ask_kernel(wanted, out):
    padded = jnp.concatenate([wanted[...], jnp.zeros((LANES, LANES - N_TILE), jnp.int32)], axis=1)
    turned = jnp.transpose(padded)
    for b in range(N_TILE):
        out[8 * b : 8 * b + 8, :] = jnp.broadcast_to(turned[b : b + 1, :], (8, LANES))


def asked_lanes(asked, my_img):
    group = lax.broadcasted_iota(jnp.int32, (8, LANES), 1) // CAP
    base = LANES - CAP * my_img
    result = []
    for q in range(4):
        total = None
        for k in range(8):
            piece = pltpu.roll(asked[8 * (8 * q + k) : 8 * (8 * q + k) + 8, :], (base + CAP * k) & (LANES - 1), 1)
            total = piece if k == 0 else jnp.where(group == k, piece, total)
        result.append(total)
    return result


def project(means, log_scales, quat_w, quat_v, opacity, sh, cam, out, harm):
    column = [jnp.broadcast_to(cam[:, m : m + 1], (N_IMG, PROJECT_CHUNK)) for m in range(8)]

    def chunk(h, carry):
        at = pl.ds(pl.multiple_of(h * PROJECT_CHUNK, PROJECT_CHUNK), PROJECT_CHUNK)
        mean = [means[c : c + 1, at] for c in range(3)]
        quat = [quat_w[0:1, at]] + [quat_v[c : c + 1, at] for c in range(3)]
        m = shape_matrix([log_scales[c : c + 1, at] for c in range(3)], quat)
        for row in range(2):
            a = column[3 * row : 3 * row + 3]
            out[row, :, at] = a[0] * mean[0] + a[1] * mean[1] + a[2] * mean[2] + column[6 + row]
        p = [
            [
                sum(column[3 * row + r] * m[r][c] for r in range(3))
                for c in range(3)
            ]
            for row in range(2)
        ]
        s00 = p[0][0] * p[0][0] + p[0][1] * p[0][1] + p[0][2] * p[0][2] + dilation
        s01 = p[0][0] * p[1][0] + p[0][1] * p[1][1] + p[0][2] * p[1][2]
        s11 = p[1][0] * p[1][0] + p[1][1] * p[1][1] + p[1][2] * p[1][2] + dilation
        det = s00 * s11 - s01 * s01
        out[2, :, at] = s11 / det
        out[3, :, at] = -s01 / det
        out[4, :, at] = s00 / det
        base = 1.0 / (1.0 + jnp.exp(-opacity[0:1, at]))
        out[5, :, at] = jnp.broadcast_to(base, (N_IMG, PROJECT_CHUNK))
        for c in range(3):
            out[9 + c, :, at] = jnp.broadcast_to(mean[c], (N_IMG, PROJECT_CHUNK))
            for row in range(2):
                out[12 + 3 * row + c, :, at] = (
                    m[c][0] * p[row][0] + m[c][1] * p[row][1] + m[c][2] * p[row][2]
                )
        for base_row, first, start in ((6, 0, 0.5), (18, 16, 0.0), (21, 32, 0.0)):
            total = [jnp.full((N_IMG, PROJECT_CHUNK), start, f32) for _ in range(3)]
            for b in range(16):
                y = jnp.concatenate([harm[first + b]] * (PROJECT_CHUNK // LANES), axis=1)
                for k in range(3):
                    total[k] = total[k] + y * sh[16 * k + b : 16 * k + b + 1, at]
            for k in range(3):
                out[base_row + k, :, at] = total[k]
        return carry

    lax.fori_loop(0, OWNED // PROJECT_CHUNK, chunk, 0)


def project_kernel(means, log_scales, quat_w, quat_v, opacity, sh, cam, feats, table, harm):
    polar = jnp.broadcast_to(cam[:, 8:9], (N_IMG, LANES))
    azimuth = jnp.broadcast_to(cam[:, 9:10], (N_IMG, LANES))
    one, zero = jnp.ones_like(polar), jnp.zeros_like(polar)
    values, d_polar = jax.jvp(harmonics_of, (polar, azimuth), (one, zero))
    d_azimuth = jax.jvp(harmonics_of, (polar, azimuth), (zero, one))[1]
    lanes = lax.broadcasted_iota(jnp.int32, (N_IMG, LANES), 1)
    packed = jnp.zeros((N_IMG, LANES), f32)
    for b in range(16):
        harm[b] = values[b]
        harm[16 + b] = d_polar[b]
        harm[32 + b] = d_azimuth[b]
        packed = jnp.where(lanes == b, values[b], packed)
    table[...] = packed
    project(means, log_scales, quat_w, quat_v, opacity, sh, cam, feats, harm)


def pick_kernel(meta, asked, feats, out, index):
    for q, value in enumerate(asked_lanes(asked, meta[TILES_HERE + 1])):
        for f in range(8):
            index[8 * q + f] = rotate(value, f)

    def step(n, carry):
        g, q = n >> 2, n & 3
        picked = []
        for f in range(8):
            here = index[8 * q + f]
            low, high = here & (LANES - 1), here >> 7
            value = None
            for h in range(OWNED // LANES):
                found = lane_take(feats[8 * g + f, :, h * LANES : (h + 1) * LANES], low)
                value = found if h == 0 else jnp.where(high == h, found, value)
            picked.append(value)
        for k, row in enumerate(turn_groups(picked)):
            out[pl.ds(FEAT_ROWS * 8 * (8 * q + k) + g, 8, stride=FEAT_ROWS), :] = row
        return carry

    lax.fori_loop(0, 4 * FEAT_ROWS, step, 0, unroll=4)


def render_kernel(
    meta,
    rows,
    lists,
    cot,
    image,
    out,
    tab,
    feat,
    grads,
    slot,
    upper,
    lower,
    al_s,
    lk_s,
    lb_s,
    s_s,
    w_s,
    sw_s,
):
    tile_base = meta[TILES_HERE] * TILES_HERE
    turned = meta[TILES_HERE] & 7

    def sort_rows(n, carry):
        g, q = n >> 2, n & 3
        pieces = [
            rows[pl.ds(FEAT_ROWS * 8 * (8 * q + k) + g, 8, stride=FEAT_ROWS), :] for k in range(8)
        ]
        pieces = swap_groups(pieces, turned)
        for f in range(8):
            tab[8 * g + f, pl.ds(pl.multiple_of(8 * q, 8), 8), :] = pieces[f]
        return carry

    lax.fori_loop(0, 4 * FEAT_ROWS, sort_rows, 0, unroll=4)
    entry_lane = [lists[:, h * LANES : (h + 1) * LANES] & (LANES - 1) for h in range(2)]
    entry_chunk = []
    for h in range(2):
        s = lists[:, h * LANES : (h + 1) * LANES]
        entry_chunk.append(((s >> 7) & 3) * 8 + (s >> 9))

    def gather(ch, carry):
        new = list(carry)
        for h in range(2):
            hit = entry_chunk[h] == ch
            for f in range(N_USED):
                row = jnp.broadcast_to(tab[f, pl.ds(ch, 1), :], (8, LANES))
                new[2 * f + h] = jnp.where(hit, lane_take(row, entry_lane[h]), carry[2 * f + h])
        return tuple(new)

    zero = jnp.zeros((8, LANES), f32)
    found = lax.fori_loop(0, 32, gather, tuple([zero] * (2 * N_USED)), unroll=8)
    for f in range(N_USED):
        for h in range(2):
            feat[f, :, h * LANES : (h + 1) * LANES] = found[2 * f + h]
    ri = lax.broadcasted_iota(jnp.int32, (LIST, LIST), 0)
    ci = lax.broadcasted_iota(jnp.int32, (LIST, LIST), 1)
    up = (ri < ci).astype(f32).astype(bf16)
    lo = (ri > ci).astype(f32).astype(bf16)
    for part in range(2):
        upper[part * LIST : (part + 1) * LIST, :] = up
        lower[part * LIST : (part + 1) * LIST, :] = lo
    slot[...] = jnp.zeros_like(slot)
    lane = lax.broadcasted_iota(jnp.int32, (1, LIST), 1)
    px = lax.broadcasted_iota(jnp.int32, (8, LIST), 0).astype(f32) - 7.5
    ch_iota = lax.broadcasted_iota(jnp.int32, (32, LIST), 0)
    lane_iota = lax.broadcasted_iota(jnp.int32, (LANES, LIST), 0)

    def row8(v):
        return jnp.broadcast_to(v, (8, LIST))

    def pair(pair_index, carry):
        tiles = [2 * pair_index, 2 * pair_index + 1]
        state = []
        for p in range(2):
            j = tiles[p]
            number = tile_base + j
            centre_x = (TILE_SIDE * (number % TW)).astype(f32) + (0.5 * TILE_SIDE - 0.5 * TILE_SIDE * TW)
            centre_y = (TILE_SIDE * (number // TW)).astype(f32) + (0.5 * TILE_SIDE - 0.5 * TILE_SIDE * TW)
            at = pl.ds(j, 1)
            ux = feat[0, at, :] - centre_x
            uy = row8(feat[1, at, :] - centre_y)
            ca, cb, cc = feat[2, at, :], feat[3, at, :], feat[4, at, :]
            op = row8(jnp.where(lane < meta[j], feat[5, at, :], 0.0))
            cc = row8(cc * (-0.5 * LOG2E))
            ux, na, nb = row8(ux), row8(ca * (-0.5 * LOG2E)), row8(cb * (-LOG2E))
            dx = [px - ux, px + (8.0 - ux)]
            na = [na * d * d for d in dx]
            nb = [nb * d for d in dx]
            colours = jnp.concatenate([feat[6 + k, at, :] for k in range(3)], axis=0)
            cots = jnp.concatenate([cot[k, at, :] for k in range(3)], axis=0)
            col_h, col_l, cot_h, cot_l = [v.astype(f32) for v in halves(colours) + halves(cots)]
            pad = jnp.zeros((4, LIST), f32)
            cot_k = jnp.concatenate([cot_h, cot_h, cot_l, cot_l, pad], axis=0)
            col_k = jnp.concatenate([col_h, col_l, col_h, col_l, pad], axis=0).astype(bf16)
            s_s[p] = dot(jnp.transpose(cot_k).astype(bf16), col_k)
            for py in range(TILE_SIDE):
                r = slice(TILE_SIDE * py, TILE_SIDE * (py + 1))
                dy = (py - 7.5) - uy
                cy = cc * dy * dy
                alpha = jnp.concatenate(
                    [op * jnp.exp2((na[h] + cy) + nb[h] * dy) for h in range(2)], axis=0
                )
                al_s[p, r, :] = alpha
                hi, low = halves(jnp.log2(1.0 - alpha))
                lk_s[p, r, 0:LIST] = hi
                lk_s[p, r, LIST : 2 * LIST] = low
            lb_s[p] = dot(lk_s[p], upper[...])
            state.append((at, uy, dx, col_h, col_l, cot_h, cot_l))
        for p in range(2):
            for py in range(TILE_SIDE):
                r = slice(TILE_SIDE * py, TILE_SIDE * (py + 1))
                w = al_s[p, r, :] * jnp.exp2(lb_s[p, r, :])
                hi, low = halves(w)
                w_s[p, r, :] = hi
                w_s[p, PIX + TILE_SIDE * py : PIX + TILE_SIDE * (py + 1), :] = low
                sw = s_s[p, r, :] * w
                s_s[p, r, :] = sw
                hi, low = halves(sw)
                sw_s[p, r, 0:LIST] = hi
                sw_s[p, r, LIST : 2 * LIST] = low
            lb_s[p] = dot(sw_s[p], lower[...])
        for p in range(2):
            at, uy, dx, col_h, col_l, cot_h, cot_l = state[p]
            pad2 = jnp.zeros((2, LIST), f32)
            col_rows = jnp.concatenate([col_h, col_l, pad2], axis=0).astype(bf16)
            shown = dot_t(col_rows, w_s[p, 0:PIX, :]) + dot_t(col_rows, w_s[p, PIX : 2 * PIX, :])
            for k in range(3):
                image[k, at, :] = shown[k : k + 1, :] + shown[3 + k : 4 + k, :]
            cot_rows = jnp.concatenate([cot_h, cot_l, pad2], axis=0).astype(bf16)
            gcol = dot(jnp.concatenate([cot_rows, cot_rows], axis=1), w_s[p])
            acc = [[None, None] for _ in range(3)]
            for py in range(TILE_SIDE):
                dy = (py - 7.5) - uy
                for h in range(2):
                    r = slice(TILE_SIDE * py + 8 * h, TILE_SIDE * py + 8 * h + 8)
                    alpha = al_s[p, r, :]
                    g = s_s[p, r, :] - lb_s[p, r, :] * (alpha / (1.0 - alpha))
                    gy = g * dy
                    for n, v in enumerate((g, gy, gy * dy)):
                        acc[n][h] = v if py == 0 else acc[n][h] + v

            def down(a, b):
                return jnp.sum(a + b, axis=0, keepdims=True)

            xg = [dx[h] * acc[0][h] for h in range(2)]
            grad = [
                down(acc[0][0], acc[0][1]),
                down(xg[0], xg[1]),
                down(acc[1][0], acc[1][1]),
                down(dx[0] * xg[0], dx[1] * xg[1]),
                down(dx[0] * acc[1][0], dx[1] * acc[1][1]),
                down(acc[2][0], acc[2][1]),
            ] + [gcol[k : k + 1, :] + gcol[3 + k : 4 + k, :] for k in range(3)]
            s = lists[at, :]
            chunk_hit = ch_iota == (((s >> 7) & 3) * 8 + (s >> 9))
            for f in range(N_GRAD):
                hi, low = halves(jnp.where(chunk_hit, grad[f], 0.0))
                grads[p, 32 * f : 32 * (f + 1), 0:LIST] = hi
                grads[p, 32 * f : 32 * (f + 1), LIST : 2 * LIST] = low
            lane_hit = (lane_iota == (s & (LANES - 1))).astype(f32).astype(bf16)
            slot[...] += dot_t(grads[p], jnp.concatenate([lane_hit, lane_hit], axis=1))
        return carry

    lax.fori_loop(0, TILES_HERE // 2, pair, 0)

    terms = [jnp.zeros((8, LANES), f32) for _ in range(10)]
    for q in range(4):
        r = slice(8 * q, 8 * q + 8)
        ca, cb, cc = tab[2, r, :], tab[3, r, :], tab[4, r, :]
        gr = [slot[32 * f + 8 * q : 32 * f + 8 * q + 8, :] for f in range(N_GRAD)]
        du = (ca * gr[1] + cb * gr[2], cb * gr[1] + cc * gr[2])
        h00, h01, h11 = conic_pull(ca, cb, cc, gr[3], gr[4], gr[5])
        for c in range(3):
            mean, n0, n1 = tab[9 + c, r, :], tab[12 + c, r, :], tab[15 + c, r, :]
            terms[c] += du[0] * mean + 2.0 * (h00 * n0 + h01 * n1)
            terms[3 + c] += du[1] * mean + 2.0 * (h01 * n0 + h11 * n1)
            terms[8] += gr[6 + c] * tab[18 + c, r, :]
            terms[9] += gr[6 + c] * tab[21 + c, r, :]
        terms[6] += du[0]
        terms[7] += du[1]
    lanes = lax.broadcasted_iota(jnp.int32, (8, LANES), 1)
    share = jnp.zeros((8, LANES), f32)
    for m in range(10):
        total = jnp.sum(jnp.sum(terms[m], axis=0, keepdims=True), axis=1, keepdims=True)
        share = jnp.where(lanes == CAP + m, jnp.broadcast_to(total, (8, LANES)), share)
    group = lanes // CAP
    shares = [rotate(share, k) for k in range(8)]
    for q in range(4):
        pieces = swap_groups([slot[32 * f + 8 * q : 32 * f + 8 * q + 8, :] for f in range(8)], leave=True)
        last = slot[32 * 8 + 8 * q : 32 * 8 + 8 * q + 8, :]
        for k in range(8):
            first_row = GRAD_ROWS * 8 * (8 * q + k)
            out[pl.ds(first_row, 8, stride=GRAD_ROWS), :] = pieces[k]
            out[pl.ds(first_row + 1, 8, stride=GRAD_ROWS), :] = jnp.where(group == k, last, shares[k])


def conic_pull(ca, cb, cc, qxx, qxy, qyy):
    t00, t01 = ca * qxx + cb * qxy, ca * qxy + cb * qyy
    t10, t11 = cb * qxx + cc * qxy, cb * qxy + cc * qyy
    return 0.5 * (t00 * ca + t01 * cb), 0.5 * (t00 * cb + t01 * cc), 0.5 * (t10 * cb + t11 * cc)


PULL_CHUNK = 512


def pull_kernel(
    meta, returned, asked, feats, table, log_scales, quat_w, quat_v, cam, out, cam_out, row_s, idx_s, lhs_s, sum_s, gc_s
):
    index = asked_lanes(asked, meta[TILES_HERE + 1])
    for q in range(4):
        idx_s[:, q * LANES : (q + 1) * LANES] = index[q]
    group = lax.broadcasted_iota(jnp.int32, (8, LANES), 1) // CAP
    turned = meta[TILES_HERE] & 7
    camera = jnp.zeros((8, LANES), f32)
    for q in range(4):
        pieces = [returned[pl.ds(GRAD_ROWS * 8 * (8 * q + k), 8, stride=GRAD_ROWS), :] for k in range(8)]
        pieces = swap_groups(pieces, turned)
        for f in range(8):
            row_s[f, :, q * LANES : (q + 1) * LANES] = pieces[f]
        last = None
        for k in range(8):
            piece = returned[pl.ds(GRAD_ROWS * 8 * (8 * q + k) + 1, 8, stride=GRAD_ROWS), :]
            camera = camera + piece
            moved = rotate(piece, k + 8 - turned)
            last = moved if k == 0 else jnp.where(group == k, moved, last)
        row_s[8, :, q * LANES : (q + 1) * LANES] = last
    cam_out[...] = rotate(camera, 7 - turned)[:, 0:10]

    slots = N_TILE * CAP
    high_iota = lax.broadcasted_iota(jnp.int32, (16, slots), 0)
    lane_iota = lax.broadcasted_iota(jnp.int32, (LANES, slots), 0)

    def image(i, carry):
        at = pl.ds(i, 1)
        s = idx_s[at, :]
        high_hit = high_iota == (s >> 7)
        lane_hit = (lane_iota == (s & (LANES - 1))).astype(f32).astype(bf16)
        for f in range(N_GRAD):
            hi, low = halves(jnp.where(high_hit, row_s[f, at, :], 0.0))
            lhs_s[16 * f : 16 * (f + 1), 0:slots] = hi
            lhs_s[16 * f : 16 * (f + 1), slots : 2 * slots] = low
        sum_s[pl.ds(pl.multiple_of(i * (16 * N_GRAD), 16), 16 * N_GRAD), :] = dot_t(
            lhs_s[...], jnp.concatenate([lane_hit, lane_hit], axis=1)
        )
        return carry

    lax.fori_loop(0, N_IMG, image, 0, unroll=8)

    column = [jnp.broadcast_to(cam[:, m : m + 1], (N_IMG, PULL_CHUNK)) for m in range(6)]

    def chunk(h, carry):
        at = pl.ds(pl.multiple_of(h * PULL_CHUNK, PULL_CHUNK), PULL_CHUNK)
        parts = PULL_CHUNK // LANES
        gr = [
            jnp.concatenate(
                [sum_s[pl.ds(16 * f + h * parts + e, 8, stride=16 * N_GRAD), :] for e in range(parts)],
                axis=1,
            )
            for f in range(N_GRAD)
        ]
        ca, cb, cc = feats[2, :, at], feats[3, :, at], feats[4, :, at]
        du = (ca * gr[1] + cb * gr[2], cb * gr[1] + cc * gr[2])
        h00, h01, h11 = conic_pull(ca, cb, cc, gr[3], gr[4], gr[5])
        a0, a1 = column[0:3], column[3:6]

        def over_images(v):
            return jnp.sum(v, axis=0, keepdims=True)

        for c in range(3):
            out[c : c + 1, at] = over_images(a0[c] * du[0] + a1[c] * du[1])
        t0 = [h00 * a0[c] + h01 * a1[c] for c in range(3)]
        t1 = [h01 * a0[c] + h11 * a1[c] for c in range(3)]
        v = [[None] * 3 for _ in range(3)]
        for c in range(3):
            for d in range(c, 3):
                v[c][d] = v[d][c] = over_images(t0[c] * a0[d] + t1[c] * a1[d])
        ls = [log_scales[c : c + 1, at] for c in range(3)]
        quat = [quat_w[0:1, at]] + [quat_v[c : c + 1, at] for c in range(3)]
        m, pull = jax.vjp(shape_matrix, ls, quat)
        dm = [[2.0 * sum(v[r][d] * m[d][c] for d in range(3)) for c in range(3)] for r in range(3)]
        dls, dquat = pull(dm)
        for c in range(3):
            out[3 + c : 4 + c, at] = dls[c]
        for c in range(4):
            out[6 + c : 7 + c, at] = dquat[c]
        base = feats[5, 0:1, at]
        out[10:11, at] = over_images(gr[0]) * (1.0 - base)
        for k in range(3):
            gc_s[8 * k : 8 * k + 8, at] = gr[6 + k]
        return carry

    lax.fori_loop(0, OWNED // PULL_CHUNK, chunk, 0)

    y_h, y_l = halves(jnp.transpose(table[...])[0:16, :])
    y_all = jnp.concatenate([y_h.astype(f32), y_h.astype(f32), y_l.astype(f32), y_l.astype(f32)], axis=1).astype(bf16)
    for k in range(3):
        g_h, g_l = halves(gc_s[8 * k : 8 * k + 8, :])
        g_all = jnp.concatenate([g_h.astype(f32), g_l.astype(f32), g_h.astype(f32), g_l.astype(f32)], axis=0).astype(bf16)
        out[11 + 16 * k : 27 + 16 * k, :] = dot(y_all, g_all)


def whole(memory=pltpu.VMEM):
    return pl.BlockSpec(memory_space=memory)


def call(kernel, name, out_shape, scratch, n_in, smem=0, cost=None):
    return pl.pallas_call(
        kernel,
        name=name,
        out_shape=out_shape,
        in_specs=[whole(pltpu.SMEM)] * smem + [whole()] * (n_in - smem),
        out_specs=jax.tree.map(lambda _: whole(), out_shape),
        scratch_shapes=scratch,
        cost_estimate=cost,
        compiler_params=pltpu.CompilerParams(vmem_limit_bytes=32 << 20),
    )


def exchange(array):
    return lax.all_to_all(array, ORDER, split_axis=0, concat_axis=0, tiled=True)


def exchange_rows(array, rows):
    shape = array.shape
    return exchange(array.reshape(-1, 1, rows * LANES)).reshape(shape)


def local(
    means, log_scales, quat_w, quat_v, opacity, sh_coeffs, cameras, requests, lists, counts, image_cot
):
    devices = N_IMG * N_TILE
    by_owner = jnp.transpose(requests.reshape(N_IMG, N_TILE, CAP), (0, 2, 1)).reshape(N_IMG * CAP, N_TILE)
    wanted = call(ask_kernel, "ask", jax.ShapeDtypeStruct((devices, LANES), jnp.int32), [], 1)(by_owner)
    asked = exchange_rows(wanted, 1)
    meta = jnp.concatenate(
        [counts[0], jnp.stack([lax.axis_index("tile"), lax.axis_index("img")]).astype(jnp.int32)]
    )
    feats, table = call(
        project_kernel,
        "project",
        (jax.ShapeDtypeStruct((N_FEAT, N_IMG, OWNED), f32), jax.ShapeDtypeStruct((N_IMG, LANES), f32)),
        [pltpu.VMEM((48, N_IMG, LANES), f32)],
        7,
        cost=pl.CostEstimate(flops=20_000_000, transcendentals=0, bytes_accessed=1_000_000),
    )(means, log_scales, quat_w, quat_v, opacity, sh_coeffs, cameras)
    asked, feats, meta = lax.optimization_barrier((asked, feats, meta))
    packed = call(
        pick_kernel,
        "pick",
        jax.ShapeDtypeStruct((FEAT_ROWS * devices, LANES), f32),
        [pltpu.VMEM((32, N_IMG, LANES), jnp.int32)],
        3,
        smem=1,
    )(meta, asked, feats)
    rows = exchange_rows(packed, FEAT_ROWS)
    rendered, slot_grads = call(
        render_kernel,
        "render",
        (
            jax.ShapeDtypeStruct((3, TILES_HERE, PIX), f32),
            jax.ShapeDtypeStruct((GRAD_ROWS * devices, LANES), f32),
        ),
        [
            pltpu.VMEM((N_FEAT, 32, LANES), f32),
            pltpu.VMEM((N_USED, 8, LIST), f32),
            pltpu.VMEM((2, 32 * N_GRAD, 2 * LIST), bf16),
            pltpu.VMEM((32 * N_GRAD, LANES), f32),
            pltpu.VMEM((2 * LIST, LIST), bf16),
            pltpu.VMEM((2 * LIST, LIST), bf16),
            pltpu.VMEM((2, PIX, LIST), f32),
            pltpu.VMEM((2, PIX, 2 * LIST), bf16),
            pltpu.VMEM((2, PIX, LIST), f32),
            pltpu.VMEM((2, PIX, LIST), f32),
            pltpu.VMEM((2, 2 * PIX, LIST), bf16),
            pltpu.VMEM((2, PIX, 2 * LIST), bf16),
        ],
        4,
        smem=1,
    )(meta, rows, lists[0], image_cot[0])
    returned = exchange_rows(slot_grads, GRAD_ROWS)
    param_grad, camera_grad = call(
        pull_kernel,
        "pull",
        (
            jax.ShapeDtypeStruct((59, OWNED), f32),
            jax.ShapeDtypeStruct((N_IMG, 10), f32),
        ),
        [
            pltpu.VMEM((N_GRAD, N_IMG, N_TILE * CAP), f32),
            pltpu.VMEM((N_IMG, N_TILE * CAP), jnp.int32),
            pltpu.VMEM((16 * N_GRAD, 2 * N_TILE * CAP), bf16),
            pltpu.VMEM((N_IMG * 16 * N_GRAD, LANES), f32),
            pltpu.VMEM((24, OWNED), f32),
        ],
        9,
        smem=1,
    )(meta, returned, asked, feats, table, log_scales, quat_w, quat_v, cameras)
    return (rendered[None], param_grad, camera_grad)


def solution(mesh):
    own = P(None, ALL)
    return jax.shard_map(
        local,
        mesh=mesh,
        in_specs=(
            own,
            own,
            own,
            own,
            own,
            own,
            P(),
            P("img", "tile", None, None, None),
            P("img", "tile", None),
            P("img", "tile"),
            P("img", None, "tile", None),
        ),
        out_specs=(P("img", None, "tile", None), own, P()),
        check_vma=False,
    )
```

```python
import jax
import jax.numpy as jnp
from jax import lax
from jax.experimental import pallas as pl
from jax.experimental.pallas import tpu as pltpu
from jax.sharding import PartitionSpec as P

TILE_SIDE = 16
TW = 16
ALL = ("img", "tile")
ORDER = ("tile", "img")
N_IMG = 8
N_TILE = 32
CAP = 16
OWNED = 2048
LIST = 256
TILES_HERE = 8
PIX = 256
LANES = 128
N_FEAT = 24
N_USED = 9
N_GRAD = 9
FEAT_ROWS = 3
GRAD_ROWS = 2

sh_first = 0.28209479177387814
sh_second = 0.4886025119029199
sh_third = (
    1.0925484305920792,
    -1.0925484305920792,
    0.31539156525252005,
    -1.0925484305920792,
    0.5462742152960396,
)
sh_fourth = (
    -0.5900435899266435,
    2.890611442640554,
    -0.4570457994644658,
    0.3731763325901154,
    -0.4570457994644658,
    1.445305721320277,
    -0.5900435899266435,
)
dilation = 0.3
LOG2E = 1.4426950408889634
f32 = jnp.float32
bf16 = jnp.bfloat16


def harmonics_of(polar, azimuth):
    sin_p, cos_p = jnp.sin(polar), jnp.cos(polar)
    x = sin_p * jnp.cos(azimuth)
    y = sin_p * jnp.sin(azimuth)
    z = cos_p
    xx, yy, zz = x * x, y * y, z * z
    return [
        sh_first + 0.0 * x,
        -sh_second * y,
        sh_second * z,
        -sh_second * x,
        sh_third[0] * x * y,
        sh_third[1] * y * z,
        sh_third[2] * (2.0 * zz - xx - yy),
        sh_third[3] * x * z,
        sh_third[4] * (xx - yy),
        sh_fourth[0] * y * (3.0 * xx - yy),
        sh_fourth[1] * x * y * z,
        sh_fourth[2] * y * (4.0 * zz - xx - yy),
        sh_fourth[3] * z * (2.0 * zz - 3.0 * xx - 3.0 * yy),
        sh_fourth[4] * x * (4.0 * zz - xx - yy),
        sh_fourth[5] * z * (xx - yy),
        sh_fourth[6] * x * (xx - 3.0 * yy),
    ]


def shape_matrix(log_scales, quat):
    w, x, y, z = quat
    norm = jnp.sqrt(w * w + x * x + y * y + z * z)
    w, x, y, z = w / norm, x / norm, y / norm, z / norm
    rotation = (
        (1.0 - 2.0 * (y * y + z * z), 2.0 * (x * y - w * z), 2.0 * (x * z + w * y)),
        (2.0 * (x * y + w * z), 1.0 - 2.0 * (x * x + z * z), 2.0 * (y * z - w * x)),
        (2.0 * (x * z - w * y), 2.0 * (y * z + w * x), 1.0 - 2.0 * (x * x + y * y)),
    )
    stretch = [jnp.exp(v) for v in log_scales]
    return [[rotation[r][c] * stretch[c] for c in range(3)] for r in range(3)]


def turn_groups(vregs):
    group = lax.broadcasted_iota(jnp.int32, (8, LANES), 1) // CAP
    work = [vregs[-k % 8] for k in range(8)]
    for bit in (1, 2, 4):
        move = (group & bit) != 0
        work = [jnp.where(move, work[(k - bit) % 8], work[k]) for k in range(8)]
    return work


def rotate(value, groups):
    if isinstance(groups, int):
        shift = CAP * groups % LANES
        return value if shift == 0 else pltpu.roll(value, shift, 1)
    return pltpu.roll(value, (CAP * groups) & (LANES - 1), 1)


def swap_groups(vregs, turned=0, leave=False):
    vregs = turn_groups([rotate(v, i + LANES // CAP - turned) for i, v in enumerate(vregs)])
    return vregs if leave else [rotate(v, -g) for g, v in enumerate(vregs)]


def lane_take(table, lanes):
    return jnp.take_along_axis(table, lanes, axis=1, mode="promise_in_bounds")


def halves(value):
    high = value.astype(bf16)
    return high, (value - high.astype(f32)).astype(bf16)


def dot(a, b):
    return lax.dot_general(a, b, (((1,), (0,)), ((), ())), preferred_element_type=f32)


def dot_t(a, b):
    return lax.dot_general(a, b, (((1,), (1,)), ((), ())), preferred_element_type=f32)


PROJECT_CHUNK = 256


def ask_kernel(wanted, out):
    padded = jnp.concatenate([wanted[...], jnp.zeros((LANES, LANES - N_TILE), jnp.int32)], axis=1)
    turned = jnp.transpose(padded)
    for b in range(N_TILE):
        out[8 * b : 8 * b + 8, :] = jnp.broadcast_to(turned[b : b + 1, :], (8, LANES))


def asked_lanes(asked, my_img):
    group = lax.broadcasted_iota(jnp.int32, (8, LANES), 1) // CAP
    base = LANES - CAP * my_img
    result = []
    for q in range(4):
        total = None
        for k in range(8):
            piece = pltpu.roll(asked[8 * (8 * q + k) : 8 * (8 * q + k) + 8, :], (base + CAP * k) & (LANES - 1), 1)
            total = piece if k == 0 else jnp.where(group == k, piece, total)
        result.append(total)
    return result


def project(means, log_scales, quat_w, quat_v, opacity, sh, cam, out, harm):
    column = [jnp.broadcast_to(cam[:, m : m + 1], (N_IMG, PROJECT_CHUNK)) for m in range(8)]

    def chunk(h, carry):
        at = pl.ds(pl.multiple_of(h * PROJECT_CHUNK, PROJECT_CHUNK), PROJECT_CHUNK)
        mean = [means[c : c + 1, at] for c in range(3)]
        quat = [quat_w[0:1, at]] + [quat_v[c : c + 1, at] for c in range(3)]
        m = shape_matrix([log_scales[c : c + 1, at] for c in range(3)], quat)
        for row in range(2):
            a = column[3 * row : 3 * row + 3]
            out[row, :, at] = a[0] * mean[0] + a[1] * mean[1] + a[2] * mean[2] + column[6 + row]
        p = [
            [
                sum(column[3 * row + r] * m[r][c] for r in range(3))
                for c in range(3)
            ]
            for row in range(2)
        ]
        s00 = p[0][0] * p[0][0] + p[0][1] * p[0][1] + p[0][2] * p[0][2] + dilation
        s01 = p[0][0] * p[1][0] + p[0][1] * p[1][1] + p[0][2] * p[1][2]
        s11 = p[1][0] * p[1][0] + p[1][1] * p[1][1] + p[1][2] * p[1][2] + dilation
        det = s00 * s11 - s01 * s01
        out[2, :, at] = s11 / det
        out[3, :, at] = -s01 / det
        out[4, :, at] = s00 / det
        base = 1.0 / (1.0 + jnp.exp(-opacity[0:1, at]))
        out[5, :, at] = jnp.broadcast_to(base, (N_IMG, PROJECT_CHUNK))
        for c in range(3):
            out[9 + c, :, at] = jnp.broadcast_to(mean[c], (N_IMG, PROJECT_CHUNK))
            for row in range(2):
                out[12 + 3 * row + c, :, at] = (
                    m[c][0] * p[row][0] + m[c][1] * p[row][1] + m[c][2] * p[row][2]
                )
        for base_row, first, start in ((6, 0, 0.5), (18, 16, 0.0), (21, 32, 0.0)):
            total = [jnp.full((N_IMG, PROJECT_CHUNK), start, f32) for _ in range(3)]
            for b in range(16):
                y = jnp.concatenate([harm[first + b]] * (PROJECT_CHUNK // LANES), axis=1)
                for k in range(3):
                    total[k] = total[k] + y * sh[16 * k + b : 16 * k + b + 1, at]
            for k in range(3):
                out[base_row + k, :, at] = total[k]
        return carry

    lax.fori_loop(0, OWNED // PROJECT_CHUNK, chunk, 0)


def project_kernel(*refs):
    sources, (feats, table), rest = refs[:7], refs[7:9], refs[9:]
    harm, held, sems = rest[0], rest[1:8], rest[8]
    copies = [pltpu.make_async_copy(a, b, sems.at[n]) for n, (a, b) in enumerate(zip(sources, held))]
    for copy in reversed(copies):
        copy.start()
    for copy in reversed(copies):
        copy.wait()
    means, log_scales, quat_w, quat_v, opacity, sh, cam = held
    polar = jnp.broadcast_to(cam[:, 8:9], (N_IMG, LANES))
    azimuth = jnp.broadcast_to(cam[:, 9:10], (N_IMG, LANES))
    one, zero = jnp.ones_like(polar), jnp.zeros_like(polar)
    values, d_polar = jax.jvp(harmonics_of, (polar, azimuth), (one, zero))
    d_azimuth = jax.jvp(harmonics_of, (polar, azimuth), (zero, one))[1]
    lanes = lax.broadcasted_iota(jnp.int32, (N_IMG, LANES), 1)
    packed = jnp.zeros((N_IMG, LANES), f32)
    for b in range(16):
        harm[b] = values[b]
        harm[16 + b] = d_polar[b]
        harm[32 + b] = d_azimuth[b]
        packed = jnp.where(lanes == b, values[b], packed)
    table[...] = packed
    project(means, log_scales, quat_w, quat_v, opacity, sh, cam, feats, harm)


def pick_kernel(meta, asked, feats, out, index):
    for q, value in enumerate(asked_lanes(asked, meta[TILES_HERE + 1])):
        for f in range(8):
            index[8 * q + f] = rotate(value, f)

    def step(n, carry):
        g, q = n >> 2, n & 3
        picked = []
        for f in range(8):
            here = index[8 * q + f]
            low, high = here & (LANES - 1), here >> 7
            value = None
            for h in range(OWNED // LANES):
                found = lane_take(feats[8 * g + f, :, h * LANES : (h + 1) * LANES], low)
                value = found if h == 0 else jnp.where(high == h, found, value)
            picked.append(value)
        for k, row in enumerate(turn_groups(picked)):
            out[pl.ds(FEAT_ROWS * 8 * (8 * q + k) + g, 8, stride=FEAT_ROWS), :] = row
        return carry

    lax.fori_loop(0, 4 * FEAT_ROWS, step, 0, unroll=4)


def render_kernel(
    meta,
    rows,
    lists,
    cot,
    image,
    out,
    tab,
    feat,
    grads,
    slot,
    upper,
    lower,
    al_s,
    lk_s,
    lb_s,
    s_s,
    w_s,
    sw_s,
):
    tile_base = meta[TILES_HERE] * TILES_HERE
    turned = meta[TILES_HERE] & 7

    def sort_rows(n, carry):
        g, q = n >> 2, n & 3
        pieces = [
            rows[pl.ds(FEAT_ROWS * 8 * (8 * q + k) + g, 8, stride=FEAT_ROWS), :] for k in range(8)
        ]
        pieces = swap_groups(pieces, turned)
        for f in range(8):
            tab[8 * g + f, pl.ds(pl.multiple_of(8 * q, 8), 8), :] = pieces[f]
        return carry

    lax.fori_loop(0, 4 * FEAT_ROWS, sort_rows, 0, unroll=4)
    entry_lane = [lists[:, h * LANES : (h + 1) * LANES] & (LANES - 1) for h in range(2)]
    entry_chunk = []
    for h in range(2):
        s = lists[:, h * LANES : (h + 1) * LANES]
        entry_chunk.append(((s >> 7) & 3) * 8 + (s >> 9))

    def gather(ch, carry):
        new = list(carry)
        for h in range(2):
            hit = entry_chunk[h] == ch
            for f in range(N_USED):
                row = jnp.broadcast_to(tab[f, pl.ds(ch, 1), :], (8, LANES))
                new[2 * f + h] = jnp.where(hit, lane_take(row, entry_lane[h]), carry[2 * f + h])
        return tuple(new)

    zero = jnp.zeros((8, LANES), f32)
    found = lax.fori_loop(0, 32, gather, tuple([zero] * (2 * N_USED)), unroll=8)
    for f in range(N_USED):
        for h in range(2):
            feat[f, :, h * LANES : (h + 1) * LANES] = found[2 * f + h]
    ri = lax.broadcasted_iota(jnp.int32, (LIST, LIST), 0)
    ci = lax.broadcasted_iota(jnp.int32, (LIST, LIST), 1)
    up = (ri < ci).astype(f32).astype(bf16)
    lo = (ri > ci).astype(f32).astype(bf16)
    for part in range(2):
        upper[part * LIST : (part + 1) * LIST, :] = up
        lower[part * LIST : (part + 1) * LIST, :] = lo
    slot[...] = jnp.zeros_like(slot)
    lane = lax.broadcasted_iota(jnp.int32, (1, LIST), 1)
    px = lax.broadcasted_iota(jnp.int32, (8, LIST), 0).astype(f32) - 7.5
    ch_iota = lax.broadcasted_iota(jnp.int32, (32, LIST), 0)
    lane_iota = lax.broadcasted_iota(jnp.int32, (LANES, LIST), 0)

    def row8(v):
        return jnp.broadcast_to(v, (8, LIST))

    def pair(pair_index, carry):
        tiles = [2 * pair_index, 2 * pair_index + 1]
        state = []
        for p in range(2):
            j = tiles[p]
            number = tile_base + j
            centre_x = (TILE_SIDE * (number % TW)).astype(f32) + (0.5 * TILE_SIDE - 0.5 * TILE_SIDE * TW)
            centre_y = (TILE_SIDE * (number // TW)).astype(f32) + (0.5 * TILE_SIDE - 0.5 * TILE_SIDE * TW)
            at = pl.ds(j, 1)
            ux = feat[0, at, :] - centre_x
            uy = row8(feat[1, at, :] - centre_y)
            ca, cb, cc = feat[2, at, :], feat[3, at, :], feat[4, at, :]
            op = row8(jnp.where(lane < meta[j], feat[5, at, :], 0.0))
            cc = row8(cc * (-0.5 * LOG2E))
            ux, na, nb = row8(ux), row8(ca * (-0.5 * LOG2E)), row8(cb * (-LOG2E))
            dx = [px - ux, px + (8.0 - ux)]
            na = [na * d * d for d in dx]
            nb = [nb * d for d in dx]
            colours = jnp.concatenate([feat[6 + k, at, :] for k in range(3)], axis=0)
            cots = jnp.concatenate([cot[k, at, :] for k in range(3)], axis=0)
            col_h, col_l, cot_h, cot_l = [v.astype(f32) for v in halves(colours) + halves(cots)]
            pad = jnp.zeros((4, LIST), f32)
            cot_k = jnp.concatenate([cot_h, cot_h, cot_l, cot_l, pad], axis=0)
            col_k = jnp.concatenate([col_h, col_l, col_h, col_l, pad], axis=0).astype(bf16)
            s_s[p] = dot(jnp.transpose(cot_k).astype(bf16), col_k)
            for py in range(TILE_SIDE):
                r = slice(TILE_SIDE * py, TILE_SIDE * (py + 1))
                dy = (py - 7.5) - uy
                cy = cc * dy * dy
                alpha = jnp.concatenate(
                    [op * jnp.exp2((na[h] + cy) + nb[h] * dy) for h in range(2)], axis=0
                )
                al_s[p, r, :] = alpha
                hi, low = halves(jnp.log2(1.0 - alpha))
                lk_s[p, r, 0:LIST] = hi
                lk_s[p, r, LIST : 2 * LIST] = low
            lb_s[p] = dot(lk_s[p], upper[...])
            state.append((at, uy, dx, col_h, col_l, cot_h, cot_l))
        for p in range(2):
            for py in range(TILE_SIDE):
                r = slice(TILE_SIDE * py, TILE_SIDE * (py + 1))
                w = al_s[p, r, :] * jnp.exp2(lb_s[p, r, :])
                hi, low = halves(w)
                w_s[p, r, :] = hi
                w_s[p, PIX + TILE_SIDE * py : PIX + TILE_SIDE * (py + 1), :] = low
                sw = s_s[p, r, :] * w
                s_s[p, r, :] = sw
                hi, low = halves(sw)
                sw_s[p, r, 0:LIST] = hi
                sw_s[p, r, LIST : 2 * LIST] = low
            lb_s[p] = dot(sw_s[p], lower[...])
        for p in range(2):
            at, uy, dx, col_h, col_l, cot_h, cot_l = state[p]
            pad2 = jnp.zeros((2, LIST), f32)
            col_rows = jnp.concatenate([col_h, col_l, pad2], axis=0).astype(bf16)
            shown = dot_t(col_rows, w_s[p, 0:PIX, :]) + dot_t(col_rows, w_s[p, PIX : 2 * PIX, :])
            for k in range(3):
                image[k, at, :] = shown[k : k + 1, :] + shown[3 + k : 4 + k, :]
            cot_rows = jnp.concatenate([cot_h, cot_l, pad2], axis=0).astype(bf16)
            gcol = dot(jnp.concatenate([cot_rows, cot_rows], axis=1), w_s[p])
            acc = [[None, None] for _ in range(3)]
            for py in range(TILE_SIDE):
                dy = (py - 7.5) - uy
                for h in range(2):
                    r = slice(TILE_SIDE * py + 8 * h, TILE_SIDE * py + 8 * h + 8)
                    alpha = al_s[p, r, :]
                    g = s_s[p, r, :] - lb_s[p, r, :] * (alpha / (1.0 - alpha))
                    gy = g * dy
                    for n, v in enumerate((g, gy, gy * dy)):
                        acc[n][h] = v if py == 0 else acc[n][h] + v

            def down(a, b):
                return jnp.sum(a + b, axis=0, keepdims=True)

            xg = [dx[h] * acc[0][h] for h in range(2)]
            grad = [
                down(acc[0][0], acc[0][1]),
                down(xg[0], xg[1]),
                down(acc[1][0], acc[1][1]),
                down(dx[0] * xg[0], dx[1] * xg[1]),
                down(dx[0] * acc[1][0], dx[1] * acc[1][1]),
                down(acc[2][0], acc[2][1]),
            ] + [gcol[k : k + 1, :] + gcol[3 + k : 4 + k, :] for k in range(3)]
            s = lists[at, :]
            chunk_hit = ch_iota == (((s >> 7) & 3) * 8 + (s >> 9))
            for f in range(N_GRAD):
                hi, low = halves(jnp.where(chunk_hit, grad[f], 0.0))
                grads[p, 32 * f : 32 * (f + 1), 0:LIST] = hi
                grads[p, 32 * f : 32 * (f + 1), LIST : 2 * LIST] = low
            lane_hit = (lane_iota == (s & (LANES - 1))).astype(f32).astype(bf16)
            slot[...] += dot_t(grads[p], jnp.concatenate([lane_hit, lane_hit], axis=1))
        return carry

    lax.fori_loop(0, TILES_HERE // 2, pair, 0)

    terms = [jnp.zeros((8, LANES), f32) for _ in range(10)]
    for q in range(4):
        r = slice(8 * q, 8 * q + 8)
        ca, cb, cc = tab[2, r, :], tab[3, r, :], tab[4, r, :]
        gr = [slot[32 * f + 8 * q : 32 * f + 8 * q + 8, :] for f in range(N_GRAD)]
        du = (ca * gr[1] + cb * gr[2], cb * gr[1] + cc * gr[2])
        h00, h01, h11 = conic_pull(ca, cb, cc, gr[3], gr[4], gr[5])
        for c in range(3):
            mean, n0, n1 = tab[9 + c, r, :], tab[12 + c, r, :], tab[15 + c, r, :]
            terms[c] += du[0] * mean + 2.0 * (h00 * n0 + h01 * n1)
            terms[3 + c] += du[1] * mean + 2.0 * (h01 * n0 + h11 * n1)
            terms[8] += gr[6 + c] * tab[18 + c, r, :]
            terms[9] += gr[6 + c] * tab[21 + c, r, :]
        terms[6] += du[0]
        terms[7] += du[1]
    lanes = lax.broadcasted_iota(jnp.int32, (8, LANES), 1)
    share = jnp.zeros((8, LANES), f32)
    for m in range(10):
        total = jnp.sum(jnp.sum(terms[m], axis=0, keepdims=True), axis=1, keepdims=True)
        share = jnp.where(lanes == CAP + m, jnp.broadcast_to(total, (8, LANES)), share)
    group = lanes // CAP
    shares = [rotate(share, k) for k in range(8)]
    for q in range(4):
        pieces = swap_groups([slot[32 * f + 8 * q : 32 * f + 8 * q + 8, :] for f in range(8)], leave=True)
        last = slot[32 * 8 + 8 * q : 32 * 8 + 8 * q + 8, :]
        for k in range(8):
            first_row = GRAD_ROWS * 8 * (8 * q + k)
            out[pl.ds(first_row, 8, stride=GRAD_ROWS), :] = pieces[k]
            out[pl.ds(first_row + 1, 8, stride=GRAD_ROWS), :] = jnp.where(group == k, last, shares[k])


def conic_pull(ca, cb, cc, qxx, qxy, qyy):
    t00, t01 = ca * qxx + cb * qxy, ca * qxy + cb * qyy
    t10, t11 = cb * qxx + cc * qxy, cb * qxy + cc * qyy
    return 0.5 * (t00 * ca + t01 * cb), 0.5 * (t00 * cb + t01 * cc), 0.5 * (t10 * cb + t11 * cc)


PULL_CHUNK = 512


def pull_kernel(
    meta, returned, asked, feats, table, log_scales, quat_w, quat_v, cam, out, cam_out, row_s, idx_s, lhs_s, sum_s, gc_s
):
    index = asked_lanes(asked, meta[TILES_HERE + 1])
    for q in range(4):
        idx_s[:, q * LANES : (q + 1) * LANES] = index[q]
    group = lax.broadcasted_iota(jnp.int32, (8, LANES), 1) // CAP
    turned = meta[TILES_HERE] & 7
    camera = jnp.zeros((8, LANES), f32)
    for q in range(4):
        pieces = [returned[pl.ds(GRAD_ROWS * 8 * (8 * q + k), 8, stride=GRAD_ROWS), :] for k in range(8)]
        pieces = swap_groups(pieces, turned)
        for f in range(8):
            row_s[f, :, q * LANES : (q + 1) * LANES] = pieces[f]
        last = None
        for k in range(8):
            piece = returned[pl.ds(GRAD_ROWS * 8 * (8 * q + k) + 1, 8, stride=GRAD_ROWS), :]
            camera = camera + piece
            moved = rotate(piece, k + 8 - turned)
            last = moved if k == 0 else jnp.where(group == k, moved, last)
        row_s[8, :, q * LANES : (q + 1) * LANES] = last
    cam_out[...] = rotate(camera, 7 - turned)[:, 0:10]

    slots = N_TILE * CAP
    high_iota = lax.broadcasted_iota(jnp.int32, (16, slots), 0)
    lane_iota = lax.broadcasted_iota(jnp.int32, (LANES, slots), 0)

    def image(i, carry):
        at = pl.ds(i, 1)
        s = idx_s[at, :]
        high_hit = high_iota == (s >> 7)
        lane_hit = (lane_iota == (s & (LANES - 1))).astype(f32).astype(bf16)
        for f in range(N_GRAD):
            hi, low = halves(jnp.where(high_hit, row_s[f, at, :], 0.0))
            lhs_s[16 * f : 16 * (f + 1), 0:slots] = hi
            lhs_s[16 * f : 16 * (f + 1), slots : 2 * slots] = low
        sum_s[pl.ds(pl.multiple_of(i * (16 * N_GRAD), 16), 16 * N_GRAD), :] = dot_t(
            lhs_s[...], jnp.concatenate([lane_hit, lane_hit], axis=1)
        )
        return carry

    lax.fori_loop(0, N_IMG, image, 0, unroll=8)

    column = [jnp.broadcast_to(cam[:, m : m + 1], (N_IMG, PULL_CHUNK)) for m in range(6)]

    def chunk(h, carry):
        at = pl.ds(pl.multiple_of(h * PULL_CHUNK, PULL_CHUNK), PULL_CHUNK)
        parts = PULL_CHUNK // LANES
        gr = [
            jnp.concatenate(
                [sum_s[pl.ds(16 * f + h * parts + e, 8, stride=16 * N_GRAD), :] for e in range(parts)],
                axis=1,
            )
            for f in range(N_GRAD)
        ]
        ca, cb, cc = feats[2, :, at], feats[3, :, at], feats[4, :, at]
        du = (ca * gr[1] + cb * gr[2], cb * gr[1] + cc * gr[2])
        h00, h01, h11 = conic_pull(ca, cb, cc, gr[3], gr[4], gr[5])
        a0, a1 = column[0:3], column[3:6]

        def over_images(v):
            return jnp.sum(v, axis=0, keepdims=True)

        for c in range(3):
            out[c : c + 1, at] = over_images(a0[c] * du[0] + a1[c] * du[1])
        t0 = [h00 * a0[c] + h01 * a1[c] for c in range(3)]
        t1 = [h01 * a0[c] + h11 * a1[c] for c in range(3)]
        v = [[None] * 3 for _ in range(3)]
        for c in range(3):
            for d in range(c, 3):
                v[c][d] = v[d][c] = over_images(t0[c] * a0[d] + t1[c] * a1[d])
        ls = [log_scales[c : c + 1, at] for c in range(3)]
        quat = [quat_w[0:1, at]] + [quat_v[c : c + 1, at] for c in range(3)]
        m, pull = jax.vjp(shape_matrix, ls, quat)
        dm = [[2.0 * sum(v[r][d] * m[d][c] for d in range(3)) for c in range(3)] for r in range(3)]
        dls, dquat = pull(dm)
        for c in range(3):
            out[3 + c : 4 + c, at] = dls[c]
        for c in range(4):
            out[6 + c : 7 + c, at] = dquat[c]
        base = feats[5, 0:1, at]
        out[10:11, at] = over_images(gr[0]) * (1.0 - base)
        for k in range(3):
            gc_s[8 * k : 8 * k + 8, at] = gr[6 + k]
        return carry

    lax.fori_loop(0, OWNED // PULL_CHUNK, chunk, 0)

    y_h, y_l = halves(jnp.transpose(table[...])[0:16, :])
    y_all = jnp.concatenate([y_h.astype(f32), y_h.astype(f32), y_l.astype(f32), y_l.astype(f32)], axis=1).astype(bf16)
    for k in range(3):
        g_h, g_l = halves(gc_s[8 * k : 8 * k + 8, :])
        g_all = jnp.concatenate([g_h.astype(f32), g_l.astype(f32), g_h.astype(f32), g_l.astype(f32)], axis=0).astype(bf16)
        out[11 + 16 * k : 27 + 16 * k, :] = dot(y_all, g_all)


def whole(memory=pltpu.VMEM):
    return pl.BlockSpec(memory_space=memory)


def call(kernel, name, out_shape, scratch, n_in, smem=0, memory=pltpu.VMEM, cost=None):
    return pl.pallas_call(
        kernel,
        name=name,
        out_shape=out_shape,
        in_specs=[whole(pltpu.SMEM)] * smem + [whole(memory)] * (n_in - smem),
        out_specs=jax.tree.map(lambda _: whole(), out_shape),
        scratch_shapes=scratch,
        cost_estimate=cost,
        compiler_params=pltpu.CompilerParams(vmem_limit_bytes=32 << 20),
    )


def exchange(array):
    return lax.all_to_all(array, ORDER, split_axis=0, concat_axis=0, tiled=True)


def exchange_rows(array, rows):
    shape = array.shape
    return exchange(array.reshape(-1, 1, rows * LANES)).reshape(shape)


def local(
    means, log_scales, quat_w, quat_v, opacity, sh_coeffs, cameras, requests, lists, counts, image_cot
):
    devices = N_IMG * N_TILE
    by_owner = jnp.transpose(requests.reshape(N_IMG, N_TILE, CAP), (0, 2, 1)).reshape(N_IMG * CAP, N_TILE)
    wanted = call(ask_kernel, "ask", jax.ShapeDtypeStruct((devices, LANES), jnp.int32), [], 1)(by_owner)
    asked = exchange_rows(wanted, 1)
    meta = jnp.concatenate(
        [counts[0], jnp.stack([lax.axis_index("tile"), lax.axis_index("img")]).astype(jnp.int32)]
    )
    owned = [
        pltpu.with_memory_space_constraint(a, pltpu.HBM)
        for a in (means, log_scales, quat_w, quat_v, opacity, sh_coeffs, cameras)
    ]
    feats, table = call(
        project_kernel,
        "project",
        (jax.ShapeDtypeStruct((N_FEAT, N_IMG, OWNED), f32), jax.ShapeDtypeStruct((N_IMG, LANES), f32)),
        [pltpu.VMEM((48, N_IMG, LANES), f32)]
        + [pltpu.VMEM(a.shape, f32) for a in owned]
        + [pltpu.SemaphoreType.DMA((7,))],
        7,
        memory=pltpu.HBM,
        cost=pl.CostEstimate(flops=20_000_000, transcendentals=0, bytes_accessed=1_000_000),
    )(*owned)
    asked, feats, meta = lax.optimization_barrier((asked, feats, meta))
    packed = call(
        pick_kernel,
        "pick",
        jax.ShapeDtypeStruct((FEAT_ROWS * devices, LANES), f32),
        [pltpu.VMEM((32, N_IMG, LANES), jnp.int32)],
        3,
        smem=1,
    )(meta, asked, feats)
    rows = exchange_rows(packed, FEAT_ROWS)
    rendered, slot_grads = call(
        render_kernel,
        "render",
        (
            jax.ShapeDtypeStruct((3, TILES_HERE, PIX), f32),
            jax.ShapeDtypeStruct((GRAD_ROWS * devices, LANES), f32),
        ),
        [
            pltpu.VMEM((N_FEAT, 32, LANES), f32),
            pltpu.VMEM((N_USED, 8, LIST), f32),
            pltpu.VMEM((2, 32 * N_GRAD, 2 * LIST), bf16),
            pltpu.VMEM((32 * N_GRAD, LANES), f32),
            pltpu.VMEM((2 * LIST, LIST), bf16),
            pltpu.VMEM((2 * LIST, LIST), bf16),
            pltpu.VMEM((2, PIX, LIST), f32),
            pltpu.VMEM((2, PIX, 2 * LIST), bf16),
            pltpu.VMEM((2, PIX, LIST), f32),
            pltpu.VMEM((2, PIX, LIST), f32),
            pltpu.VMEM((2, 2 * PIX, LIST), bf16),
            pltpu.VMEM((2, PIX, 2 * LIST), bf16),
        ],
        4,
        smem=1,
    )(meta, rows, lists[0], image_cot[0])
    returned = exchange_rows(slot_grads, GRAD_ROWS)
    param_grad, camera_grad = call(
        pull_kernel,
        "pull",
        (
            jax.ShapeDtypeStruct((59, OWNED), f32),
            jax.ShapeDtypeStruct((N_IMG, 10), f32),
        ),
        [
            pltpu.VMEM((N_GRAD, N_IMG, N_TILE * CAP), f32),
            pltpu.VMEM((N_IMG, N_TILE * CAP), jnp.int32),
            pltpu.VMEM((16 * N_GRAD, 2 * N_TILE * CAP), bf16),
            pltpu.VMEM((N_IMG * 16 * N_GRAD, LANES), f32),
            pltpu.VMEM((24, OWNED), f32),
        ],
        9,
        smem=1,
    )(meta, returned, asked, feats, table, log_scales, quat_w, quat_v, cameras)
    return (rendered[None], param_grad, camera_grad)


def solution(mesh):
    own = P(None, ALL)
    return jax.shard_map(
        local,
        mesh=mesh,
        in_specs=(
            own,
            own,
            own,
            own,
            own,
            own,
            P(),
            P("img", "tile", None, None, None),
            P("img", "tile", None),
            P("img", "tile"),
            P("img", None, "tile", None),
        ),
        out_specs=(P("img", None, "tile", None), own, P()),
        check_vma=False,
    )
```

```python
import jax
import jax.numpy as jnp
from jax import lax
from jax.experimental import pallas as pl
from jax.experimental.pallas import tpu as pltpu
from jax.sharding import PartitionSpec as P

TILE_SIDE = 16
TW = 16
ALL = ("img", "tile")
ORDER = ("tile", "img")
N_IMG = 8
N_TILE = 32
CAP = 16
OWNED = 2048
LIST = 256
TILES_HERE = 8
PIX = 256
LANES = 128
N_FEAT = 24
N_USED = 9
N_GRAD = 9
FEAT_ROWS = 3
GRAD_ROWS = 2

sh_first = 0.28209479177387814
sh_second = 0.4886025119029199
sh_third = (
    1.0925484305920792,
    -1.0925484305920792,
    0.31539156525252005,
    -1.0925484305920792,
    0.5462742152960396,
)
sh_fourth = (
    -0.5900435899266435,
    2.890611442640554,
    -0.4570457994644658,
    0.3731763325901154,
    -0.4570457994644658,
    1.445305721320277,
    -0.5900435899266435,
)
dilation = 0.3
LOG2E = 1.4426950408889634
f32 = jnp.float32
bf16 = jnp.bfloat16


def harmonics_of(polar, azimuth):
    sin_p, cos_p = jnp.sin(polar), jnp.cos(polar)
    x = sin_p * jnp.cos(azimuth)
    y = sin_p * jnp.sin(azimuth)
    z = cos_p
    xx, yy, zz = x * x, y * y, z * z
    return [
        sh_first + 0.0 * x,
        -sh_second * y,
        sh_second * z,
        -sh_second * x,
        sh_third[0] * x * y,
        sh_third[1] * y * z,
        sh_third[2] * (2.0 * zz - xx - yy),
        sh_third[3] * x * z,
        sh_third[4] * (xx - yy),
        sh_fourth[0] * y * (3.0 * xx - yy),
        sh_fourth[1] * x * y * z,
        sh_fourth[2] * y * (4.0 * zz - xx - yy),
        sh_fourth[3] * z * (2.0 * zz - 3.0 * xx - 3.0 * yy),
        sh_fourth[4] * x * (4.0 * zz - xx - yy),
        sh_fourth[5] * z * (xx - yy),
        sh_fourth[6] * x * (xx - 3.0 * yy),
    ]


def shape_matrix(log_scales, quat):
    w, x, y, z = quat
    norm = jnp.sqrt(w * w + x * x + y * y + z * z)
    w, x, y, z = w / norm, x / norm, y / norm, z / norm
    rotation = (
        (1.0 - 2.0 * (y * y + z * z), 2.0 * (x * y - w * z), 2.0 * (x * z + w * y)),
        (2.0 * (x * y + w * z), 1.0 - 2.0 * (x * x + z * z), 2.0 * (y * z - w * x)),
        (2.0 * (x * z - w * y), 2.0 * (y * z + w * x), 1.0 - 2.0 * (x * x + y * y)),
    )
    stretch = [jnp.exp(v) for v in log_scales]
    return [[rotation[r][c] * stretch[c] for c in range(3)] for r in range(3)]


def turn_groups(vregs):
    group = lax.broadcasted_iota(jnp.int32, (8, LANES), 1) // CAP
    work = [vregs[-k % 8] for k in range(8)]
    for bit in (1, 2, 4):
        move = (group & bit) != 0
        work = [jnp.where(move, work[(k - bit) % 8], work[k]) for k in range(8)]
    return work


def rotate(value, groups):
    if isinstance(groups, int):
        shift = CAP * groups % LANES
        return value if shift == 0 else pltpu.roll(value, shift, 1)
    return pltpu.roll(value, (CAP * groups) & (LANES - 1), 1)


def swap_groups(vregs, turned=0, leave=False):
    vregs = turn_groups([rotate(v, i + LANES // CAP - turned) for i, v in enumerate(vregs)])
    return vregs if leave else [rotate(v, -g) for g, v in enumerate(vregs)]


def lane_take(table, lanes):
    return jnp.take_along_axis(table, lanes, axis=1, mode="promise_in_bounds")


def halves(value):
    high = value.astype(bf16)
    return high, (value - high.astype(f32)).astype(bf16)


def row_parts(row):
    return halves(jnp.broadcast_to(row, (16, row.shape[1])))


def dot(a, b):
    return lax.dot_general(a, b, (((1,), (0,)), ((), ())), preferred_element_type=f32)


def dot_t(a, b):
    return lax.dot_general(a, b, (((1,), (1,)), ((), ())), preferred_element_type=f32)


PROJECT_CHUNK = 256


def ask_kernel(wanted, out):
    padded = jnp.concatenate([wanted[...], jnp.zeros((LANES, LANES - N_TILE), jnp.int32)], axis=1)
    turned = jnp.transpose(padded)
    for b in range(N_TILE):
        out[8 * b : 8 * b + 8, :] = jnp.broadcast_to(turned[b : b + 1, :], (8, LANES))


def asked_lanes(asked, my_img):
    group = lax.broadcasted_iota(jnp.int32, (8, LANES), 1) // CAP
    base = LANES - CAP * my_img
    result = []
    for q in range(4):
        total = None
        for k in range(8):
            piece = pltpu.roll(asked[8 * (8 * q + k) : 8 * (8 * q + k) + 8, :], (base + CAP * k) & (LANES - 1), 1)
            total = piece if k == 0 else jnp.where(group == k, piece, total)
        result.append(total)
    return result


def project(means, log_scales, quat_w, quat_v, opacity, sh, cam, out, harm):
    column = [jnp.broadcast_to(cam[:, m : m + 1], (N_IMG, PROJECT_CHUNK)) for m in range(8)]

    def chunk(h, carry):
        at = pl.ds(pl.multiple_of(h * PROJECT_CHUNK, PROJECT_CHUNK), PROJECT_CHUNK)
        mean = [means[c : c + 1, at] for c in range(3)]
        quat = [quat_w[0:1, at]] + [quat_v[c : c + 1, at] for c in range(3)]
        m = shape_matrix([log_scales[c : c + 1, at] for c in range(3)], quat)
        for row in range(2):
            a = column[3 * row : 3 * row + 3]
            out[row, :, at] = a[0] * mean[0] + a[1] * mean[1] + a[2] * mean[2] + column[6 + row]
        p = [
            [
                sum(column[3 * row + r] * m[r][c] for r in range(3))
                for c in range(3)
            ]
            for row in range(2)
        ]
        s00 = p[0][0] * p[0][0] + p[0][1] * p[0][1] + p[0][2] * p[0][2] + dilation
        s01 = p[0][0] * p[1][0] + p[0][1] * p[1][1] + p[0][2] * p[1][2]
        s11 = p[1][0] * p[1][0] + p[1][1] * p[1][1] + p[1][2] * p[1][2] + dilation
        det = s00 * s11 - s01 * s01
        out[2, :, at] = s11 / det
        out[3, :, at] = -s01 / det
        out[4, :, at] = s00 / det
        base = 1.0 / (1.0 + jnp.exp(-opacity[0:1, at]))
        out[5, :, at] = jnp.broadcast_to(base, (N_IMG, PROJECT_CHUNK))
        for c in range(3):
            out[9 + c, :, at] = jnp.broadcast_to(mean[c], (N_IMG, PROJECT_CHUNK))
            for row in range(2):
                out[12 + 3 * row + c, :, at] = (
                    m[c][0] * p[row][0] + m[c][1] * p[row][1] + m[c][2] * p[row][2]
                )
        for base_row, first, start in ((6, 0, 0.5), (18, 16, 0.0), (21, 32, 0.0)):
            total = [jnp.full((N_IMG, PROJECT_CHUNK), start, f32) for _ in range(3)]
            for b in range(16):
                y = jnp.concatenate([harm[first + b]] * (PROJECT_CHUNK // LANES), axis=1)
                for k in range(3):
                    total[k] = total[k] + y * sh[16 * k + b : 16 * k + b + 1, at]
            for k in range(3):
                out[base_row + k, :, at] = total[k]
        return carry

    lax.fori_loop(0, OWNED // PROJECT_CHUNK, chunk, 0)


def project_kernel(*refs):
    sources, (feats, table), rest = refs[:7], refs[7:9], refs[9:]
    harm, held, sems = rest[0], rest[1:8], rest[8]
    copies = [pltpu.make_async_copy(a, b, sems.at[n]) for n, (a, b) in enumerate(zip(sources, held))]
    for copy in reversed(copies):
        copy.start()
    for copy in reversed(copies):
        copy.wait()
    means, log_scales, quat_w, quat_v, opacity, sh, cam = held
    polar = jnp.broadcast_to(cam[:, 8:9], (N_IMG, LANES))
    azimuth = jnp.broadcast_to(cam[:, 9:10], (N_IMG, LANES))
    one, zero = jnp.ones_like(polar), jnp.zeros_like(polar)
    values, d_polar = jax.jvp(harmonics_of, (polar, azimuth), (one, zero))
    d_azimuth = jax.jvp(harmonics_of, (polar, azimuth), (zero, one))[1]
    lanes = lax.broadcasted_iota(jnp.int32, (N_IMG, LANES), 1)
    packed = jnp.zeros((N_IMG, LANES), f32)
    for b in range(16):
        harm[b] = values[b]
        harm[16 + b] = d_polar[b]
        harm[32 + b] = d_azimuth[b]
        packed = jnp.where(lanes == b, values[b], packed)
    table[...] = packed
    project(means, log_scales, quat_w, quat_v, opacity, sh, cam, feats, harm)


def pick_kernel(meta, asked, feats, out, index):
    for q, value in enumerate(asked_lanes(asked, meta[TILES_HERE + 1])):
        for f in range(8):
            index[8 * q + f] = rotate(value, f)

    def step(n, carry):
        g, q = n >> 2, n & 3
        picked = []
        for f in range(8):
            here = index[8 * q + f]
            low, high = here & (LANES - 1), here >> 7
            value = None
            for h in range(OWNED // LANES):
                found = lane_take(feats[8 * g + f, :, h * LANES : (h + 1) * LANES], low)
                value = found if h == 0 else jnp.where(high == h, found, value)
            picked.append(value)
        for k, row in enumerate(turn_groups(picked)):
            out[pl.ds(FEAT_ROWS * 8 * (8 * q + k) + g, 8, stride=FEAT_ROWS), :] = row
        return carry

    lax.fori_loop(0, 4 * FEAT_ROWS, step, 0, unroll=4)


def render_kernel(
    meta,
    rows,
    lists,
    cot,
    image,
    out,
    tab,
    feat,
    grads,
    slot,
    upper,
    lower,
    al_s,
    lk_s,
    lb_s,
    s_s,
    w_s,
    sw_s,
):
    tile_base = meta[TILES_HERE] * TILES_HERE
    turned = meta[TILES_HERE] & 7

    def sort_rows(n, carry):
        g, q = n >> 2, n & 3
        pieces = [
            rows[pl.ds(FEAT_ROWS * 8 * (8 * q + k) + g, 8, stride=FEAT_ROWS), :] for k in range(8)
        ]
        pieces = swap_groups(pieces, turned)
        for f in range(8):
            tab[8 * g + f, pl.ds(pl.multiple_of(8 * q, 8), 8), :] = pieces[f]
        return carry

    lax.fori_loop(0, 4 * FEAT_ROWS, sort_rows, 0, unroll=4)
    entry_lane = [lists[:, h * LANES : (h + 1) * LANES] & (LANES - 1) for h in range(2)]
    entry_chunk = []
    for h in range(2):
        s = lists[:, h * LANES : (h + 1) * LANES]
        entry_chunk.append(((s >> 7) & 3) * 8 + (s >> 9))

    def gather(ch, carry):
        new = list(carry)
        for h in range(2):
            hit = entry_chunk[h] == ch
            for f in range(N_USED):
                row = jnp.broadcast_to(tab[f, pl.ds(ch, 1), :], (8, LANES))
                new[2 * f + h] = jnp.where(hit, lane_take(row, entry_lane[h]), carry[2 * f + h])
        return tuple(new)

    zero = jnp.zeros((8, LANES), f32)
    found = lax.fori_loop(0, 32, gather, tuple([zero] * (2 * N_USED)), unroll=8)
    for f in range(N_USED):
        for h in range(2):
            feat[f, :, h * LANES : (h + 1) * LANES] = found[2 * f + h]
    ri = lax.broadcasted_iota(jnp.int32, (LIST, LIST), 0)
    ci = lax.broadcasted_iota(jnp.int32, (LIST, LIST), 1)
    up = (ri < ci).astype(f32).astype(bf16)
    lo = (ri > ci).astype(f32).astype(bf16)
    for part in range(2):
        upper[part * LIST : (part + 1) * LIST, :] = up
        lower[part * LIST : (part + 1) * LIST, :] = lo
    slot[...] = jnp.zeros_like(slot)
    lane = lax.broadcasted_iota(jnp.int32, (1, LIST), 1)
    px = lax.broadcasted_iota(jnp.int32, (8, LIST), 0).astype(f32) - 7.5
    ch_iota = lax.broadcasted_iota(jnp.int32, (32, LIST), 0)
    lane_iota = lax.broadcasted_iota(jnp.int32, (LANES, LIST), 0)

    def row8(v):
        return jnp.broadcast_to(v, (8, LIST))

    def pair(pair_index, carry):
        tiles = [2 * pair_index, 2 * pair_index + 1]
        state = []
        for p in range(2):
            j = tiles[p]
            number = tile_base + j
            centre_x = (TILE_SIDE * (number % TW)).astype(f32) + (0.5 * TILE_SIDE - 0.5 * TILE_SIDE * TW)
            centre_y = (TILE_SIDE * (number // TW)).astype(f32) + (0.5 * TILE_SIDE - 0.5 * TILE_SIDE * TW)
            at = pl.ds(j, 1)
            ux = feat[0, at, :] - centre_x
            uy = row8(feat[1, at, :] - centre_y)
            ca, cb, cc = feat[2, at, :], feat[3, at, :], feat[4, at, :]
            op = row8(jnp.where(lane < meta[j], feat[5, at, :], 0.0))
            cc = row8(cc * (-0.5 * LOG2E))
            ux, na, nb = row8(ux), row8(ca * (-0.5 * LOG2E)), row8(cb * (-LOG2E))
            dx = [px - ux, px + (8.0 - ux)]
            na = [na * d * d for d in dx]
            nb = [nb * d for d in dx]
            colours = jnp.concatenate([feat[6 + k, at, :] for k in range(3)], axis=0)
            cots = jnp.concatenate([cot[k, at, :] for k in range(3)], axis=0)
            col_h, col_l, cot_h, cot_l = [v.astype(f32) for v in halves(colours) + halves(cots)]
            pad = jnp.zeros((4, LIST), f32)
            cot_k = jnp.concatenate([cot_h, cot_h, cot_l, cot_l, pad], axis=0)
            col_k = jnp.concatenate([col_h, col_l, col_h, col_l, pad], axis=0).astype(bf16)
            s_s[p] = dot(jnp.transpose(cot_k).astype(bf16), col_k)
            for py in range(TILE_SIDE):
                r = slice(TILE_SIDE * py, TILE_SIDE * (py + 1))
                dy = (py - 7.5) - uy
                cy = cc * dy * dy
                alpha = jnp.concatenate(
                    [op * jnp.exp2((na[h] + cy) + nb[h] * dy) for h in range(2)], axis=0
                )
                al_s[p, r, :] = alpha
                hi, low = halves(jnp.log2(1.0 - alpha))
                lk_s[p, r, 0:LIST] = hi
                lk_s[p, r, LIST : 2 * LIST] = low
            state.append((at, uy, dx, col_h, col_l, cot_h, cot_l))
        for p in range(2):
            lb_s[p] = dot(lk_s[p], upper[...])
        for p in range(2):
            for py in range(TILE_SIDE):
                r = slice(TILE_SIDE * py, TILE_SIDE * (py + 1))
                w = al_s[p, r, :] * jnp.exp2(lb_s[p, r, :])
                hi, low = halves(w)
                w_s[p, r, :] = hi
                w_s[p, PIX + TILE_SIDE * py : PIX + TILE_SIDE * (py + 1), :] = low
                sw = s_s[p, r, :] * w
                s_s[p, r, :] = sw
                hi, low = halves(sw)
                sw_s[p, r, 0:LIST] = hi
                sw_s[p, r, LIST : 2 * LIST] = low
        for p in range(2):
            lb_s[p] = dot(sw_s[p], lower[...])
        for p in range(2):
            at, uy, dx, col_h, col_l, cot_h, cot_l = state[p]
            pad2 = jnp.zeros((2, LIST), f32)
            col_rows = jnp.concatenate([col_h, col_l, pad2], axis=0).astype(bf16)
            shown = dot_t(col_rows, w_s[p, 0:PIX, :]) + dot_t(col_rows, w_s[p, PIX : 2 * PIX, :])
            for k in range(3):
                image[k, at, :] = shown[k : k + 1, :] + shown[3 + k : 4 + k, :]
            cot_rows = jnp.concatenate([cot_h, cot_l, pad2], axis=0).astype(bf16)
            gcol = dot(jnp.concatenate([cot_rows, cot_rows], axis=1), w_s[p])
            acc = [[None, None] for _ in range(3)]
            for py in range(TILE_SIDE):
                dy = (py - 7.5) - uy
                for h in range(2):
                    r = slice(TILE_SIDE * py + 8 * h, TILE_SIDE * py + 8 * h + 8)
                    alpha = al_s[p, r, :]
                    g = s_s[p, r, :] - lb_s[p, r, :] * (alpha / (1.0 - alpha))
                    gy = g * dy
                    for n, v in enumerate((g, gy, gy * dy)):
                        acc[n][h] = v if py == 0 else acc[n][h] + v

            def down(a, b):
                return jnp.sum(a + b, axis=0, keepdims=True)

            xg = [dx[h] * acc[0][h] for h in range(2)]
            grad = [
                down(acc[0][0], acc[0][1]),
                down(xg[0], xg[1]),
                down(acc[1][0], acc[1][1]),
                down(dx[0] * xg[0], dx[1] * xg[1]),
                down(dx[0] * acc[1][0], dx[1] * acc[1][1]),
                down(acc[2][0], acc[2][1]),
            ] + [gcol[k : k + 1, :] + gcol[3 + k : 4 + k, :] for k in range(3)]
            s = lists[at, :]
            chunk_hit = (ch_iota == (((s >> 7) & 3) * 8 + (s >> 9))).astype(f32).astype(bf16)
            for f in range(N_GRAD):
                for n, part in enumerate(row_parts(grad[f])):
                    for r in range(0, 32, 16):
                        grads[p, 32 * f + r : 32 * f + r + 16, n * LIST : (n + 1) * LIST] = (
                            chunk_hit[r : r + 16, :] * part
                        )
            lane_hit = (lane_iota == (s & (LANES - 1))).astype(f32).astype(bf16)
            slot[...] += dot_t(grads[p], jnp.concatenate([lane_hit, lane_hit], axis=1))
        return carry

    lax.fori_loop(0, TILES_HERE // 2, pair, 0)

    terms = [jnp.zeros((8, LANES), f32) for _ in range(10)]
    for q in range(4):
        r = slice(8 * q, 8 * q + 8)
        ca, cb, cc = tab[2, r, :], tab[3, r, :], tab[4, r, :]
        gr = [slot[32 * f + 8 * q : 32 * f + 8 * q + 8, :] for f in range(N_GRAD)]
        du = (ca * gr[1] + cb * gr[2], cb * gr[1] + cc * gr[2])
        h00, h01, h11 = conic_pull(ca, cb, cc, gr[3], gr[4], gr[5])
        for c in range(3):
            mean, n0, n1 = tab[9 + c, r, :], tab[12 + c, r, :], tab[15 + c, r, :]
            terms[c] += du[0] * mean + 2.0 * (h00 * n0 + h01 * n1)
            terms[3 + c] += du[1] * mean + 2.0 * (h01 * n0 + h11 * n1)
            terms[8] += gr[6 + c] * tab[18 + c, r, :]
            terms[9] += gr[6 + c] * tab[21 + c, r, :]
        terms[6] += du[0]
        terms[7] += du[1]
    lanes = lax.broadcasted_iota(jnp.int32, (8, LANES), 1)
    share = jnp.zeros((8, LANES), f32)
    for m in range(10):
        total = jnp.sum(jnp.sum(terms[m], axis=0, keepdims=True), axis=1, keepdims=True)
        share = jnp.where(lanes == CAP + m, jnp.broadcast_to(total, (8, LANES)), share)
    group = lanes // CAP
    shares = [rotate(share, k) for k in range(8)]
    for q in range(4):
        pieces = swap_groups([slot[32 * f + 8 * q : 32 * f + 8 * q + 8, :] for f in range(8)], leave=True)
        last = slot[32 * 8 + 8 * q : 32 * 8 + 8 * q + 8, :]
        for k in range(8):
            first_row = GRAD_ROWS * 8 * (8 * q + k)
            out[pl.ds(first_row, 8, stride=GRAD_ROWS), :] = pieces[k]
            out[pl.ds(first_row + 1, 8, stride=GRAD_ROWS), :] = jnp.where(group == k, last, shares[k])


def conic_pull(ca, cb, cc, qxx, qxy, qyy):
    t00, t01 = ca * qxx + cb * qxy, ca * qxy + cb * qyy
    t10, t11 = cb * qxx + cc * qxy, cb * qxy + cc * qyy
    return 0.5 * (t00 * ca + t01 * cb), 0.5 * (t00 * cb + t01 * cc), 0.5 * (t10 * cb + t11 * cc)


PULL_CHUNK = 512


def pull_kernel(
    meta, returned, asked, feats, table, log_scales, quat_w, quat_v, cam, image, out, cam_out, image_out, row_s, idx_s, lhs_s, sum_s, gc_s
):
    image_out[...] = image[...]
    index = asked_lanes(asked, meta[TILES_HERE + 1])
    for q in range(4):
        idx_s[:, q * LANES : (q + 1) * LANES] = index[q]
    group = lax.broadcasted_iota(jnp.int32, (8, LANES), 1) // CAP
    turned = meta[TILES_HERE] & 7
    camera = jnp.zeros((8, LANES), f32)
    for q in range(4):
        pieces = [returned[pl.ds(GRAD_ROWS * 8 * (8 * q + k), 8, stride=GRAD_ROWS), :] for k in range(8)]
        pieces = swap_groups(pieces, turned)
        for f in range(8):
            row_s[f, :, q * LANES : (q + 1) * LANES] = pieces[f]
        last = None
        for k in range(8):
            piece = returned[pl.ds(GRAD_ROWS * 8 * (8 * q + k) + 1, 8, stride=GRAD_ROWS), :]
            camera = camera + piece
            moved = rotate(piece, k + 8 - turned)
            last = moved if k == 0 else jnp.where(group == k, moved, last)
        row_s[8, :, q * LANES : (q + 1) * LANES] = last
    cam_out[...] = rotate(camera, 7 - turned)[:, 0:10]

    slots = N_TILE * CAP
    high_iota = lax.broadcasted_iota(jnp.int32, (16, slots), 0)
    lane_iota = lax.broadcasted_iota(jnp.int32, (LANES, slots), 0)

    def image(i, carry):
        at = pl.ds(i, 1)
        s = idx_s[at, :]
        high_hit = (high_iota == (s >> 7)).astype(f32).astype(bf16)
        lane_hit = (lane_iota == (s & (LANES - 1))).astype(f32).astype(bf16)
        for f in range(N_GRAD):
            for n, part in enumerate(row_parts(row_s[f, at, :])):
                lhs_s[16 * f : 16 * (f + 1), n * slots : (n + 1) * slots] = high_hit * part
        sum_s[pl.ds(pl.multiple_of(i * (16 * N_GRAD), 16), 16 * N_GRAD), :] = dot_t(
            lhs_s[...], jnp.concatenate([lane_hit, lane_hit], axis=1)
        )
        return carry

    lax.fori_loop(0, N_IMG, image, 0, unroll=8)

    column = [jnp.broadcast_to(cam[:, m : m + 1], (N_IMG, PULL_CHUNK)) for m in range(6)]

    def chunk(h, carry):
        at = pl.ds(pl.multiple_of(h * PULL_CHUNK, PULL_CHUNK), PULL_CHUNK)
        parts = PULL_CHUNK // LANES
        gr = [
            jnp.concatenate(
                [sum_s[pl.ds(16 * f + h * parts + e, 8, stride=16 * N_GRAD), :] for e in range(parts)],
                axis=1,
            )
            for f in range(N_GRAD)
        ]
        ca, cb, cc = feats[2, :, at], feats[3, :, at], feats[4, :, at]
        du = (ca * gr[1] + cb * gr[2], cb * gr[1] + cc * gr[2])
        h00, h01, h11 = conic_pull(ca, cb, cc, gr[3], gr[4], gr[5])
        a0, a1 = column[0:3], column[3:6]

        def over_images(v):
            return jnp.sum(v, axis=0, keepdims=True)

        for c in range(3):
            out[c : c + 1, at] = over_images(a0[c] * du[0] + a1[c] * du[1])
        t0 = [h00 * a0[c] + h01 * a1[c] for c in range(3)]
        t1 = [h01 * a0[c] + h11 * a1[c] for c in range(3)]
        v = [[None] * 3 for _ in range(3)]
        for c in range(3):
            for d in range(c, 3):
                v[c][d] = v[d][c] = over_images(t0[c] * a0[d] + t1[c] * a1[d])
        ls = [log_scales[c : c + 1, at] for c in range(3)]
        quat = [quat_w[0:1, at]] + [quat_v[c : c + 1, at] for c in range(3)]
        m, pull = jax.vjp(shape_matrix, ls, quat)
        dm = [[2.0 * sum(v[r][d] * m[d][c] for d in range(3)) for c in range(3)] for r in range(3)]
        dls, dquat = pull(dm)
        for c in range(3):
            out[3 + c : 4 + c, at] = dls[c]
        for c in range(4):
            out[6 + c : 7 + c, at] = dquat[c]
        base = feats[5, 0:1, at]
        out[10:11, at] = over_images(gr[0]) * (1.0 - base)
        for k in range(3):
            gc_s[8 * k : 8 * k + 8, at] = gr[6 + k]
        return carry

    lax.fori_loop(0, OWNED // PULL_CHUNK, chunk, 0)

    y_h, y_l = halves(jnp.transpose(table[...])[0:16, :])
    y_all = jnp.concatenate([y_h.astype(f32), y_h.astype(f32), y_l.astype(f32), y_l.astype(f32)], axis=1).astype(bf16)
    for k in range(3):
        g_h, g_l = halves(gc_s[8 * k : 8 * k + 8, :])
        g_all = jnp.concatenate([g_h.astype(f32), g_l.astype(f32), g_h.astype(f32), g_l.astype(f32)], axis=0).astype(bf16)
        out[11 + 16 * k : 27 + 16 * k, :] = dot(y_all, g_all)


def whole(memory=pltpu.VMEM):
    return pl.BlockSpec(memory_space=memory)


def call(kernel, name, out_shape, scratch, n_in, smem=0, memory=pltpu.VMEM, cost=None):
    return pl.pallas_call(
        kernel,
        name=name,
        out_shape=out_shape,
        in_specs=[whole(pltpu.SMEM)] * smem + [whole(memory)] * (n_in - smem),
        out_specs=jax.tree.map(lambda _: whole(), out_shape),
        scratch_shapes=scratch,
        cost_estimate=cost,
        compiler_params=pltpu.CompilerParams(vmem_limit_bytes=32 << 20),
    )


def exchange(array):
    return lax.all_to_all(array, ORDER, split_axis=0, concat_axis=0, tiled=True)


def exchange_rows(array, rows):
    shape = array.shape
    return exchange(array.reshape(-1, 1, rows * LANES)).reshape(shape)


def local(
    means, log_scales, quat_w, quat_v, opacity, sh_coeffs, cameras, requests, lists, counts, image_cot
):
    devices = N_IMG * N_TILE
    by_owner = jnp.transpose(requests.reshape(N_IMG, N_TILE, CAP), (0, 2, 1)).reshape(N_IMG * CAP, N_TILE)
    wanted = call(ask_kernel, "ask", jax.ShapeDtypeStruct((devices, LANES), jnp.int32), [], 1)(by_owner)
    asked = exchange_rows(wanted, 1)
    meta = jnp.concatenate(
        [counts[0], jnp.stack([lax.axis_index("tile"), lax.axis_index("img")]).astype(jnp.int32)]
    )
    owned = [
        pltpu.with_memory_space_constraint(a, pltpu.HBM)
        for a in (means, log_scales, quat_w, quat_v, opacity, sh_coeffs, cameras)
    ]
    feats, table = call(
        project_kernel,
        "project",
        (jax.ShapeDtypeStruct((N_FEAT, N_IMG, OWNED), f32), jax.ShapeDtypeStruct((N_IMG, LANES), f32)),
        [pltpu.VMEM((48, N_IMG, LANES), f32)]
        + [pltpu.VMEM(a.shape, f32) for a in owned]
        + [pltpu.SemaphoreType.DMA((7,))],
        7,
        memory=pltpu.HBM,
        cost=pl.CostEstimate(flops=20_000_000, transcendentals=0, bytes_accessed=1_000_000),
    )(*owned)
    asked, feats, meta = lax.optimization_barrier((asked, feats, meta))
    packed = call(
        pick_kernel,
        "pick",
        jax.ShapeDtypeStruct((FEAT_ROWS * devices, LANES), f32),
        [pltpu.VMEM((32, N_IMG, LANES), jnp.int32)],
        3,
        smem=1,
    )(meta, asked, feats)
    rows = exchange_rows(packed, FEAT_ROWS)
    rendered, slot_grads = call(
        render_kernel,
        "render",
        (
            jax.ShapeDtypeStruct((3, TILES_HERE, PIX), f32),
            jax.ShapeDtypeStruct((GRAD_ROWS * devices, LANES), f32),
        ),
        [
            pltpu.VMEM((N_FEAT, 32, LANES), f32),
            pltpu.VMEM((N_USED, 8, LIST), f32),
            pltpu.VMEM((2, 32 * N_GRAD, 2 * LIST), bf16),
            pltpu.VMEM((32 * N_GRAD, LANES), f32),
            pltpu.VMEM((2 * LIST, LIST), bf16),
            pltpu.VMEM((2 * LIST, LIST), bf16),
            pltpu.VMEM((2, PIX, LIST), f32),
            pltpu.VMEM((2, PIX, 2 * LIST), bf16),
            pltpu.VMEM((2, PIX, LIST), f32),
            pltpu.VMEM((2, PIX, LIST), f32),
            pltpu.VMEM((2, 2 * PIX, LIST), bf16),
            pltpu.VMEM((2, PIX, 2 * LIST), bf16),
        ],
        4,
        smem=1,
    )(meta, rows, lists[0], image_cot[0])
    returned = exchange_rows(slot_grads, GRAD_ROWS)
    param_grad, camera_grad, rendered = call(
        pull_kernel,
        "pull",
        (
            jax.ShapeDtypeStruct((59, OWNED), f32),
            jax.ShapeDtypeStruct((N_IMG, 10), f32),
            jax.ShapeDtypeStruct((3, TILES_HERE, PIX), f32),
        ),
        [
            pltpu.VMEM((N_GRAD, N_IMG, N_TILE * CAP), f32),
            pltpu.VMEM((N_IMG, N_TILE * CAP), jnp.int32),
            pltpu.VMEM((16 * N_GRAD, 2 * N_TILE * CAP), bf16),
            pltpu.VMEM((N_IMG * 16 * N_GRAD, LANES), f32),
            pltpu.VMEM((24, OWNED), f32),
        ],
        10,
        smem=1,
    )(meta, returned, asked, feats, table, log_scales, quat_w, quat_v, cameras, rendered)
    return (rendered[None], param_grad, camera_grad)


def solution(mesh):
    own = P(None, ALL)
    return jax.shard_map(
        local,
        mesh=mesh,
        in_specs=(
            own,
            own,
            own,
            own,
            own,
            own,
            P(),
            P("img", "tile", None, None, None),
            P("img", "tile", None),
            P("img", "tile"),
            P("img", None, "tile", None),
        ),
        out_specs=(P("img", None, "tile", None), own, P()),
        check_vma=False,
    )
```

```python
import jax
import jax.numpy as jnp
from jax import lax
from jax.experimental import pallas as pl
from jax.experimental.pallas import tpu as pltpu
from jax.sharding import PartitionSpec as P

TILE_SIDE = 16
TW = 16
ALL = ("img", "tile")
ORDER = ("tile", "img")
N_IMG = 8
N_TILE = 32
CAP = 16
OWNED = 2048
LIST = 256
TILES_HERE = 8
PIX = 256
LANES = 128
N_FEAT = 24
N_USED = 9
N_GRAD = 9
FEAT_ROWS = 3
GRAD_ROWS = 2

sh_first = 0.28209479177387814
sh_second = 0.4886025119029199
sh_third = (
    1.0925484305920792,
    -1.0925484305920792,
    0.31539156525252005,
    -1.0925484305920792,
    0.5462742152960396,
)
sh_fourth = (
    -0.5900435899266435,
    2.890611442640554,
    -0.4570457994644658,
    0.3731763325901154,
    -0.4570457994644658,
    1.445305721320277,
    -0.5900435899266435,
)
dilation = 0.3
LOG2E = 1.4426950408889634
f32 = jnp.float32
bf16 = jnp.bfloat16


def harmonics_of(polar, azimuth):
    sin_p, cos_p = jnp.sin(polar), jnp.cos(polar)
    x = sin_p * jnp.cos(azimuth)
    y = sin_p * jnp.sin(azimuth)
    z = cos_p
    xx, yy, zz = x * x, y * y, z * z
    return [
        sh_first + 0.0 * x,
        -sh_second * y,
        sh_second * z,
        -sh_second * x,
        sh_third[0] * x * y,
        sh_third[1] * y * z,
        sh_third[2] * (2.0 * zz - xx - yy),
        sh_third[3] * x * z,
        sh_third[4] * (xx - yy),
        sh_fourth[0] * y * (3.0 * xx - yy),
        sh_fourth[1] * x * y * z,
        sh_fourth[2] * y * (4.0 * zz - xx - yy),
        sh_fourth[3] * z * (2.0 * zz - 3.0 * xx - 3.0 * yy),
        sh_fourth[4] * x * (4.0 * zz - xx - yy),
        sh_fourth[5] * z * (xx - yy),
        sh_fourth[6] * x * (xx - 3.0 * yy),
    ]


def shape_matrix(log_scales, quat):
    w, x, y, z = quat
    norm = jnp.sqrt(w * w + x * x + y * y + z * z)
    w, x, y, z = w / norm, x / norm, y / norm, z / norm
    rotation = (
        (1.0 - 2.0 * (y * y + z * z), 2.0 * (x * y - w * z), 2.0 * (x * z + w * y)),
        (2.0 * (x * y + w * z), 1.0 - 2.0 * (x * x + z * z), 2.0 * (y * z - w * x)),
        (2.0 * (x * z - w * y), 2.0 * (y * z + w * x), 1.0 - 2.0 * (x * x + y * y)),
    )
    stretch = [jnp.exp(v) for v in log_scales]
    return [[rotation[r][c] * stretch[c] for c in range(3)] for r in range(3)]


def turn_groups(vregs):
    group = lax.broadcasted_iota(jnp.int32, (8, LANES), 1) // CAP
    work = [vregs[-k % 8] for k in range(8)]
    for bit in (1, 2, 4):
        move = (group & bit) != 0
        work = [jnp.where(move, work[(k - bit) % 8], work[k]) for k in range(8)]
    return work


def rotate(value, groups):
    if isinstance(groups, int):
        shift = CAP * groups % LANES
        return value if shift == 0 else pltpu.roll(value, shift, 1)
    return pltpu.roll(value, (CAP * groups) & (LANES - 1), 1)


def swap_groups(vregs, turned=0, leave=False):
    vregs = turn_groups([rotate(v, i + LANES // CAP - turned) for i, v in enumerate(vregs)])
    return vregs if leave else [rotate(v, -g) for g, v in enumerate(vregs)]


def lane_take(table, lanes):
    return jnp.take_along_axis(table, lanes, axis=1, mode="promise_in_bounds")


def halves(value):
    high = value.astype(bf16)
    return high, (value - high.astype(f32)).astype(bf16)


def row_parts(row):
    return halves(jnp.broadcast_to(row, (16, row.shape[1])))


def dot(a, b):
    return lax.dot_general(a, b, (((1,), (0,)), ((), ())), preferred_element_type=f32)


def dot_t(a, b):
    return lax.dot_general(a, b, (((1,), (1,)), ((), ())), preferred_element_type=f32)


PROJECT_CHUNK = 256


def ask_kernel(wanted, out):
    padded = jnp.concatenate([wanted[...], jnp.zeros((LANES, LANES - N_TILE), jnp.int32)], axis=1)
    turned = jnp.transpose(padded)
    for b in range(N_TILE):
        out[8 * b : 8 * b + 8, :] = jnp.broadcast_to(turned[b : b + 1, :], (8, LANES))


def asked_lanes(asked, my_img):
    group = lax.broadcasted_iota(jnp.int32, (8, LANES), 1) // CAP
    base = LANES - CAP * my_img
    result = []
    for q in range(4):
        total = None
        for k in range(8):
            piece = pltpu.roll(asked[8 * (8 * q + k) : 8 * (8 * q + k) + 8, :], (base + CAP * k) & (LANES - 1), 1)
            total = piece if k == 0 else jnp.where(group == k, piece, total)
        result.append(total)
    return result


def project(means, log_scales, quat_w, quat_v, opacity, sh, cam, out, harm):
    column = [jnp.broadcast_to(cam[:, m : m + 1], (N_IMG, PROJECT_CHUNK)) for m in range(8)]

    def chunk(h, carry):
        at = pl.ds(pl.multiple_of(h * PROJECT_CHUNK, PROJECT_CHUNK), PROJECT_CHUNK)
        mean = [means[c : c + 1, at] for c in range(3)]
        quat = [quat_w[0:1, at]] + [quat_v[c : c + 1, at] for c in range(3)]
        m = shape_matrix([log_scales[c : c + 1, at] for c in range(3)], quat)
        for row in range(2):
            a = column[3 * row : 3 * row + 3]
            out[row, :, at] = a[0] * mean[0] + a[1] * mean[1] + a[2] * mean[2] + column[6 + row]
        p = [
            [
                sum(column[3 * row + r] * m[r][c] for r in range(3))
                for c in range(3)
            ]
            for row in range(2)
        ]
        s00 = p[0][0] * p[0][0] + p[0][1] * p[0][1] + p[0][2] * p[0][2] + dilation
        s01 = p[0][0] * p[1][0] + p[0][1] * p[1][1] + p[0][2] * p[1][2]
        s11 = p[1][0] * p[1][0] + p[1][1] * p[1][1] + p[1][2] * p[1][2] + dilation
        det = s00 * s11 - s01 * s01
        out[2, :, at] = s11 / det
        out[3, :, at] = -s01 / det
        out[4, :, at] = s00 / det
        base = 1.0 / (1.0 + jnp.exp(-opacity[0:1, at]))
        out[5, :, at] = jnp.broadcast_to(base, (N_IMG, PROJECT_CHUNK))
        for c in range(3):
            out[9 + c, :, at] = jnp.broadcast_to(mean[c], (N_IMG, PROJECT_CHUNK))
            for row in range(2):
                out[12 + 3 * row + c, :, at] = (
                    m[c][0] * p[row][0] + m[c][1] * p[row][1] + m[c][2] * p[row][2]
                )
        for base_row, first, start in ((6, 0, 0.5), (18, 16, 0.0), (21, 32, 0.0)):
            total = [jnp.full((N_IMG, PROJECT_CHUNK), start, f32) for _ in range(3)]
            for b in range(16):
                y = jnp.concatenate([harm[first + b]] * (PROJECT_CHUNK // LANES), axis=1)
                for k in range(3):
                    total[k] = total[k] + y * sh[16 * k + b : 16 * k + b + 1, at]
            for k in range(3):
                out[base_row + k, :, at] = total[k]
        return carry

    lax.fori_loop(0, OWNED // PROJECT_CHUNK, chunk, 0)


def project_kernel(*refs):
    sources, (feats, table), rest = refs[:7], refs[7:9], refs[9:]
    harm, held, sems = rest[0], rest[1:8], rest[8]
    copies = [pltpu.make_async_copy(a, b, sems.at[n]) for n, (a, b) in enumerate(zip(sources, held))]
    for copy in reversed(copies):
        copy.start()
    for copy in reversed(copies):
        copy.wait()
    means, log_scales, quat_w, quat_v, opacity, sh, cam = held
    polar = jnp.broadcast_to(cam[:, 8:9], (N_IMG, LANES))
    azimuth = jnp.broadcast_to(cam[:, 9:10], (N_IMG, LANES))
    one, zero = jnp.ones_like(polar), jnp.zeros_like(polar)
    values, d_polar = jax.jvp(harmonics_of, (polar, azimuth), (one, zero))
    d_azimuth = jax.jvp(harmonics_of, (polar, azimuth), (zero, one))[1]
    lanes = lax.broadcasted_iota(jnp.int32, (N_IMG, LANES), 1)
    packed = jnp.zeros((N_IMG, LANES), f32)
    for b in range(16):
        harm[b] = values[b]
        harm[16 + b] = d_polar[b]
        harm[32 + b] = d_azimuth[b]
        packed = jnp.where(lanes == b, values[b], packed)
    table[...] = packed
    project(means, log_scales, quat_w, quat_v, opacity, sh, cam, feats, harm)


def pick_kernel(meta, asked, feats, out, idx_out, index):
    for q, value in enumerate(asked_lanes(asked, meta[TILES_HERE + 1])):
        idx_out[:, q * LANES : (q + 1) * LANES] = value
        for f in range(8):
            index[8 * q + f] = rotate(value, f)

    def step(n, carry):
        g, q = n >> 2, n & 3
        picked = []
        for f in range(8):
            here = index[8 * q + f]
            low, high = here & (LANES - 1), here >> 7
            value = None
            for h in range(OWNED // LANES):
                found = lane_take(feats[8 * g + f, :, h * LANES : (h + 1) * LANES], low)
                value = found if h == 0 else jnp.where(high == h, found, value)
            picked.append(value)
        for k, row in enumerate(turn_groups(picked)):
            out[pl.ds(FEAT_ROWS * 8 * (8 * q + k) + g, 8, stride=FEAT_ROWS), :] = row
        return carry

    lax.fori_loop(0, 4 * FEAT_ROWS, step, 0, unroll=4)


def render_kernel(
    meta,
    rows,
    lists,
    cot,
    image,
    out,
    tab,
    feat,
    grads,
    slot,
    upper,
    lower,
    al_s,
    lk_s,
    lb_s,
    s_s,
    w_s,
    sw_s,
    later,
):
    tile_base = meta[TILES_HERE] * TILES_HERE
    turned = meta[TILES_HERE] & 7

    def sort_rows(n, carry):
        g, q = n >> 2, n & 3
        pieces = [
            rows[pl.ds(FEAT_ROWS * 8 * (8 * q + k) + g, 8, stride=FEAT_ROWS), :] for k in range(8)
        ]
        pieces = swap_groups(pieces, turned)
        for f in range(8):
            tab[8 * g + f, pl.ds(pl.multiple_of(8 * q, 8), 8), :] = pieces[f]
        return carry

    lax.fori_loop(0, 4 * FEAT_ROWS, sort_rows, 0, unroll=4)

    def entries(quad):
        s = jnp.concatenate(
            [lists[4 * quad : 4 * quad + 4, h * LANES : (h + 1) * LANES] for h in range(2)], axis=0
        )
        return s & (LANES - 1), ((s >> 7) & 3) * 8 + (s >> 9)

    def gather(ch, carry, lane, chunk):
        hit = chunk == ch
        return tuple(
            jnp.where(hit, lane_take(jnp.broadcast_to(tab[f, pl.ds(ch, 1), :], (8, LANES)), lane), carry[f])
            for f in range(N_USED)
        )

    def keep(found, quad):
        for f in range(N_USED):
            for h in range(2):
                feat[f, 4 * quad : 4 * quad + 4, h * LANES : (h + 1) * LANES] = found[f][4 * h : 4 * h + 4, :]

    zero = jnp.zeros((8, LANES), f32)
    first_lane, first_chunk = entries(0)
    keep(
        lax.fori_loop(
            0, 32, lambda ch, c: gather(ch, c, first_lane, first_chunk), tuple([zero] * N_USED), unroll=8
        ),
        0,
    )
    for f in range(N_USED):
        later[f] = zero
    ri = lax.broadcasted_iota(jnp.int32, (LIST, LIST), 0)
    ci = lax.broadcasted_iota(jnp.int32, (LIST, LIST), 1)
    up = (ri < ci).astype(f32).astype(bf16)
    lo = (ri > ci).astype(f32).astype(bf16)
    for part in range(2):
        upper[part * LIST : (part + 1) * LIST, :] = up
        lower[part * LIST : (part + 1) * LIST, :] = lo
    slot[...] = jnp.zeros_like(slot)
    lane = lax.broadcasted_iota(jnp.int32, (1, LIST), 1)
    px = lax.broadcasted_iota(jnp.int32, (8, LIST), 0).astype(f32) - 7.5
    ch_iota = lax.broadcasted_iota(jnp.int32, (32, LIST), 0)
    lane_iota = lax.broadcasted_iota(jnp.int32, (LANES, LIST), 0)

    def row8(v):
        return jnp.broadcast_to(v, (8, LIST))

    def pair(pair_index, carry):
        tiles = [2 * pair_index, 2 * pair_index + 1]
        state = []
        for p in range(2):
            j = tiles[p]
            number = tile_base + j
            centre_x = (TILE_SIDE * (number % TW)).astype(f32) + (0.5 * TILE_SIDE - 0.5 * TILE_SIDE * TW)
            centre_y = (TILE_SIDE * (number // TW)).astype(f32) + (0.5 * TILE_SIDE - 0.5 * TILE_SIDE * TW)
            at = pl.ds(j, 1)
            ux = feat[0, at, :] - centre_x
            uy = row8(feat[1, at, :] - centre_y)
            ca, cb, cc = feat[2, at, :], feat[3, at, :], feat[4, at, :]
            op = row8(jnp.where(lane < meta[j], feat[5, at, :], 0.0))
            cc = row8(cc * (-0.5 * LOG2E))
            ux, na, nb = row8(ux), row8(ca * (-0.5 * LOG2E)), row8(cb * (-LOG2E))
            dx = [px - ux, px + (8.0 - ux)]
            na = [na * d * d for d in dx]
            nb = [nb * d for d in dx]
            colours = jnp.concatenate([feat[6 + k, at, :] for k in range(3)], axis=0)
            cots = jnp.concatenate([cot[k, at, :] for k in range(3)], axis=0)
            col_h, col_l, cot_h, cot_l = [v.astype(f32) for v in halves(colours) + halves(cots)]
            pad = jnp.zeros((4, LIST), f32)
            cot_k = jnp.concatenate([cot_h, cot_h, cot_l, cot_l, pad], axis=0)
            col_k = jnp.concatenate([col_h, col_l, col_h, col_l, pad], axis=0).astype(bf16)
            s_s[p] = dot(jnp.transpose(cot_k).astype(bf16), col_k)
            for py in range(TILE_SIDE):
                r = slice(TILE_SIDE * py, TILE_SIDE * (py + 1))
                dy = (py - 7.5) - uy
                cy = cc * dy * dy
                alpha = jnp.concatenate(
                    [op * jnp.exp2((na[h] + cy) + nb[h] * dy) for h in range(2)], axis=0
                )
                al_s[p, r, :] = alpha
                hi, low = halves(jnp.log2(1.0 - alpha))
                lk_s[p, r, 0:LIST] = hi
                lk_s[p, r, LIST : 2 * LIST] = low
            state.append((at, uy, dx, col_h, col_l, cot_h, cot_l))
        for p in range(2):
            lb_s[p] = dot(lk_s[p], upper[...])
        for p in range(2):
            for py in range(TILE_SIDE):
                r = slice(TILE_SIDE * py, TILE_SIDE * (py + 1))
                w = al_s[p, r, :] * jnp.exp2(lb_s[p, r, :])
                hi, low = halves(w)
                w_s[p, r, :] = hi
                w_s[p, PIX + TILE_SIDE * py : PIX + TILE_SIDE * (py + 1), :] = low
                sw = s_s[p, r, :] * w
                s_s[p, r, :] = sw
                hi, low = halves(sw)
                sw_s[p, r, 0:LIST] = hi
                sw_s[p, r, LIST : 2 * LIST] = low
        for p in range(2):
            lb_s[p] = dot(sw_s[p], lower[...])
        for p in range(2):
            at, uy, dx, col_h, col_l, cot_h, cot_l = state[p]
            pad2 = jnp.zeros((2, LIST), f32)
            col_rows = jnp.concatenate([col_h, col_l, pad2], axis=0).astype(bf16)
            shown = dot_t(col_rows, w_s[p, 0:PIX, :]) + dot_t(col_rows, w_s[p, PIX : 2 * PIX, :])
            for k in range(3):
                image[k, at, :] = shown[k : k + 1, :] + shown[3 + k : 4 + k, :]
            cot_rows = jnp.concatenate([cot_h, cot_l, pad2], axis=0).astype(bf16)
            gcol = dot(jnp.concatenate([cot_rows, cot_rows], axis=1), w_s[p])
            acc = [[None, None] for _ in range(3)]
            for py in range(TILE_SIDE):
                dy = (py - 7.5) - uy
                for h in range(2):
                    r = slice(TILE_SIDE * py + 8 * h, TILE_SIDE * py + 8 * h + 8)
                    alpha = al_s[p, r, :]
                    g = s_s[p, r, :] - lb_s[p, r, :] * (alpha / (1.0 - alpha))
                    gy = g * dy
                    for n, v in enumerate((g, gy, gy * dy)):
                        acc[n][h] = v if py == 0 else acc[n][h] + v

            def down(a, b):
                return jnp.sum(a + b, axis=0, keepdims=True)

            xg = [dx[h] * acc[0][h] for h in range(2)]
            grad = [
                down(acc[0][0], acc[0][1]),
                down(xg[0], xg[1]),
                down(acc[1][0], acc[1][1]),
                down(dx[0] * xg[0], dx[1] * xg[1]),
                down(dx[0] * acc[1][0], dx[1] * acc[1][1]),
                down(acc[2][0], acc[2][1]),
            ] + [gcol[k : k + 1, :] + gcol[3 + k : 4 + k, :] for k in range(3)]
            s = lists[at, :]
            chunk_hit = (ch_iota == (((s >> 7) & 3) * 8 + (s >> 9))).astype(f32).astype(bf16)
            for f in range(N_GRAD):
                for n, part in enumerate(row_parts(grad[f])):
                    for r in range(0, 32, 16):
                        grads[p, 32 * f + r : 32 * f + r + 16, n * LIST : (n + 1) * LIST] = (
                            chunk_hit[r : r + 16, :] * part
                        )
            lane_hit = (lane_iota == (s & (LANES - 1))).astype(f32).astype(bf16)
            slot[...] += dot_t(grads[p], jnp.concatenate([lane_hit, lane_hit], axis=1))
        lane_at, chunk_at = entries(1)
        found = tuple(later[f] for f in range(N_USED))
        for n in range(16):
            found = gather(16 * (pair_index & 1) + n, found, lane_at, chunk_at)
        for f in range(N_USED):
            later[f] = found[f]
        keep(found, 1)
        return carry

    lax.fori_loop(0, TILES_HERE // 2, pair, 0)

    terms = [jnp.zeros((8, LANES), f32) for _ in range(10)]
    for q in range(4):
        r = slice(8 * q, 8 * q + 8)
        ca, cb, cc = tab[2, r, :], tab[3, r, :], tab[4, r, :]
        gr = [slot[32 * f + 8 * q : 32 * f + 8 * q + 8, :] for f in range(N_GRAD)]
        du = (ca * gr[1] + cb * gr[2], cb * gr[1] + cc * gr[2])
        h00, h01, h11 = conic_pull(ca, cb, cc, gr[3], gr[4], gr[5])
        for c in range(3):
            mean, n0, n1 = tab[9 + c, r, :], tab[12 + c, r, :], tab[15 + c, r, :]
            terms[c] += du[0] * mean + 2.0 * (h00 * n0 + h01 * n1)
            terms[3 + c] += du[1] * mean + 2.0 * (h01 * n0 + h11 * n1)
            terms[8] += gr[6 + c] * tab[18 + c, r, :]
            terms[9] += gr[6 + c] * tab[21 + c, r, :]
        terms[6] += du[0]
        terms[7] += du[1]
    lanes = lax.broadcasted_iota(jnp.int32, (8, LANES), 1)
    share = jnp.zeros((8, LANES), f32)
    for m in range(10):
        total = jnp.sum(jnp.sum(terms[m], axis=0, keepdims=True), axis=1, keepdims=True)
        share = jnp.where(lanes == CAP + m, jnp.broadcast_to(total, (8, LANES)), share)
    group = lanes // CAP
    shares = [rotate(share, k) for k in range(8)]
    for q in range(4):
        pieces = swap_groups([slot[32 * f + 8 * q : 32 * f + 8 * q + 8, :] for f in range(8)], leave=True)
        last = slot[32 * 8 + 8 * q : 32 * 8 + 8 * q + 8, :]
        for k in range(8):
            first_row = GRAD_ROWS * 8 * (8 * q + k)
            out[pl.ds(first_row, 8, stride=GRAD_ROWS), :] = pieces[k]
            out[pl.ds(first_row + 1, 8, stride=GRAD_ROWS), :] = jnp.where(group == k, last, shares[k])


def conic_pull(ca, cb, cc, qxx, qxy, qyy):
    t00, t01 = ca * qxx + cb * qxy, ca * qxy + cb * qyy
    t10, t11 = cb * qxx + cc * qxy, cb * qxy + cc * qyy
    return 0.5 * (t00 * ca + t01 * cb), 0.5 * (t00 * cb + t01 * cc), 0.5 * (t10 * cb + t11 * cc)


PULL_CHUNK = 512


def pull_kernel(
    meta, returned, idx_s, feats, table, log_scales, quat_w, quat_v, cam, image, out, cam_out, image_out, row_s, lhs_s, sum_s, gc_s
):
    image_out[...] = image[...]
    group = lax.broadcasted_iota(jnp.int32, (8, LANES), 1) // CAP
    turned = meta[TILES_HERE] & 7
    camera = jnp.zeros((8, LANES), f32)
    for q in range(4):
        pieces = [returned[pl.ds(GRAD_ROWS * 8 * (8 * q + k), 8, stride=GRAD_ROWS), :] for k in range(8)]
        pieces = swap_groups(pieces, turned)
        for f in range(8):
            row_s[f, :, q * LANES : (q + 1) * LANES] = pieces[f]
        last = None
        for k in range(8):
            piece = returned[pl.ds(GRAD_ROWS * 8 * (8 * q + k) + 1, 8, stride=GRAD_ROWS), :]
            camera = camera + piece
            moved = rotate(piece, k + 8 - turned)
            last = moved if k == 0 else jnp.where(group == k, moved, last)
        row_s[8, :, q * LANES : (q + 1) * LANES] = last
    cam_out[...] = rotate(camera, 7 - turned)[:, 0:10]

    slots = N_TILE * CAP
    high_iota = lax.broadcasted_iota(jnp.int32, (16, slots), 0)
    lane_iota = lax.broadcasted_iota(jnp.int32, (LANES, slots), 0)

    def image(i, carry):
        at = pl.ds(i, 1)
        s = idx_s[at, :]
        high_hit = (high_iota == (s >> 7)).astype(f32).astype(bf16)
        lane_hit = (lane_iota == (s & (LANES - 1))).astype(f32).astype(bf16)
        for f in range(N_GRAD):
            for n, part in enumerate(row_parts(row_s[f, at, :])):
                lhs_s[16 * f : 16 * (f + 1), n * slots : (n + 1) * slots] = high_hit * part
        sum_s[pl.ds(pl.multiple_of(i * (16 * N_GRAD), 16), 16 * N_GRAD), :] = dot_t(
            lhs_s[...], jnp.concatenate([lane_hit, lane_hit], axis=1)
        )
        return carry

    lax.fori_loop(0, N_IMG, image, 0, unroll=8)

    column = [jnp.broadcast_to(cam[:, m : m + 1], (N_IMG, PULL_CHUNK)) for m in range(6)]

    def chunk(h, carry):
        at = pl.ds(pl.multiple_of(h * PULL_CHUNK, PULL_CHUNK), PULL_CHUNK)
        parts = PULL_CHUNK // LANES
        gr = [
            jnp.concatenate(
                [sum_s[pl.ds(16 * f + h * parts + e, 8, stride=16 * N_GRAD), :] for e in range(parts)],
                axis=1,
            )
            for f in range(N_GRAD)
        ]
        ca, cb, cc = feats[2, :, at], feats[3, :, at], feats[4, :, at]
        du = (ca * gr[1] + cb * gr[2], cb * gr[1] + cc * gr[2])
        h00, h01, h11 = conic_pull(ca, cb, cc, gr[3], gr[4], gr[5])
        a0, a1 = column[0:3], column[3:6]

        def over_images(v):
            return jnp.sum(v, axis=0, keepdims=True)

        for c in range(3):
            out[c : c + 1, at] = over_images(a0[c] * du[0] + a1[c] * du[1])
        t0 = [h00 * a0[c] + h01 * a1[c] for c in range(3)]
        t1 = [h01 * a0[c] + h11 * a1[c] for c in range(3)]
        v = [[None] * 3 for _ in range(3)]
        for c in range(3):
            for d in range(c, 3):
                v[c][d] = v[d][c] = over_images(t0[c] * a0[d] + t1[c] * a1[d])
        ls = [log_scales[c : c + 1, at] for c in range(3)]
        quat = [quat_w[0:1, at]] + [quat_v[c : c + 1, at] for c in range(3)]
        m, pull = jax.vjp(shape_matrix, ls, quat)
        dm = [[2.0 * sum(v[r][d] * m[d][c] for d in range(3)) for c in range(3)] for r in range(3)]
        dls, dquat = pull(dm)
        for c in range(3):
            out[3 + c : 4 + c, at] = dls[c]
        for c in range(4):
            out[6 + c : 7 + c, at] = dquat[c]
        base = feats[5, 0:1, at]
        out[10:11, at] = over_images(gr[0]) * (1.0 - base)
        for k in range(3):
            gc_s[8 * k : 8 * k + 8, at] = gr[6 + k]
        return carry

    lax.fori_loop(0, OWNED // PULL_CHUNK, chunk, 0)

    y_h, y_l = halves(jnp.transpose(table[...])[0:16, :])
    y_all = jnp.concatenate([y_h.astype(f32), y_h.astype(f32), y_l.astype(f32), y_l.astype(f32)], axis=1).astype(bf16)
    for k in range(3):
        g_h, g_l = halves(gc_s[8 * k : 8 * k + 8, :])
        g_all = jnp.concatenate([g_h.astype(f32), g_l.astype(f32), g_h.astype(f32), g_l.astype(f32)], axis=0).astype(bf16)
        out[11 + 16 * k : 27 + 16 * k, :] = dot(y_all, g_all)


def whole(memory=pltpu.VMEM):
    return pl.BlockSpec(memory_space=memory)


def call(kernel, name, out_shape, scratch, n_in, smem=0, memory=pltpu.VMEM, cost=None):
    return pl.pallas_call(
        kernel,
        name=name,
        out_shape=out_shape,
        in_specs=[whole(pltpu.SMEM)] * smem + [whole(memory)] * (n_in - smem),
        out_specs=jax.tree.map(lambda _: whole(), out_shape),
        scratch_shapes=scratch,
        cost_estimate=cost,
        compiler_params=pltpu.CompilerParams(vmem_limit_bytes=32 << 20),
    )


def exchange(array):
    return lax.all_to_all(array, ORDER, split_axis=0, concat_axis=0, tiled=True)


def exchange_rows(array, rows):
    shape = array.shape
    return exchange(array.reshape(-1, 1, rows * LANES)).reshape(shape)


def local(
    means, log_scales, quat_w, quat_v, opacity, sh_coeffs, cameras, requests, lists, counts, image_cot
):
    devices = N_IMG * N_TILE
    by_owner = jnp.transpose(requests.reshape(N_IMG, N_TILE, CAP), (0, 2, 1)).reshape(N_IMG * CAP, N_TILE)
    wanted = call(ask_kernel, "ask", jax.ShapeDtypeStruct((devices, LANES), jnp.int32), [], 1)(by_owner)
    asked = exchange_rows(wanted, 1)
    meta = jnp.concatenate(
        [counts[0], jnp.stack([lax.axis_index("tile"), lax.axis_index("img")]).astype(jnp.int32)]
    )
    owned = [
        pltpu.with_memory_space_constraint(a, pltpu.HBM)
        for a in (means, log_scales, quat_w, quat_v, opacity, sh_coeffs, cameras)
    ]
    feats, table = call(
        project_kernel,
        "project",
        (jax.ShapeDtypeStruct((N_FEAT, N_IMG, OWNED), f32), jax.ShapeDtypeStruct((N_IMG, LANES), f32)),
        [pltpu.VMEM((48, N_IMG, LANES), f32)]
        + [pltpu.VMEM(a.shape, f32) for a in owned]
        + [pltpu.SemaphoreType.DMA((7,))],
        7,
        memory=pltpu.HBM,
        cost=pl.CostEstimate(flops=20_000_000, transcendentals=0, bytes_accessed=1_000_000),
    )(*owned)
    asked, feats, meta = lax.optimization_barrier((asked, feats, meta))
    packed, index = call(
        pick_kernel,
        "pick",
        (
            jax.ShapeDtypeStruct((FEAT_ROWS * devices, LANES), f32),
            jax.ShapeDtypeStruct((N_IMG, N_TILE * CAP), jnp.int32),
        ),
        [pltpu.VMEM((32, N_IMG, LANES), jnp.int32)],
        3,
        smem=1,
    )(meta, asked, feats)
    rows = exchange_rows(packed, FEAT_ROWS)
    rendered, slot_grads = call(
        render_kernel,
        "render",
        (
            jax.ShapeDtypeStruct((3, TILES_HERE, PIX), f32),
            jax.ShapeDtypeStruct((GRAD_ROWS * devices, LANES), f32),
        ),
        [
            pltpu.VMEM((N_FEAT, 32, LANES), f32),
            pltpu.VMEM((N_USED, 8, LIST), f32),
            pltpu.VMEM((2, 32 * N_GRAD, 2 * LIST), bf16),
            pltpu.VMEM((32 * N_GRAD, LANES), f32),
            pltpu.VMEM((2 * LIST, LIST), bf16),
            pltpu.VMEM((2 * LIST, LIST), bf16),
            pltpu.VMEM((2, PIX, LIST), f32),
            pltpu.VMEM((2, PIX, 2 * LIST), bf16),
            pltpu.VMEM((2, PIX, LIST), f32),
            pltpu.VMEM((2, PIX, LIST), f32),
            pltpu.VMEM((2, 2 * PIX, LIST), bf16),
            pltpu.VMEM((2, PIX, 2 * LIST), bf16),
            pltpu.VMEM((N_USED, 8, LANES), f32),
        ],
        4,
        smem=1,
    )(meta, rows, lists[0], image_cot[0])
    returned = exchange_rows(slot_grads, GRAD_ROWS)
    param_grad, camera_grad, rendered = call(
        pull_kernel,
        "pull",
        (
            jax.ShapeDtypeStruct((59, OWNED), f32),
            jax.ShapeDtypeStruct((N_IMG, 10), f32),
            jax.ShapeDtypeStruct((3, TILES_HERE, PIX), f32),
        ),
        [
            pltpu.VMEM((N_GRAD, N_IMG, N_TILE * CAP), f32),
            pltpu.VMEM((16 * N_GRAD, 2 * N_TILE * CAP), bf16),
            pltpu.VMEM((N_IMG * 16 * N_GRAD, LANES), f32),
            pltpu.VMEM((24, OWNED), f32),
        ],
        10,
        smem=1,
    )(meta, returned, index, feats, table, log_scales, quat_w, quat_v, cameras, rendered)
    return (rendered[None], param_grad, camera_grad)


def solution(mesh):
    own = P(None, ALL)
    return jax.shard_map(
        local,
        mesh=mesh,
        in_specs=(
            own,
            own,
            own,
            own,
            own,
            own,
            P(),
            P("img", "tile", None, None, None),
            P("img", "tile", None),
            P("img", "tile"),
            P("img", None, "tile", None),
        ),
        out_specs=(P("img", None, "tile", None), own, P()),
        check_vma=False,
    )
```

```python
import jax
import jax.numpy as jnp
from jax import lax
from jax.experimental import pallas as pl
from jax.experimental.pallas import tpu as pltpu
from jax.sharding import PartitionSpec as P

TILE_SIDE = 16
TW = 16
ALL = ("img", "tile")
ORDER = ("tile", "img")
N_IMG = 8
N_TILE = 32
CAP = 16
OWNED = 2048
LIST = 256
TILES_HERE = 8
PIX = 256
LANES = 128
N_FEAT = 24
N_USED = 9
N_GRAD = 9
FEAT_ROWS = 3
GRAD_ROWS = 2

sh_first = 0.28209479177387814
sh_second = 0.4886025119029199
sh_third = (
    1.0925484305920792,
    -1.0925484305920792,
    0.31539156525252005,
    -1.0925484305920792,
    0.5462742152960396,
)
sh_fourth = (
    -0.5900435899266435,
    2.890611442640554,
    -0.4570457994644658,
    0.3731763325901154,
    -0.4570457994644658,
    1.445305721320277,
    -0.5900435899266435,
)
dilation = 0.3
LOG2E = 1.4426950408889634
f32 = jnp.float32
bf16 = jnp.bfloat16


def harmonics_of(polar, azimuth):
    sin_p, cos_p = jnp.sin(polar), jnp.cos(polar)
    x = sin_p * jnp.cos(azimuth)
    y = sin_p * jnp.sin(azimuth)
    z = cos_p
    xx, yy, zz = x * x, y * y, z * z
    return [
        sh_first + 0.0 * x,
        -sh_second * y,
        sh_second * z,
        -sh_second * x,
        sh_third[0] * x * y,
        sh_third[1] * y * z,
        sh_third[2] * (2.0 * zz - xx - yy),
        sh_third[3] * x * z,
        sh_third[4] * (xx - yy),
        sh_fourth[0] * y * (3.0 * xx - yy),
        sh_fourth[1] * x * y * z,
        sh_fourth[2] * y * (4.0 * zz - xx - yy),
        sh_fourth[3] * z * (2.0 * zz - 3.0 * xx - 3.0 * yy),
        sh_fourth[4] * x * (4.0 * zz - xx - yy),
        sh_fourth[5] * z * (xx - yy),
        sh_fourth[6] * x * (xx - 3.0 * yy),
    ]


def shape_matrix(log_scales, quat):
    w, x, y, z = quat
    norm = jnp.sqrt(w * w + x * x + y * y + z * z)
    w, x, y, z = w / norm, x / norm, y / norm, z / norm
    rotation = (
        (1.0 - 2.0 * (y * y + z * z), 2.0 * (x * y - w * z), 2.0 * (x * z + w * y)),
        (2.0 * (x * y + w * z), 1.0 - 2.0 * (x * x + z * z), 2.0 * (y * z - w * x)),
        (2.0 * (x * z - w * y), 2.0 * (y * z + w * x), 1.0 - 2.0 * (x * x + y * y)),
    )
    stretch = [jnp.exp(v) for v in log_scales]
    return [[rotation[r][c] * stretch[c] for c in range(3)] for r in range(3)]


def turn_groups(vregs):
    group = lax.broadcasted_iota(jnp.int32, (8, LANES), 1) // CAP
    work = [vregs[-k % 8] for k in range(8)]
    for bit in (1, 2, 4):
        move = (group & bit) != 0
        work = [jnp.where(move, work[(k - bit) % 8], work[k]) for k in range(8)]
    return work


def rotate(value, groups):
    if isinstance(groups, int):
        shift = CAP * groups % LANES
        return value if shift == 0 else pltpu.roll(value, shift, 1)
    return pltpu.roll(value, (CAP * groups) & (LANES - 1), 1)


def swap_groups(vregs, turned=0, leave=False):
    vregs = turn_groups([rotate(v, i + LANES // CAP - turned) for i, v in enumerate(vregs)])
    return vregs if leave else [rotate(v, -g) for g, v in enumerate(vregs)]


def lane_take(table, lanes):
    return jnp.take_along_axis(table, lanes, axis=1, mode="promise_in_bounds")


def halves(value):
    high = value.astype(bf16)
    return high, (value - high.astype(f32)).astype(bf16)


def row_parts(row):
    return halves(jnp.broadcast_to(row, (16, row.shape[1])))


def dot(a, b):
    return lax.dot_general(a, b, (((1,), (0,)), ((), ())), preferred_element_type=f32)


def dot_t(a, b):
    return lax.dot_general(a, b, (((1,), (1,)), ((), ())), preferred_element_type=f32)


PROJECT_CHUNK = 256


def ask_kernel(wanted, out):
    padded = jnp.concatenate([wanted[...], jnp.zeros((LANES, LANES - N_TILE), jnp.int32)], axis=1)
    turned = jnp.transpose(padded)
    for b in range(N_TILE):
        out[8 * b : 8 * b + 8, :] = jnp.broadcast_to(turned[b : b + 1, :], (8, LANES))


def asked_lanes(asked, my_img):
    group = lax.broadcasted_iota(jnp.int32, (8, LANES), 1) // CAP
    base = LANES - CAP * my_img
    result = []
    for q in range(4):
        total = None
        for k in range(8):
            piece = pltpu.roll(asked[8 * (8 * q + k) : 8 * (8 * q + k) + 8, :], (base + CAP * k) & (LANES - 1), 1)
            total = piece if k == 0 else jnp.where(group == k, piece, total)
        result.append(total)
    return result


def project(means, log_scales, quat_w, quat_v, opacity, sh, cam, out, harm):
    column = [jnp.broadcast_to(cam[:, m : m + 1], (N_IMG, PROJECT_CHUNK)) for m in range(8)]

    def chunk(h, carry):
        at = pl.ds(pl.multiple_of(h * PROJECT_CHUNK, PROJECT_CHUNK), PROJECT_CHUNK)
        mean = [means[c : c + 1, at] for c in range(3)]
        quat = [quat_w[0:1, at]] + [quat_v[c : c + 1, at] for c in range(3)]
        m = shape_matrix([log_scales[c : c + 1, at] for c in range(3)], quat)
        for row in range(2):
            a = column[3 * row : 3 * row + 3]
            out[row, :, at] = a[0] * mean[0] + a[1] * mean[1] + a[2] * mean[2] + column[6 + row]
        p = [
            [
                sum(column[3 * row + r] * m[r][c] for r in range(3))
                for c in range(3)
            ]
            for row in range(2)
        ]
        s00 = p[0][0] * p[0][0] + p[0][1] * p[0][1] + p[0][2] * p[0][2] + dilation
        s01 = p[0][0] * p[1][0] + p[0][1] * p[1][1] + p[0][2] * p[1][2]
        s11 = p[1][0] * p[1][0] + p[1][1] * p[1][1] + p[1][2] * p[1][2] + dilation
        det = s00 * s11 - s01 * s01
        out[2, :, at] = s11 / det
        out[3, :, at] = -s01 / det
        out[4, :, at] = s00 / det
        base = 1.0 / (1.0 + jnp.exp(-opacity[0:1, at]))
        out[5, :, at] = jnp.broadcast_to(base, (N_IMG, PROJECT_CHUNK))
        for c in range(3):
            out[9 + c, :, at] = jnp.broadcast_to(mean[c], (N_IMG, PROJECT_CHUNK))
            for row in range(2):
                out[12 + 3 * row + c, :, at] = (
                    m[c][0] * p[row][0] + m[c][1] * p[row][1] + m[c][2] * p[row][2]
                )
        for base_row, first, start in ((6, 0, 0.5), (18, 16, 0.0), (21, 32, 0.0)):
            total = [jnp.full((N_IMG, PROJECT_CHUNK), start, f32) for _ in range(3)]
            for b in range(16):
                y = jnp.concatenate([harm[first + b]] * (PROJECT_CHUNK // LANES), axis=1)
                for k in range(3):
                    total[k] = total[k] + y * sh[16 * k + b : 16 * k + b + 1, at]
            for k in range(3):
                out[base_row + k, :, at] = total[k]
        return carry

    lax.fori_loop(0, OWNED // PROJECT_CHUNK, chunk, 0)


def project_kernel(*refs):
    sources, (feats, table), rest = refs[:7], refs[7:9], refs[9:]
    harm, held, sems = rest[0], rest[1:8], rest[8]
    copies = [pltpu.make_async_copy(a, b, sems.at[n]) for n, (a, b) in enumerate(zip(sources, held))]
    for copy in reversed(copies):
        copy.start()
    for copy in reversed(copies):
        copy.wait()
    means, log_scales, quat_w, quat_v, opacity, sh, cam = held
    polar = jnp.broadcast_to(cam[:, 8:9], (N_IMG, LANES))
    azimuth = jnp.broadcast_to(cam[:, 9:10], (N_IMG, LANES))
    one, zero = jnp.ones_like(polar), jnp.zeros_like(polar)
    values, d_polar = jax.jvp(harmonics_of, (polar, azimuth), (one, zero))
    d_azimuth = jax.jvp(harmonics_of, (polar, azimuth), (zero, one))[1]
    lanes = lax.broadcasted_iota(jnp.int32, (N_IMG, LANES), 1)
    packed = jnp.zeros((N_IMG, LANES), f32)
    for b in range(16):
        harm[b] = values[b]
        harm[16 + b] = d_polar[b]
        harm[32 + b] = d_azimuth[b]
        packed = jnp.where(lanes == b, values[b], packed)
    table[...] = packed
    project(means, log_scales, quat_w, quat_v, opacity, sh, cam, feats, harm)


def pick_kernel(meta, asked, feats, out, idx_out, index):
    for q, value in enumerate(asked_lanes(asked, meta[TILES_HERE + 1])):
        idx_out[:, q * LANES : (q + 1) * LANES] = value
        for f in range(8):
            index[8 * q + f] = rotate(value, f)

    def step(n, carry):
        g, q = n >> 2, n & 3
        picked = []
        for f in range(8):
            here = index[8 * q + f]
            low, high = here & (LANES - 1), here >> 7
            value = None
            for h in range(OWNED // LANES):
                found = lane_take(feats[8 * g + f, :, h * LANES : (h + 1) * LANES], low)
                value = found if h == 0 else jnp.where(high == h, found, value)
            picked.append(value)
        for k, row in enumerate(turn_groups(picked)):
            out[pl.ds(FEAT_ROWS * 8 * (8 * q + k) + g, 8, stride=FEAT_ROWS), :] = row
        return carry

    lax.fori_loop(0, 4 * FEAT_ROWS, step, 0, unroll=6)


def render_kernel(
    meta,
    rows,
    lists,
    cot,
    image,
    out,
    tab,
    feat,
    grads,
    slot,
    upper,
    lower,
    al_s,
    lk_s,
    lb_s,
    s_s,
    w_s,
    sw_s,
    later,
):
    tile_base = meta[TILES_HERE] * TILES_HERE
    turned = meta[TILES_HERE] & 7

    def sort_rows(n, carry):
        g, q = n >> 2, n & 3
        pieces = [
            rows[pl.ds(FEAT_ROWS * 8 * (8 * q + k) + g, 8, stride=FEAT_ROWS), :] for k in range(8)
        ]
        pieces = swap_groups(pieces, turned)
        for f in range(8):
            tab[8 * g + f, pl.ds(pl.multiple_of(8 * q, 8), 8), :] = pieces[f]
        return carry

    lax.fori_loop(0, 4 * FEAT_ROWS, sort_rows, 0, unroll=4)

    def entries(quad):
        s = jnp.concatenate(
            [lists[4 * quad : 4 * quad + 4, h * LANES : (h + 1) * LANES] for h in range(2)], axis=0
        )
        return s & (LANES - 1), ((s >> 7) & 3) * 8 + (s >> 9)

    def gather(ch, carry, lane, chunk):
        hit = chunk == ch
        return tuple(
            jnp.where(hit, lane_take(jnp.broadcast_to(tab[f, pl.ds(ch, 1), :], (8, LANES)), lane), carry[f])
            for f in range(N_USED)
        )

    def keep(found, quad):
        for f in range(N_USED):
            for h in range(2):
                feat[f, 4 * quad : 4 * quad + 4, h * LANES : (h + 1) * LANES] = found[f][4 * h : 4 * h + 4, :]

    zero = jnp.zeros((8, LANES), f32)
    first_lane, first_chunk = entries(0)
    keep(
        lax.fori_loop(
            0, 32, lambda ch, c: gather(ch, c, first_lane, first_chunk), tuple([zero] * N_USED), unroll=16
        ),
        0,
    )
    for f in range(N_USED):
        later[f] = zero
    ri = lax.broadcasted_iota(jnp.int32, (LIST, LIST), 0)
    ci = lax.broadcasted_iota(jnp.int32, (LIST, LIST), 1)
    up = (ri < ci).astype(f32).astype(bf16)
    lo = (ri > ci).astype(f32).astype(bf16)
    for part in range(2):
        upper[part * LIST : (part + 1) * LIST, :] = up
        lower[part * LIST : (part + 1) * LIST, :] = lo
    slot[...] = jnp.zeros_like(slot)
    lane = lax.broadcasted_iota(jnp.int32, (1, LIST), 1)
    px = lax.broadcasted_iota(jnp.int32, (8, LIST), 0).astype(f32) - 7.5
    ch_iota = lax.broadcasted_iota(jnp.int32, (32, LIST), 0)
    lane_iota = lax.broadcasted_iota(jnp.int32, (LANES, LIST), 0)

    def row8(v):
        return jnp.broadcast_to(v, (8, LIST))

    def pair(pair_index, carry):
        tiles = [2 * pair_index, 2 * pair_index + 1]
        state = []
        for p in range(2):
            j = tiles[p]
            number = tile_base + j
            centre_x = (TILE_SIDE * (number % TW)).astype(f32) + (0.5 * TILE_SIDE - 0.5 * TILE_SIDE * TW)
            centre_y = (TILE_SIDE * (number // TW)).astype(f32) + (0.5 * TILE_SIDE - 0.5 * TILE_SIDE * TW)
            at = pl.ds(j, 1)
            ux = feat[0, at, :] - centre_x
            uy = row8(feat[1, at, :] - centre_y)
            ca, cb, cc = feat[2, at, :], feat[3, at, :], feat[4, at, :]
            op = row8(jnp.where(lane < meta[j], feat[5, at, :], 0.0))
            cc = row8(cc * (-0.5 * LOG2E))
            ux, na, nb = row8(ux), row8(ca * (-0.5 * LOG2E)), row8(cb * (-LOG2E))
            dx = [px - ux, px + (8.0 - ux)]
            na = [na * d * d for d in dx]
            nb = [nb * d for d in dx]
            colours = jnp.concatenate([feat[6 + k, at, :] for k in range(3)], axis=0)
            cots = jnp.concatenate([cot[k, at, :] for k in range(3)], axis=0)
            col_h, col_l, cot_h, cot_l = [v.astype(f32) for v in halves(colours) + halves(cots)]
            pad = jnp.zeros((4, LIST), f32)
            cot_k = jnp.concatenate([cot_h, cot_h, cot_l, cot_l, pad], axis=0)
            col_k = jnp.concatenate([col_h, col_l, col_h, col_l, pad], axis=0).astype(bf16)
            s_s[p] = dot(jnp.transpose(cot_k).astype(bf16), col_k)
            for py in range(TILE_SIDE):
                r = slice(TILE_SIDE * py, TILE_SIDE * (py + 1))
                dy = (py - 7.5) - uy
                cy = cc * dy * dy
                alpha = jnp.concatenate(
                    [op * jnp.exp2((na[h] + cy) + nb[h] * dy) for h in range(2)], axis=0
                )
                al_s[p, r, :] = alpha
                hi, low = halves(jnp.log2(1.0 - alpha))
                lk_s[p, r, 0:LIST] = hi
                lk_s[p, r, LIST : 2 * LIST] = low
            state.append((at, uy, dx, col_h, col_l, cot_h, cot_l))
        for p in range(2):
            lb_s[p] = dot(lk_s[p], upper[...])
        for p in range(2):
            for py in range(TILE_SIDE):
                r = slice(TILE_SIDE * py, TILE_SIDE * (py + 1))
                w = al_s[p, r, :] * jnp.exp2(lb_s[p, r, :])
                hi, low = halves(w)
                w_s[p, r, :] = hi
                w_s[p, PIX + TILE_SIDE * py : PIX + TILE_SIDE * (py + 1), :] = low
                sw = s_s[p, r, :] * w
                s_s[p, r, :] = sw
                hi, low = halves(sw)
                sw_s[p, r, 0:LIST] = hi
                sw_s[p, r, LIST : 2 * LIST] = low
        for p in range(2):
            lb_s[p] = dot(sw_s[p], lower[...])
        for p in range(2):
            at, uy, dx, col_h, col_l, cot_h, cot_l = state[p]
            pad2 = jnp.zeros((2, LIST), f32)
            col_rows = jnp.concatenate([col_h, col_l, pad2], axis=0).astype(bf16)
            shown = dot_t(col_rows, w_s[p, 0:PIX, :]) + dot_t(col_rows, w_s[p, PIX : 2 * PIX, :])
            for k in range(3):
                image[k, at, :] = shown[k : k + 1, :] + shown[3 + k : 4 + k, :]
            cot_rows = jnp.concatenate([cot_h, cot_l, pad2], axis=0).astype(bf16)
            gcol = dot(jnp.concatenate([cot_rows, cot_rows], axis=1), w_s[p])
            acc = [[None, None] for _ in range(3)]
            for py in range(TILE_SIDE):
                dy = (py - 7.5) - uy
                for h in range(2):
                    r = slice(TILE_SIDE * py + 8 * h, TILE_SIDE * py + 8 * h + 8)
                    alpha = al_s[p, r, :]
                    g = s_s[p, r, :] - lb_s[p, r, :] * (alpha / (1.0 - alpha))
                    gy = g * dy
                    for n, v in enumerate((g, gy, gy * dy)):
                        acc[n][h] = v if py == 0 else acc[n][h] + v

            def down(a, b):
                return jnp.sum(a + b, axis=0, keepdims=True)

            xg = [dx[h] * acc[0][h] for h in range(2)]
            grad = [
                down(acc[0][0], acc[0][1]),
                down(xg[0], xg[1]),
                down(acc[1][0], acc[1][1]),
                down(dx[0] * xg[0], dx[1] * xg[1]),
                down(dx[0] * acc[1][0], dx[1] * acc[1][1]),
                down(acc[2][0], acc[2][1]),
            ] + [gcol[k : k + 1, :] + gcol[3 + k : 4 + k, :] for k in range(3)]
            s = lists[at, :]
            chunk_hit = (ch_iota == (((s >> 7) & 3) * 8 + (s >> 9))).astype(f32).astype(bf16)
            for f in range(N_GRAD):
                for n, part in enumerate(row_parts(grad[f])):
                    for r in range(0, 32, 16):
                        grads[p, 32 * f + r : 32 * f + r + 16, n * LIST : (n + 1) * LIST] = (
                            chunk_hit[r : r + 16, :] * part
                        )
            lane_hit = (lane_iota == (s & (LANES - 1))).astype(f32).astype(bf16)
            slot[...] += dot_t(grads[p], jnp.concatenate([lane_hit, lane_hit], axis=1))
        lane_at, chunk_at = entries(1)
        found = tuple(later[f] for f in range(N_USED))
        for n in range(16):
            found = gather(16 * (pair_index & 1) + n, found, lane_at, chunk_at)
        for f in range(N_USED):
            later[f] = found[f]
        keep(found, 1)
        return carry

    lax.fori_loop(0, TILES_HERE // 2, pair, 0)

    terms = [jnp.zeros((8, LANES), f32) for _ in range(10)]
    for q in range(4):
        r = slice(8 * q, 8 * q + 8)
        ca, cb, cc = tab[2, r, :], tab[3, r, :], tab[4, r, :]
        gr = [slot[32 * f + 8 * q : 32 * f + 8 * q + 8, :] for f in range(N_GRAD)]
        du = (ca * gr[1] + cb * gr[2], cb * gr[1] + cc * gr[2])
        h00, h01, h11 = conic_pull(ca, cb, cc, gr[3], gr[4], gr[5])
        for c in range(3):
            mean, n0, n1 = tab[9 + c, r, :], tab[12 + c, r, :], tab[15 + c, r, :]
            terms[c] += du[0] * mean + 2.0 * (h00 * n0 + h01 * n1)
            terms[3 + c] += du[1] * mean + 2.0 * (h01 * n0 + h11 * n1)
            terms[8] += gr[6 + c] * tab[18 + c, r, :]
            terms[9] += gr[6 + c] * tab[21 + c, r, :]
        terms[6] += du[0]
        terms[7] += du[1]
    lanes = lax.broadcasted_iota(jnp.int32, (8, LANES), 1)
    share = jnp.zeros((8, LANES), f32)
    for m in range(10):
        total = jnp.sum(jnp.sum(terms[m], axis=0, keepdims=True), axis=1, keepdims=True)
        share = jnp.where(lanes == CAP + m, jnp.broadcast_to(total, (8, LANES)), share)
    group = lanes // CAP
    shares = [rotate(share, k) for k in range(8)]
    for q in range(4):
        pieces = swap_groups([slot[32 * f + 8 * q : 32 * f + 8 * q + 8, :] for f in range(8)], leave=True)
        last = slot[32 * 8 + 8 * q : 32 * 8 + 8 * q + 8, :]
        for k in range(8):
            first_row = GRAD_ROWS * 8 * (8 * q + k)
            out[pl.ds(first_row, 8, stride=GRAD_ROWS), :] = pieces[k]
            out[pl.ds(first_row + 1, 8, stride=GRAD_ROWS), :] = jnp.where(group == k, last, shares[k])


def conic_pull(ca, cb, cc, qxx, qxy, qyy):
    t00, t01 = ca * qxx + cb * qxy, ca * qxy + cb * qyy
    t10, t11 = cb * qxx + cc * qxy, cb * qxy + cc * qyy
    return 0.5 * (t00 * ca + t01 * cb), 0.5 * (t00 * cb + t01 * cc), 0.5 * (t10 * cb + t11 * cc)


PULL_CHUNK = 512


def pull_kernel(
    meta, returned, idx_s, feats, table, log_scales, quat_w, quat_v, cam, image, out, cam_out, image_out, row_s, lhs_s, sum_s
):
    image_out[...] = image[...]
    group = lax.broadcasted_iota(jnp.int32, (8, LANES), 1) // CAP
    turned = meta[TILES_HERE] & 7
    camera = jnp.zeros((8, LANES), f32)
    for q in range(4):
        pieces = [returned[pl.ds(GRAD_ROWS * 8 * (8 * q + k), 8, stride=GRAD_ROWS), :] for k in range(8)]
        pieces = swap_groups(pieces, turned)
        for f in range(8):
            row_s[f, :, q * LANES : (q + 1) * LANES] = pieces[f]
        last = None
        for k in range(8):
            piece = returned[pl.ds(GRAD_ROWS * 8 * (8 * q + k) + 1, 8, stride=GRAD_ROWS), :]
            camera = camera + piece
            moved = rotate(piece, k + 8 - turned)
            last = moved if k == 0 else jnp.where(group == k, moved, last)
        row_s[8, :, q * LANES : (q + 1) * LANES] = last
    cam_out[...] = rotate(camera, 7 - turned)[:, 0:10]

    slots = N_TILE * CAP
    high_iota = lax.broadcasted_iota(jnp.int32, (16, slots), 0)
    lane_iota = lax.broadcasted_iota(jnp.int32, (LANES, slots), 0)

    def image(i, carry):
        at = pl.ds(i, 1)
        s = idx_s[at, :]
        high_hit = (high_iota == (s >> 7)).astype(f32).astype(bf16)
        lane_hit = (lane_iota == (s & (LANES - 1))).astype(f32).astype(bf16)
        for f in range(N_GRAD):
            for n, part in enumerate(row_parts(row_s[f, at, :])):
                lhs_s[16 * f : 16 * (f + 1), n * slots : (n + 1) * slots] = high_hit * part
        sum_s[pl.ds(pl.multiple_of(i * (16 * N_GRAD), 16), 16 * N_GRAD), :] = dot_t(
            lhs_s[...], jnp.concatenate([lane_hit, lane_hit], axis=1)
        )
        return carry

    lax.fori_loop(0, N_IMG, image, 0, unroll=8)

    column = [jnp.broadcast_to(cam[:, m : m + 1], (N_IMG, PULL_CHUNK)) for m in range(6)]

    y_h, y_l = [v.astype(f32) for v in halves(jnp.transpose(table[...])[0:16, :])]
    y_all = jnp.concatenate([y_h, y_h, y_l, y_l], axis=1).astype(bf16)

    def chunk(h, carry):
        at = pl.ds(pl.multiple_of(h * PULL_CHUNK, PULL_CHUNK), PULL_CHUNK)
        parts = PULL_CHUNK // LANES
        gr = [
            jnp.concatenate(
                [sum_s[pl.ds(16 * f + h * parts + e, 8, stride=16 * N_GRAD), :] for e in range(parts)],
                axis=1,
            )
            for f in range(N_GRAD)
        ]
        ca, cb, cc = feats[2, :, at], feats[3, :, at], feats[4, :, at]
        du = (ca * gr[1] + cb * gr[2], cb * gr[1] + cc * gr[2])
        h00, h01, h11 = conic_pull(ca, cb, cc, gr[3], gr[4], gr[5])
        a0, a1 = column[0:3], column[3:6]

        def over_images(v):
            return jnp.sum(v, axis=0, keepdims=True)

        for c in range(3):
            out[c : c + 1, at] = over_images(a0[c] * du[0] + a1[c] * du[1])
        t0 = [h00 * a0[c] + h01 * a1[c] for c in range(3)]
        t1 = [h01 * a0[c] + h11 * a1[c] for c in range(3)]
        v = [[None] * 3 for _ in range(3)]
        for c in range(3):
            for d in range(c, 3):
                v[c][d] = v[d][c] = over_images(t0[c] * a0[d] + t1[c] * a1[d])
        ls = [log_scales[c : c + 1, at] for c in range(3)]
        quat = [quat_w[0:1, at]] + [quat_v[c : c + 1, at] for c in range(3)]
        m, pull = jax.vjp(shape_matrix, ls, quat)
        dm = [[2.0 * sum(v[r][d] * m[d][c] for d in range(3)) for c in range(3)] for r in range(3)]
        dls, dquat = pull(dm)
        for c in range(3):
            out[3 + c : 4 + c, at] = dls[c]
        for c in range(4):
            out[6 + c : 7 + c, at] = dquat[c]
        base = feats[5, 0:1, at]
        out[10:11, at] = over_images(gr[0]) * (1.0 - base)
        for k in range(3):
            g_h, g_l = [v.astype(f32) for v in halves(gr[6 + k])]
            g_all = jnp.concatenate([g_h, g_l, g_h, g_l], axis=0).astype(bf16)
            out[11 + 16 * k : 27 + 16 * k, at] = dot(y_all, g_all)
        return carry

    lax.fori_loop(0, OWNED // PULL_CHUNK, chunk, 0, unroll=2)


def whole(memory=pltpu.VMEM):
    return pl.BlockSpec(memory_space=memory)


def call(kernel, name, out_shape, scratch, n_in, smem=0, memory=pltpu.VMEM, cost=None):
    return pl.pallas_call(
        kernel,
        name=name,
        out_shape=out_shape,
        in_specs=[whole(pltpu.SMEM)] * smem + [whole(memory)] * (n_in - smem),
        out_specs=jax.tree.map(lambda _: whole(), out_shape),
        scratch_shapes=scratch,
        cost_estimate=cost,
        compiler_params=pltpu.CompilerParams(vmem_limit_bytes=32 << 20),
    )


def exchange(array):
    return lax.all_to_all(array, ORDER, split_axis=0, concat_axis=0, tiled=True)


def exchange_rows(array, rows):
    shape = array.shape
    return exchange(array.reshape(-1, 1, rows * LANES)).reshape(shape)


def local(
    means, log_scales, quat_w, quat_v, opacity, sh_coeffs, cameras, requests, lists, counts, image_cot
):
    devices = N_IMG * N_TILE
    by_owner = jnp.transpose(requests.reshape(N_IMG, N_TILE, CAP), (0, 2, 1)).reshape(N_IMG * CAP, N_TILE)
    wanted = call(ask_kernel, "ask", jax.ShapeDtypeStruct((devices, LANES), jnp.int32), [], 1)(by_owner)
    asked = exchange_rows(wanted, 1)
    meta = jnp.concatenate(
        [counts[0], jnp.stack([lax.axis_index("tile"), lax.axis_index("img")]).astype(jnp.int32)]
    )
    owned = [
        pltpu.with_memory_space_constraint(a, pltpu.HBM)
        for a in (means, log_scales, quat_w, quat_v, opacity, sh_coeffs, cameras)
    ]
    feats, table = call(
        project_kernel,
        "project",
        (jax.ShapeDtypeStruct((N_FEAT, N_IMG, OWNED), f32), jax.ShapeDtypeStruct((N_IMG, LANES), f32)),
        [pltpu.VMEM((48, N_IMG, LANES), f32)]
        + [pltpu.VMEM(a.shape, f32) for a in owned]
        + [pltpu.SemaphoreType.DMA((7,))],
        7,
        memory=pltpu.HBM,
        cost=pl.CostEstimate(flops=20_000_000, transcendentals=0, bytes_accessed=1_000_000),
    )(*owned)
    asked, feats, meta = lax.optimization_barrier((asked, feats, meta))
    packed, index = call(
        pick_kernel,
        "pick",
        (
            jax.ShapeDtypeStruct((FEAT_ROWS * devices, LANES), f32),
            jax.ShapeDtypeStruct((N_IMG, N_TILE * CAP), jnp.int32),
        ),
        [pltpu.VMEM((32, N_IMG, LANES), jnp.int32)],
        3,
        smem=1,
    )(meta, asked, feats)
    rows = exchange_rows(packed, FEAT_ROWS)
    rendered, slot_grads = call(
        render_kernel,
        "render",
        (
            jax.ShapeDtypeStruct((3, TILES_HERE, PIX), f32),
            jax.ShapeDtypeStruct((GRAD_ROWS * devices, LANES), f32),
        ),
        [
            pltpu.VMEM((N_FEAT, 32, LANES), f32),
            pltpu.VMEM((N_USED, 8, LIST), f32),
            pltpu.VMEM((2, 32 * N_GRAD, 2 * LIST), bf16),
            pltpu.VMEM((32 * N_GRAD, LANES), f32),
            pltpu.VMEM((2 * LIST, LIST), bf16),
            pltpu.VMEM((2 * LIST, LIST), bf16),
            pltpu.VMEM((2, PIX, LIST), f32),
            pltpu.VMEM((2, PIX, 2 * LIST), bf16),
            pltpu.VMEM((2, PIX, LIST), f32),
            pltpu.VMEM((2, PIX, LIST), f32),
            pltpu.VMEM((2, 2 * PIX, LIST), bf16),
            pltpu.VMEM((2, PIX, 2 * LIST), bf16),
            pltpu.VMEM((N_USED, 8, LANES), f32),
        ],
        4,
        smem=1,
    )(meta, rows, lists[0], image_cot[0])
    returned = exchange_rows(slot_grads, GRAD_ROWS)
    param_grad, camera_grad, rendered = call(
        pull_kernel,
        "pull",
        (
            jax.ShapeDtypeStruct((59, OWNED), f32),
            jax.ShapeDtypeStruct((N_IMG, 10), f32),
            jax.ShapeDtypeStruct((3, TILES_HERE, PIX), f32),
        ),
        [
            pltpu.VMEM((N_GRAD, N_IMG, N_TILE * CAP), f32),
            pltpu.VMEM((16 * N_GRAD, 2 * N_TILE * CAP), bf16),
            pltpu.VMEM((N_IMG * 16 * N_GRAD, LANES), f32),
        ],
        10,
        smem=1,
    )(meta, returned, index, feats, table, log_scales, quat_w, quat_v, cameras, rendered)
    return (rendered[None], param_grad, camera_grad)


def solution(mesh):
    own = P(None, ALL)
    return jax.shard_map(
        local,
        mesh=mesh,
        in_specs=(
            own,
            own,
            own,
            own,
            own,
            own,
            P(),
            P("img", "tile", None, None, None),
            P("img", "tile", None),
            P("img", "tile"),
            P("img", None, "tile", None),
        ),
        out_specs=(P("img", None, "tile", None), own, P()),
        check_vma=False,
    )
```

```python
import jax
import jax.numpy as jnp
from jax import lax
from jax.experimental import pallas as pl
from jax.experimental.pallas import tpu as pltpu
from jax.sharding import PartitionSpec as P

TILE_SIDE = 16
TW = 16
ALL = ("img", "tile")
ORDER = ("tile", "img")
N_IMG = 8
N_TILE = 32
CAP = 16
OWNED = 2048
LIST = 256
TILES_HERE = 8
PIX = 256
LANES = 128
N_FEAT = 24
N_USED = 9
N_GRAD = 9
FEAT_ROWS = 3
GRAD_ROWS = 2

sh_first = 0.28209479177387814
sh_second = 0.4886025119029199
sh_third = (
    1.0925484305920792,
    -1.0925484305920792,
    0.31539156525252005,
    -1.0925484305920792,
    0.5462742152960396,
)
sh_fourth = (
    -0.5900435899266435,
    2.890611442640554,
    -0.4570457994644658,
    0.3731763325901154,
    -0.4570457994644658,
    1.445305721320277,
    -0.5900435899266435,
)
dilation = 0.3
LOG2E = 1.4426950408889634
f32 = jnp.float32
bf16 = jnp.bfloat16


def harmonics_of(polar, azimuth):
    sin_p, cos_p = jnp.sin(polar), jnp.cos(polar)
    x = sin_p * jnp.cos(azimuth)
    y = sin_p * jnp.sin(azimuth)
    z = cos_p
    xx, yy, zz = x * x, y * y, z * z
    return [
        sh_first + 0.0 * x,
        -sh_second * y,
        sh_second * z,
        -sh_second * x,
        sh_third[0] * x * y,
        sh_third[1] * y * z,
        sh_third[2] * (2.0 * zz - xx - yy),
        sh_third[3] * x * z,
        sh_third[4] * (xx - yy),
        sh_fourth[0] * y * (3.0 * xx - yy),
        sh_fourth[1] * x * y * z,
        sh_fourth[2] * y * (4.0 * zz - xx - yy),
        sh_fourth[3] * z * (2.0 * zz - 3.0 * xx - 3.0 * yy),
        sh_fourth[4] * x * (4.0 * zz - xx - yy),
        sh_fourth[5] * z * (xx - yy),
        sh_fourth[6] * x * (xx - 3.0 * yy),
    ]


def shape_matrix(log_scales, quat):
    w, x, y, z = quat
    norm = jnp.sqrt(w * w + x * x + y * y + z * z)
    w, x, y, z = w / norm, x / norm, y / norm, z / norm
    rotation = (
        (1.0 - 2.0 * (y * y + z * z), 2.0 * (x * y - w * z), 2.0 * (x * z + w * y)),
        (2.0 * (x * y + w * z), 1.0 - 2.0 * (x * x + z * z), 2.0 * (y * z - w * x)),
        (2.0 * (x * z - w * y), 2.0 * (y * z + w * x), 1.0 - 2.0 * (x * x + y * y)),
    )
    stretch = [jnp.exp(v) for v in log_scales]
    return [[rotation[r][c] * stretch[c] for c in range(3)] for r in range(3)]


def turn_groups(vregs):
    group = lax.broadcasted_iota(jnp.int32, (8, LANES), 1) // CAP
    work = [vregs[-k % 8] for k in range(8)]
    for bit in (1, 2, 4):
        move = (group & bit) != 0
        work = [jnp.where(move, work[(k - bit) % 8], work[k]) for k in range(8)]
    return work


def rotate(value, groups):
    if isinstance(groups, int):
        shift = CAP * groups % LANES
        return value if shift == 0 else pltpu.roll(value, shift, 1)
    return pltpu.roll(value, (CAP * groups) & (LANES - 1), 1)


def swap_groups(vregs, turned=0, leave=False):
    vregs = turn_groups([rotate(v, i + LANES // CAP - turned) for i, v in enumerate(vregs)])
    return vregs if leave else [rotate(v, -g) for g, v in enumerate(vregs)]


def lane_take(table, lanes):
    return jnp.take_along_axis(table, lanes, axis=1, mode="promise_in_bounds")


def halves(value):
    high = value.astype(bf16)
    return high, (value - high.astype(f32)).astype(bf16)


def row_parts(row):
    return halves(jnp.broadcast_to(row, (16, row.shape[1])))


def dot(a, b):
    return lax.dot_general(a, b, (((1,), (0,)), ((), ())), preferred_element_type=f32)


def dot_t(a, b):
    return lax.dot_general(a, b, (((1,), (1,)), ((), ())), preferred_element_type=f32)


PROJECT_CHUNK = 256


def ask_kernel(wanted, out):
    padded = jnp.concatenate([wanted[...], jnp.zeros((LANES, LANES - N_TILE), jnp.int32)], axis=1)
    turned = jnp.transpose(padded)
    for b in range(N_TILE):
        out[8 * b : 8 * b + 8, :] = jnp.broadcast_to(turned[b : b + 1, :], (8, LANES))


def asked_lanes(asked, my_img):
    group = lax.broadcasted_iota(jnp.int32, (8, LANES), 1) // CAP
    base = LANES - CAP * my_img
    result = []
    for q in range(4):
        total = None
        for k in range(8):
            piece = pltpu.roll(asked[8 * (8 * q + k) : 8 * (8 * q + k) + 8, :], (base + CAP * k) & (LANES - 1), 1)
            total = piece if k == 0 else jnp.where(group == k, piece, total)
        result.append(total)
    return result


def project(means, log_scales, quat_w, quat_v, opacity, sh, cam, out, harm):
    column = [jnp.broadcast_to(cam[:, m : m + 1], (N_IMG, PROJECT_CHUNK)) for m in range(8)]

    def chunk(h, carry):
        at = pl.ds(pl.multiple_of(h * PROJECT_CHUNK, PROJECT_CHUNK), PROJECT_CHUNK)
        mean = [means[c : c + 1, at] for c in range(3)]
        quat = [quat_w[0:1, at]] + [quat_v[c : c + 1, at] for c in range(3)]
        m = shape_matrix([log_scales[c : c + 1, at] for c in range(3)], quat)
        for row in range(2):
            a = column[3 * row : 3 * row + 3]
            out[row, :, at] = a[0] * mean[0] + a[1] * mean[1] + a[2] * mean[2] + column[6 + row]
        p = [
            [
                sum(column[3 * row + r] * m[r][c] for r in range(3))
                for c in range(3)
            ]
            for row in range(2)
        ]
        s00 = p[0][0] * p[0][0] + p[0][1] * p[0][1] + p[0][2] * p[0][2] + dilation
        s01 = p[0][0] * p[1][0] + p[0][1] * p[1][1] + p[0][2] * p[1][2]
        s11 = p[1][0] * p[1][0] + p[1][1] * p[1][1] + p[1][2] * p[1][2] + dilation
        det = s00 * s11 - s01 * s01
        out[2, :, at] = s11 / det
        out[3, :, at] = -s01 / det
        out[4, :, at] = s00 / det
        base = 1.0 / (1.0 + jnp.exp(-opacity[0:1, at]))
        out[5, :, at] = jnp.broadcast_to(base, (N_IMG, PROJECT_CHUNK))
        for c in range(3):
            out[9 + c, :, at] = jnp.broadcast_to(mean[c], (N_IMG, PROJECT_CHUNK))
            for row in range(2):
                out[12 + 3 * row + c, :, at] = (
                    m[c][0] * p[row][0] + m[c][1] * p[row][1] + m[c][2] * p[row][2]
                )
        for base_row, first, start in ((6, 0, 0.5), (18, 16, 0.0), (21, 32, 0.0)):
            total = [jnp.full((N_IMG, PROJECT_CHUNK), start, f32) for _ in range(3)]
            for b in range(16):
                y = jnp.concatenate([harm[first + b]] * (PROJECT_CHUNK // LANES), axis=1)
                for k in range(3):
                    total[k] = total[k] + y * sh[16 * k + b : 16 * k + b + 1, at]
            for k in range(3):
                out[base_row + k, :, at] = total[k]
        return carry

    lax.fori_loop(0, OWNED // PROJECT_CHUNK, chunk, 0)


def project_kernel(*refs):
    sources, (feats, table), rest = refs[:7], refs[7:9], refs[9:]
    harm, held, sems = rest[0], rest[1:8], rest[8]
    copies = [pltpu.make_async_copy(a, b, sems.at[n]) for n, (a, b) in enumerate(zip(sources, held))]
    for copy in reversed(copies):
        copy.start()
    for copy in reversed(copies):
        copy.wait()
    means, log_scales, quat_w, quat_v, opacity, sh, cam = held
    polar = jnp.broadcast_to(cam[:, 8:9], (N_IMG, LANES))
    azimuth = jnp.broadcast_to(cam[:, 9:10], (N_IMG, LANES))
    one, zero = jnp.ones_like(polar), jnp.zeros_like(polar)
    values, d_polar = jax.jvp(harmonics_of, (polar, azimuth), (one, zero))
    d_azimuth = jax.jvp(harmonics_of, (polar, azimuth), (zero, one))[1]
    lanes = lax.broadcasted_iota(jnp.int32, (N_IMG, LANES), 1)
    packed = jnp.zeros((N_IMG, LANES), f32)
    for b in range(16):
        harm[b] = values[b]
        harm[16 + b] = d_polar[b]
        harm[32 + b] = d_azimuth[b]
        packed = jnp.where(lanes == b, values[b], packed)
    table[...] = packed
    project(means, log_scales, quat_w, quat_v, opacity, sh, cam, feats, harm)


def pick_kernel(meta, asked, feats, out, idx_out, index):
    for q, value in enumerate(asked_lanes(asked, meta[TILES_HERE + 1])):
        idx_out[:, q * LANES : (q + 1) * LANES] = value
        for f in range(8):
            index[8 * q + f] = rotate(value, f)

    def step(n, carry):
        g, q = n >> 2, n & 3
        picked = []
        for f in range(8):
            here = index[8 * q + f]
            low, high = here & (LANES - 1), here >> 7
            value = None
            for h in range(OWNED // LANES):
                found = lane_take(feats[8 * g + f, :, h * LANES : (h + 1) * LANES], low)
                value = found if h == 0 else jnp.where(high == h, found, value)
            picked.append(value)
        for k, row in enumerate(turn_groups(picked)):
            out[pl.ds(FEAT_ROWS * 8 * (8 * q + k) + g, 8, stride=FEAT_ROWS), :] = row
        return carry

    lax.fori_loop(0, 4 * FEAT_ROWS, step, 0, unroll=6)


def render_kernel(
    meta,
    rows,
    lists,
    cot,
    image,
    out,
    tab,
    feat,
    grads,
    slot,
    upper,
    lower,
    al_s,
    lk_s,
    lb_s,
    s_s,
    w_s,
    sw_s,
    later,
):
    tile_base = meta[TILES_HERE] * TILES_HERE
    turned = meta[TILES_HERE] & 7

    def sort_rows(n, carry):
        g, q = n >> 2, n & 3
        pieces = [
            rows[pl.ds(FEAT_ROWS * 8 * (8 * q + k) + g, 8, stride=FEAT_ROWS), :] for k in range(8)
        ]
        pieces = swap_groups(pieces, turned)
        for f in range(8):
            tab[8 * g + f, pl.ds(pl.multiple_of(8 * q, 8), 8), :] = pieces[f]
        return carry

    lax.fori_loop(0, 4 * FEAT_ROWS, sort_rows, 0, unroll=4)

    def entries(quad):
        s = jnp.concatenate(
            [lists[4 * quad : 4 * quad + 4, h * LANES : (h + 1) * LANES] for h in range(2)], axis=0
        )
        return s & (LANES - 1), ((s >> 7) & 3) * 8 + (s >> 9)

    def gather(ch, carry, lane, chunk):
        hit = chunk == ch
        return tuple(
            jnp.where(hit, lane_take(jnp.broadcast_to(tab[f, pl.ds(ch, 1), :], (8, LANES)), lane), carry[f])
            for f in range(N_USED)
        )

    def keep(found, quad):
        for f in range(N_USED):
            for h in range(2):
                feat[f, 4 * quad : 4 * quad + 4, h * LANES : (h + 1) * LANES] = found[f][4 * h : 4 * h + 4, :]

    zero = jnp.zeros((8, LANES), f32)
    first_lane, first_chunk = entries(0)
    keep(
        lax.fori_loop(
            0, 32, lambda ch, c: gather(ch, c, first_lane, first_chunk), tuple([zero] * N_USED), unroll=16
        ),
        0,
    )
    for f in range(N_USED):
        later[f] = zero
    ri = lax.broadcasted_iota(jnp.int32, (LIST, LIST), 0)
    ci = lax.broadcasted_iota(jnp.int32, (LIST, LIST), 1)
    up = (ri < ci).astype(f32).astype(bf16)
    lo = (ri > ci).astype(f32).astype(bf16)
    for part in range(2):
        upper[part * LIST : (part + 1) * LIST, :] = up
        lower[part * LIST : (part + 1) * LIST, :] = lo
    slot[...] = jnp.zeros_like(slot)
    lane = lax.broadcasted_iota(jnp.int32, (1, LIST), 1)
    px = lax.broadcasted_iota(jnp.int32, (8, LIST), 0).astype(f32) - 7.5
    ch_iota = lax.broadcasted_iota(jnp.int32, (32, LIST), 0)
    lane_iota = lax.broadcasted_iota(jnp.int32, (LANES, LIST), 0)

    def row8(v):
        return jnp.broadcast_to(v, (8, LIST))

    def pair(pair_index, carry):
        tiles = [2 * pair_index, 2 * pair_index + 1]
        state = []
        for p in range(2):
            j = tiles[p]
            number = tile_base + j
            centre_x = (TILE_SIDE * (number % TW)).astype(f32) + (0.5 * TILE_SIDE - 0.5 * TILE_SIDE * TW)
            centre_y = (TILE_SIDE * (number // TW)).astype(f32) + (0.5 * TILE_SIDE - 0.5 * TILE_SIDE * TW)
            at = pl.ds(j, 1)
            ux = feat[0, at, :] - centre_x
            uy = row8(feat[1, at, :] - centre_y)
            ca, cb, cc = feat[2, at, :], feat[3, at, :], feat[4, at, :]
            op = row8(jnp.where(lane < meta[j], feat[5, at, :], 0.0))
            cc = row8(cc * (-0.5 * LOG2E))
            ux, na, nb = row8(ux), row8(ca * (-0.5 * LOG2E)), row8(cb * (-LOG2E))
            dx = [px - ux, px + (8.0 - ux)]
            na = [na * d * d for d in dx]
            nb = [nb * d for d in dx]
            colours = jnp.concatenate([feat[6 + k, at, :] for k in range(3)], axis=0)
            cots = jnp.concatenate([cot[k, at, :] for k in range(3)], axis=0)
            col_h, col_l, cot_h, cot_l = [v.astype(f32) for v in halves(colours) + halves(cots)]
            pad = jnp.zeros((4, LIST), f32)
            cot_k = jnp.concatenate([cot_h, cot_h, cot_l, cot_l, pad], axis=0)
            col_k = jnp.concatenate([col_h, col_l, col_h, col_l, pad], axis=0).astype(bf16)
            s_s[p] = dot(jnp.transpose(cot_k).astype(bf16), col_k)
            for py in range(TILE_SIDE):
                r = slice(TILE_SIDE * py, TILE_SIDE * (py + 1))
                dy = (py - 7.5) - uy
                cy = cc * dy * dy
                alpha = jnp.concatenate(
                    [op * jnp.exp2((na[h] + cy) + nb[h] * dy) for h in range(2)], axis=0
                )
                al_s[p, r, :] = alpha
                hi, low = halves(jnp.log2(1.0 - alpha))
                lk_s[p, r, 0:LIST] = hi
                lk_s[p, r, LIST : 2 * LIST] = low
            state.append((at, uy, dx, col_h, col_l, cot_h, cot_l))
        for p in range(2):
            lb_s[p] = dot(lk_s[p], upper[...])
        for p in range(2):
            for py in range(TILE_SIDE):
                r = slice(TILE_SIDE * py, TILE_SIDE * (py + 1))
                w = al_s[p, r, :] * jnp.exp2(lb_s[p, r, :])
                hi, low = halves(w)
                w_s[p, r, :] = hi
                w_s[p, PIX + TILE_SIDE * py : PIX + TILE_SIDE * (py + 1), :] = low
                sw = s_s[p, r, :] * w
                s_s[p, r, :] = sw
                hi, low = halves(sw)
                sw_s[p, r, 0:LIST] = hi
                sw_s[p, r, LIST : 2 * LIST] = low
        for p in range(2):
            lb_s[p] = dot(sw_s[p], lower[...])
        for p in range(2):
            at, uy, dx, col_h, col_l, cot_h, cot_l = state[p]
            pad2 = jnp.zeros((2, LIST), f32)
            col_rows = jnp.concatenate([col_h, col_l, pad2], axis=0).astype(bf16)
            shown = dot_t(col_rows, w_s[p, 0:PIX, :]) + dot_t(col_rows, w_s[p, PIX : 2 * PIX, :])
            for k in range(3):
                image[k, at, :] = shown[k : k + 1, :] + shown[3 + k : 4 + k, :]
            cot_rows = jnp.concatenate([cot_h, cot_l, pad2], axis=0).astype(bf16)
            gcol = dot(jnp.concatenate([cot_rows, cot_rows], axis=1), w_s[p])
            acc = [[None, None] for _ in range(3)]
            for py in range(TILE_SIDE):
                dy = (py - 7.5) - uy
                for h in range(2):
                    r = slice(TILE_SIDE * py + 8 * h, TILE_SIDE * py + 8 * h + 8)
                    alpha = al_s[p, r, :]
                    g = s_s[p, r, :] - lb_s[p, r, :] * (alpha / (1.0 - alpha))
                    gy = g * dy
                    for n, v in enumerate((g, gy, gy * dy)):
                        acc[n][h] = v if py == 0 else acc[n][h] + v

            def down(a, b):
                return jnp.sum(a + b, axis=0, keepdims=True)

            xg = [dx[h] * acc[0][h] for h in range(2)]
            grad = [
                down(acc[0][0], acc[0][1]),
                down(xg[0], xg[1]),
                down(acc[1][0], acc[1][1]),
                down(dx[0] * xg[0], dx[1] * xg[1]),
                down(dx[0] * acc[1][0], dx[1] * acc[1][1]),
                down(acc[2][0], acc[2][1]),
            ] + [gcol[k : k + 1, :] + gcol[3 + k : 4 + k, :] for k in range(3)]
            s = lists[at, :]
            chunk_hit = (ch_iota == (((s >> 7) & 3) * 8 + (s >> 9))).astype(f32).astype(bf16)
            for f in range(N_GRAD):
                for n, part in enumerate(row_parts(grad[f])):
                    for r in range(0, 32, 16):
                        grads[p, 32 * f + r : 32 * f + r + 16, n * LIST : (n + 1) * LIST] = (
                            chunk_hit[r : r + 16, :] * part
                        )
            lane_hit = (lane_iota == (s & (LANES - 1))).astype(f32).astype(bf16)
            slot[...] += dot_t(grads[p], jnp.concatenate([lane_hit, lane_hit], axis=1))
        lane_at, chunk_at = entries(1)
        found = tuple(later[f] for f in range(N_USED))
        for n in range(16):
            found = gather(16 * (pair_index & 1) + n, found, lane_at, chunk_at)
        for f in range(N_USED):
            later[f] = found[f]
        keep(found, 1)
        return carry

    lax.fori_loop(0, TILES_HERE // 2, pair, 0)

    terms = [jnp.zeros((8, LANES), f32) for _ in range(10)]
    for q in range(4):
        r = slice(8 * q, 8 * q + 8)
        ca, cb, cc = tab[2, r, :], tab[3, r, :], tab[4, r, :]
        gr = [slot[32 * f + 8 * q : 32 * f + 8 * q + 8, :] for f in range(N_GRAD)]
        du = (ca * gr[1] + cb * gr[2], cb * gr[1] + cc * gr[2])
        h00, h01, h11 = conic_pull(ca, cb, cc, gr[3], gr[4], gr[5])
        for c in range(3):
            mean, n0, n1 = tab[9 + c, r, :], tab[12 + c, r, :], tab[15 + c, r, :]
            terms[c] += du[0] * mean + 2.0 * (h00 * n0 + h01 * n1)
            terms[3 + c] += du[1] * mean + 2.0 * (h01 * n0 + h11 * n1)
            terms[8] += gr[6 + c] * tab[18 + c, r, :]
            terms[9] += gr[6 + c] * tab[21 + c, r, :]
        terms[6] += du[0]
        terms[7] += du[1]
    lanes = lax.broadcasted_iota(jnp.int32, (8, LANES), 1)
    share = jnp.zeros((8, LANES), f32)
    for m in range(10):
        total = jnp.sum(jnp.sum(terms[m], axis=0, keepdims=True), axis=1, keepdims=True)
        share = jnp.where(lanes == CAP + m, jnp.broadcast_to(total, (8, LANES)), share)
    group = lanes // CAP
    shares = [rotate(share, k) for k in range(8)]
    for q in range(4):
        pieces = swap_groups([slot[32 * f + 8 * q : 32 * f + 8 * q + 8, :] for f in range(8)], leave=True)
        last = slot[32 * 8 + 8 * q : 32 * 8 + 8 * q + 8, :]
        for k in range(8):
            first_row = GRAD_ROWS * 8 * (8 * q + k)
            out[pl.ds(first_row, 8, stride=GRAD_ROWS), :] = pieces[k]
            out[pl.ds(first_row + 1, 8, stride=GRAD_ROWS), :] = jnp.where(group == k, last, shares[k])


def conic_pull(ca, cb, cc, qxx, qxy, qyy):
    t00, t01 = ca * qxx + cb * qxy, ca * qxy + cb * qyy
    t10, t11 = cb * qxx + cc * qxy, cb * qxy + cc * qyy
    return 0.5 * (t00 * ca + t01 * cb), 0.5 * (t00 * cb + t01 * cc), 0.5 * (t10 * cb + t11 * cc)


PULL_CHUNK = 512


def pull_kernel(
    meta, returned, idx_s, feats, table, log_scales, quat_w, quat_v, cam, image, out, cam_out, image_out, row_s, lhs_s, sum_s
):
    image_out[...] = image[...]
    group = lax.broadcasted_iota(jnp.int32, (8, LANES), 1) // CAP
    turned = meta[TILES_HERE] & 7
    camera = jnp.zeros((8, LANES), f32)
    for q in range(4):
        pieces = [returned[pl.ds(GRAD_ROWS * 8 * (8 * q + k), 8, stride=GRAD_ROWS), :] for k in range(8)]
        pieces = swap_groups(pieces, turned)
        for f in range(8):
            row_s[f, :, q * LANES : (q + 1) * LANES] = pieces[f]
        last = None
        for k in range(8):
            piece = returned[pl.ds(GRAD_ROWS * 8 * (8 * q + k) + 1, 8, stride=GRAD_ROWS), :]
            camera = camera + piece
            moved = rotate(piece, k + 8 - turned)
            last = moved if k == 0 else jnp.where(group == k, moved, last)
        row_s[8, :, q * LANES : (q + 1) * LANES] = last
    cam_out[...] = rotate(camera, 7 - turned)[:, 0:10]

    slots = N_TILE * CAP
    high_iota = lax.broadcasted_iota(jnp.int32, (16, slots), 0)
    lane_iota = lax.broadcasted_iota(jnp.int32, (LANES, slots), 0)

    def image(i, carry):
        at = pl.ds(i, 1)
        s = idx_s[at, :]
        high_hit = (high_iota == (s >> 7)).astype(f32).astype(bf16)
        lane_hit = (lane_iota == (s & (LANES - 1))).astype(f32).astype(bf16)
        for f in range(N_GRAD):
            for n, part in enumerate(row_parts(row_s[f, at, :])):
                lhs_s[16 * f : 16 * (f + 1), n * slots : (n + 1) * slots] = high_hit * part
        sum_s[pl.ds(pl.multiple_of(i * (16 * N_GRAD), 16), 16 * N_GRAD), :] = dot_t(
            lhs_s[...], jnp.concatenate([lane_hit, lane_hit], axis=1)
        )
        return carry

    lax.fori_loop(0, N_IMG, image, 0, unroll=8)

    column = [jnp.broadcast_to(cam[:, m : m + 1], (N_IMG, PULL_CHUNK)) for m in range(6)]

    y_h, y_l = [v.astype(f32) for v in halves(jnp.transpose(table[...])[0:16, :])]
    y_all = jnp.concatenate([y_h, y_h, y_l, y_l], axis=1).astype(bf16)

    def chunk(h, carry):
        at = pl.ds(pl.multiple_of(h * PULL_CHUNK, PULL_CHUNK), PULL_CHUNK)
        parts = PULL_CHUNK // LANES
        gr = [
            jnp.concatenate(
                [sum_s[pl.ds(16 * f + h * parts + e, 8, stride=16 * N_GRAD), :] for e in range(parts)],
                axis=1,
            )
            for f in range(N_GRAD)
        ]
        ca, cb, cc = feats[2, :, at], feats[3, :, at], feats[4, :, at]
        du = (ca * gr[1] + cb * gr[2], cb * gr[1] + cc * gr[2])
        h00, h01, h11 = conic_pull(ca, cb, cc, gr[3], gr[4], gr[5])
        a0, a1 = column[0:3], column[3:6]

        def over_images(v):
            return jnp.sum(v, axis=0, keepdims=True)

        for c in range(3):
            out[c : c + 1, at] = over_images(a0[c] * du[0] + a1[c] * du[1])
        t0 = [h00 * a0[c] + h01 * a1[c] for c in range(3)]
        t1 = [h01 * a0[c] + h11 * a1[c] for c in range(3)]
        v = [[None] * 3 for _ in range(3)]
        for c in range(3):
            for d in range(c, 3):
                v[c][d] = v[d][c] = over_images(t0[c] * a0[d] + t1[c] * a1[d])
        ls = [log_scales[c : c + 1, at] for c in range(3)]
        quat = [quat_w[0:1, at]] + [quat_v[c : c + 1, at] for c in range(3)]
        m, pull = jax.vjp(shape_matrix, ls, quat)
        dm = [[2.0 * sum(v[r][d] * m[d][c] for d in range(3)) for c in range(3)] for r in range(3)]
        dls, dquat = pull(dm)
        for c in range(3):
            out[3 + c : 4 + c, at] = dls[c]
        for c in range(4):
            out[6 + c : 7 + c, at] = dquat[c]
        base = feats[5, 0:1, at]
        out[10:11, at] = over_images(gr[0]) * (1.0 - base)
        for k in range(3):
            g_h, g_l = [v.astype(f32) for v in halves(gr[6 + k])]
            g_all = jnp.concatenate([g_h, g_l, g_h, g_l], axis=0).astype(bf16)
            out[11 + 16 * k : 27 + 16 * k, at] = dot(y_all, g_all)
        return carry

    lax.fori_loop(0, OWNED // PULL_CHUNK, chunk, 0, unroll=2)


def whole(memory=pltpu.VMEM):
    return pl.BlockSpec(memory_space=memory)


def call(kernel, name, out_shape, scratch, n_in, smem=0, memory=pltpu.VMEM, cost=None):
    return pl.pallas_call(
        kernel,
        name=name,
        out_shape=out_shape,
        in_specs=[whole(pltpu.SMEM)] * smem + [whole(memory)] * (n_in - smem),
        out_specs=jax.tree.map(lambda _: whole(), out_shape),
        scratch_shapes=scratch,
        cost_estimate=cost,
        compiler_params=pltpu.CompilerParams(vmem_limit_bytes=32 << 20),
    )


def exchange(array):
    return lax.all_to_all(array, ORDER, split_axis=0, concat_axis=0, tiled=True)


def exchange_rows(array, rows):
    shape = array.shape
    return exchange(array.reshape(-1, 1, rows * LANES)).reshape(shape)


def local(
    means, log_scales, quat_w, quat_v, opacity, sh_coeffs, cameras, requests, lists, counts, image_cot
):
    devices = N_IMG * N_TILE
    by_owner = jnp.transpose(requests.reshape(N_IMG, N_TILE, CAP), (0, 2, 1)).reshape(N_IMG * CAP, N_TILE)
    wanted = call(ask_kernel, "ask", jax.ShapeDtypeStruct((devices, LANES), jnp.int32), [], 1)(
        pltpu.with_memory_space_constraint(by_owner, pltpu.HBM)
    )
    asked = exchange_rows(wanted, 1)
    meta = jnp.concatenate(
        [counts[0], jnp.stack([lax.axis_index("tile"), lax.axis_index("img")]).astype(jnp.int32)]
    )
    owned = [
        pltpu.with_memory_space_constraint(a, pltpu.HBM)
        for a in (means, log_scales, quat_w, quat_v, opacity, sh_coeffs, cameras)
    ]
    feats, table = call(
        project_kernel,
        "project",
        (jax.ShapeDtypeStruct((N_FEAT, N_IMG, OWNED), f32), jax.ShapeDtypeStruct((N_IMG, LANES), f32)),
        [pltpu.VMEM((48, N_IMG, LANES), f32)]
        + [pltpu.VMEM(a.shape, f32) for a in owned]
        + [pltpu.SemaphoreType.DMA((7,))],
        7,
        memory=pltpu.HBM,
        cost=pl.CostEstimate(flops=20_000_000, transcendentals=0, bytes_accessed=1_000_000),
    )(*owned)
    asked, feats, meta = lax.optimization_barrier((asked, feats, meta))
    packed, index = call(
        pick_kernel,
        "pick",
        (
            jax.ShapeDtypeStruct((FEAT_ROWS * devices, LANES), f32),
            jax.ShapeDtypeStruct((N_IMG, N_TILE * CAP), jnp.int32),
        ),
        [pltpu.VMEM((32, N_IMG, LANES), jnp.int32)],
        3,
        smem=1,
    )(meta, asked, feats)
    rows = exchange_rows(packed, FEAT_ROWS)
    rendered, slot_grads = call(
        render_kernel,
        "render",
        (
            jax.ShapeDtypeStruct((3, TILES_HERE, PIX), f32),
            jax.ShapeDtypeStruct((GRAD_ROWS * devices, LANES), f32),
        ),
        [
            pltpu.VMEM((N_FEAT, 32, LANES), f32),
            pltpu.VMEM((N_USED, 8, LIST), f32),
            pltpu.VMEM((2, 32 * N_GRAD, 2 * LIST), bf16),
            pltpu.VMEM((32 * N_GRAD, LANES), f32),
            pltpu.VMEM((2 * LIST, LIST), bf16),
            pltpu.VMEM((2 * LIST, LIST), bf16),
            pltpu.VMEM((2, PIX, LIST), f32),
            pltpu.VMEM((2, PIX, 2 * LIST), bf16),
            pltpu.VMEM((2, PIX, LIST), f32),
            pltpu.VMEM((2, PIX, LIST), f32),
            pltpu.VMEM((2, 2 * PIX, LIST), bf16),
            pltpu.VMEM((2, PIX, 2 * LIST), bf16),
            pltpu.VMEM((N_USED, 8, LANES), f32),
        ],
        4,
        smem=1,
    )(meta, rows, lists[0], image_cot[0])
    returned = exchange_rows(slot_grads, GRAD_ROWS)
    param_grad, camera_grad, rendered = call(
        pull_kernel,
        "pull",
        (
            jax.ShapeDtypeStruct((59, OWNED), f32),
            jax.ShapeDtypeStruct((N_IMG, 10), f32),
            jax.ShapeDtypeStruct((3, TILES_HERE, PIX), f32),
        ),
        [
            pltpu.VMEM((N_GRAD, N_IMG, N_TILE * CAP), f32),
            pltpu.VMEM((16 * N_GRAD, 2 * N_TILE * CAP), bf16),
            pltpu.VMEM((N_IMG * 16 * N_GRAD, LANES), f32),
        ],
        10,
        smem=1,
    )(meta, returned, index, feats, table, log_scales, quat_w, quat_v, cameras, rendered)
    return (rendered[None], param_grad, camera_grad)


def solution(mesh):
    own = P(None, ALL)
    return jax.shard_map(
        local,
        mesh=mesh,
        in_specs=(
            own,
            own,
            own,
            own,
            own,
            own,
            P(),
            P("img", "tile", None, None, None),
            P("img", "tile", None),
            P("img", "tile"),
            P("img", None, "tile", None),
        ),
        out_specs=(P("img", None, "tile", None), own, P()),
        check_vma=False,
    )
```
